8 devices in a mesh: rep: 1 (over z), tp: 2 (over y), sp: 4 (over x, core).
Axes of the slice: x: 2, y: 2, z: 1, core: 2. Of those that a mesh axis runs over, the one named last changes fastest.
Arguments:
- x: bfloat16 [4096, 4096], P(('rep', 'sp'))
- pos: int32 [4096], P(('rep', 'sp'))
- g1: float32 [4096], replicated
- g2: float32 [4096], replicated
- wq: bfloat16 [4096, 4096], P(None, 'tp')
- wk: bfloat16 [4096, 1024], P(None, 'tp')
- wv: bfloat16 [4096, 1024], P(None, 'tp')
- wo: bfloat16 [4096, 4096], P('tp')
- w1: bfloat16 [4096, 14336], P(None, 'tp')
- w3: bfloat16 [4096, 14336], P(None, 'tp')
- w2: bfloat16 [14336, 4096], P('tp')
Outputs:
- output 1: bfloat16 [4096, 4096], P(('rep', 'sp'))
- output 2: bfloat16 [4096, 8, 128], P('rep', ('tp', 'sp'))
- output 3: bfloat16 [4096, 8, 128], P('rep', ('tp', 'sp'))
All inputs are finite; a program needn't handle non-finite values.
Results may differ from the reference program's by a relative error of at most 0.00750525.
Values are sent between devices in bfloat16 or wider.
A program may use at most 1 GiB of HBM per device.

```python
import jax
import jax.numpy as jnp
from jax import lax

TOKENS = 4096
D = 4096
FF = 14336
HEADS = 32
KV_HEADS = 8
HEAD_DIM = 128
KV_REP = 8

EPS = 1e-5
ROPE_BASE = 5e5
NEG = -1e30
SCALE = HEAD_DIM ** -0.5
QBLOCK = min(512, TOKENS)
GROUP = HEADS // KV_HEADS


def setup_inputs(seed: int = 0, part: int = 0) -> dict:
    key = jax.random.PRNGKey(seed)
    ks = jax.random.split(key, 10)
    kx, kp = jax.random.split(jax.random.fold_in(ks[9], part))

    def w(k, shape, fan_in, gain=1.0):
        return (jax.random.normal(k, shape, jnp.float32) * (gain * fan_in ** -0.5)).astype(jnp.bfloat16)

    return {
        "x": jax.random.normal(kx, (TOKENS, D), jnp.float32).astype(jnp.bfloat16),
        "pos": jnp.arange(TOKENS, dtype=jnp.int32) + jax.random.randint(kp, (), 0, 8192, jnp.int32),
        "g1": 1.0 + 0.1 * jax.random.normal(ks[0], (D,), jnp.float32),
        "g2": 1.0 + 0.1 * jax.random.normal(ks[1], (D,), jnp.float32),
        "wq": w(ks[2], (D, HEADS * HEAD_DIM), D, 1.4),
        "wk": w(ks[3], (D, KV_HEADS * HEAD_DIM), D, 1.4),
        "wv": w(ks[4], (D, KV_HEADS * HEAD_DIM), D),
        "wo": w(ks[5], (HEADS * HEAD_DIM, D), HEADS * HEAD_DIM),
        "w1": w(ks[6], (D, FF), D),
        "w3": w(ks[7], (D, FF), D),
        "w2": w(ks[8], (FF, D), FF),
    }


def _rms(x, g):
    x32 = x.astype(jnp.float32)
    r = lax.rsqrt(jnp.mean(x32 * x32, axis=-1, keepdims=True) + EPS)
    return (x32 * r * g).astype(jnp.bfloat16)


def _rope(t, pos):
    half = HEAD_DIM // 2
    inv = ROPE_BASE ** (-2.0 * jnp.arange(half, dtype=jnp.float32) / HEAD_DIM)
    ang = pos.astype(jnp.float32)[:, None] * inv[None, :]
    c = jnp.cos(ang)[:, None, :]
    s = jnp.sin(ang)[:, None, :]
    t1, t2 = t[..., :half], t[..., half:]
    return jnp.concatenate([t1 * c - t2 * s, t2 * c + t1 * s], axis=-1)


def _attend(q, k, v):
    nb = TOKENS // QBLOCK
    qh = q.reshape(nb, QBLOCK, KV_HEADS, GROUP, HEAD_DIM).transpose(2, 0, 3, 1, 4)
    kh = k.transpose(1, 0, 2)
    vh = v.transpose(1, 0, 2)
    cols = jnp.arange(TOKENS)

    def head(a):
        qq, kk, vv = a
        kk = kk.astype(jnp.float32)
        vv = vv.astype(jnp.float32)

        def block(b):
            qb, i = b
            s = jnp.einsum("gqd,nd->gqn", qb.astype(jnp.float32), kk) * SCALE
            rows = i * QBLOCK + jnp.arange(QBLOCK)
            s = jnp.where(rows[:, None] >= cols[None, :], s, NEG)
            p = jax.nn.softmax(s, axis=-1).astype(jnp.bfloat16)
            return jnp.einsum("gqn,nd->gqd", p.astype(jnp.float32), vv).astype(jnp.bfloat16)

        return lax.map(block, (qq, jnp.arange(nb)))

    o = lax.map(head, (qh, kh, vh))
    return o.transpose(1, 3, 0, 2, 4).reshape(TOKENS, HEADS * HEAD_DIM)


def _mlp(x1, g2, w1, w3, w2):
    nb = TOKENS // QBLOCK

    def block(xb):
        u2 = _rms(xb, g2)
        a = jnp.dot(u2, w1, preferred_element_type=jnp.float32)
        b = jnp.dot(u2, w3, preferred_element_type=jnp.float32)
        hid = (jax.nn.silu(a) * b).astype(jnp.bfloat16)
        return (xb.astype(jnp.float32) + jnp.dot(hid, w2, preferred_element_type=jnp.float32)).astype(jnp.bfloat16)

    return lax.map(block, x1.reshape(nb, QBLOCK, D)).reshape(TOKENS, D)


def reference(x, pos, g1, g2, wq, wk, wv, wo, w1, w3, w2):
    u = _rms(x, g1)
    q = _rope(jnp.dot(u, wq, preferred_element_type=jnp.float32).reshape(TOKENS, HEADS, HEAD_DIM), pos).astype(jnp.bfloat16)
    k = _rope(jnp.dot(u, wk, preferred_element_type=jnp.float32).reshape(TOKENS, KV_HEADS, HEAD_DIM), pos).astype(jnp.bfloat16)
    v = jnp.dot(u, wv, preferred_element_type=jnp.float32).astype(jnp.bfloat16).reshape(TOKENS, KV_HEADS, HEAD_DIM)
    a = _attend(q, k, v)
    x1 = (x.astype(jnp.float32) + jnp.dot(a, wo, preferred_element_type=jnp.float32)).astype(jnp.bfloat16)
    y = _mlp(x1, g2, w1, w3, w2)
    r = KV_REP // KV_HEADS
    return y, jnp.repeat(k, r, axis=1), jnp.repeat(v, r, axis=1)
```

```python
import functools

import jax
import jax.numpy as jnp
from jax import lax
from jax.experimental import pallas as pl
from jax.experimental.pallas import tpu as pltpu
from jax.sharding import PartitionSpec as P

HEAD_DIM = 128
EPS = 1e-5
ROPE_BASE = 5e5
SCALE_LOG2E = HEAD_DIM ** -0.5 * 1.4426950408889634
NEG = -1e30
BQ = 512
BK = 1024
MESH = pl.DeviceIdType.MESH
F32 = jnp.float32
BF16 = jnp.bfloat16


def _rms(x, g):
    x32 = x.astype(F32)
    r = lax.rsqrt(jnp.mean(x32 * x32, axis=-1, keepdims=True) + EPS)
    return (x32 * r * g).astype(BF16)


def _tables(pos):
    half = HEAD_DIM // 2
    inv = ROPE_BASE ** (-2.0 * jnp.arange(half, dtype=F32) / HEAD_DIM)
    ang = pos.astype(F32)[:, None] * inv
    c, s = jnp.cos(ang), jnp.sin(ang)
    return jnp.concatenate([c, c], axis=1), jnp.concatenate([-s, s], axis=1)


def _barrier(peers):
    sem = pltpu.get_barrier_semaphore()
    for p in peers:
        pl.semaphore_signal(sem, inc=1, device_id=p, device_id_type=MESH)
    pl.semaphore_wait(sem, len(peers))


def _sp_order(s):
    return [(s + 2) % 4, 3 - s, s + 1 - 2 * (s % 2), s]


def _qkv_body(x_hbm, g_ref, cos_ref, sin_ref, wq_hbm, wk_hbm, wv_hbm, q_hbm, k_hbm, v_hbm,
              xbuf, u, wq, wkv, qo, ko, vo, xsem, wsem, ssem, rsem, lsem):
    rep, tp, s = lax.axis_index("rep"), lax.axis_index("tp"), lax.axis_index("sp")
    order = _sp_order(s)
    m = u.shape[0]
    nb = xbuf.shape[0]
    rows = m // nb
    hm = m // 2
    qw = qo.shape[2]

    def wcopies(t):
        j = order[t]
        sl = t % 2
        return [
            pltpu.make_async_copy(wq_hbm.at[:, pl.ds(pl.multiple_of(j * qw, 128), qw)], wq.at[sl], wsem.at[sl, 0]),
            pltpu.make_async_copy(wk_hbm.at[:, pl.ds(pl.multiple_of(j * 128, 128), 128)], wkv.at[sl, :, pl.ds(0, 128)], wsem.at[sl, 1]),
            pltpu.make_async_copy(wv_hbm.at[:, pl.ds(pl.multiple_of(j * 128, 128), 128)], wkv.at[sl, :, pl.ds(128, 128)], wsem.at[sl, 2]),
        ]

    xc = [pltpu.make_async_copy(x_hbm.at[pl.ds(b * rows, rows), :], xbuf.at[b], xsem.at[b]) for b in range(nb)]
    for c in xc[:2]:
        c.start()
    for c in wcopies(0):
        c.start()
    for c in xc[2:]:
        c.start()
    for c in wcopies(1):
        c.start()
    _barrier([(rep, tp, j) for j in order[:3]])
    for b in range(nb):
        xc[b].wait()

        @pl.loop(0, rows // 64)
        def _(i, b=b):
            xs = xbuf[b, pl.ds(pl.multiple_of(i * 64, 64), 64), :].astype(F32)
            r = lax.rsqrt(jnp.mean(xs * xs, axis=-1, keepdims=True) + EPS)
            u[pl.ds(pl.multiple_of(b * rows + i * 64, 64), 64), :] = (xs * r * g_ref[...]).astype(BF16)

    def rope(t, r0):
        c = cos_ref[pl.ds(r0, t.shape[0]), :]
        sn = sin_ref[pl.ds(r0, t.shape[0]), :]
        return t * c + pltpu.roll(t, 64, 1) * sn

    def pieces(t, h):
        j = order[t]
        dst = pl.ds(pl.multiple_of(s * m + h * hm, hm), hm)
        src = pl.ds(h * hm, hm)
        trip = [(qo.at[t, src, :], q_hbm.at[dst, :]), (ko.at[t, src, :], k_hbm.at[dst, :]), (vo.at[t, src, :], v_hbm.at[dst, :])]
        if t == 3:
            return [pltpu.make_async_copy(a, b, lsem.at[h, i]) for i, (a, b) in enumerate(trip)]
        return [pltpu.make_async_remote_copy(src_ref=a, dst_ref=b, send_sem=ssem.at[t, h, i], recv_sem=rsem.at[t, h, i],
                                             device_id=(rep, tp, j), device_id_type=MESH) for i, (a, b) in enumerate(trip)]

    for t in range(4):
        sl = t % 2
        for c in wcopies(t):
            c.wait()
        for h in range(2):
            @pl.loop(0, hm // 256)
            def _(i, t=t, h=h, sl=sl):
                r0 = pl.multiple_of(h * hm + i * 256, 256)
                ub = u[pl.ds(r0, 256), :]
                qq = jnp.dot(ub, wq[sl], preferred_element_type=F32)
                for n in range(qw // 128):
                    qo[t, pl.ds(r0, 256), n * 128:(n + 1) * 128] = rope(qq[:, n * 128:(n + 1) * 128], r0).astype(BF16)
                kv = jnp.dot(ub, wkv[sl], preferred_element_type=F32)
                ko[t, pl.ds(r0, 256), :] = rope(kv[:, :128], r0).astype(BF16)
                vo[t, pl.ds(r0, 256), :] = kv[:, 128:].astype(BF16)
            for c in pieces(t, h):
                c.start()
        if t < 2:
            for c in wcopies(t + 2):
                c.start()
    for h in range(2):
        for c in pieces(3, h):
            c.wait()
    for t in range(3):
        for h in range(2):
            for c in pieces(t, h):
                c.wait()


def _qkv(x, g1, cos, sin, wq, wk, wv, n):
    m, d = x.shape
    qw = wq.shape[1] // 4
    any_ = pl.BlockSpec(memory_space=pl.ANY)
    vm = pl.BlockSpec(memory_space=pltpu.VMEM)
    return pl.pallas_call(
        _qkv_body,
        in_specs=[any_, vm, vm, vm, any_, any_, any_],
        out_specs=[any_, any_, any_],
        out_shape=[jax.ShapeDtypeStruct((n, qw), BF16), jax.ShapeDtypeStruct((n, 128), BF16), jax.ShapeDtypeStruct((n, 128), BF16)],
        scratch_shapes=[
            pltpu.VMEM((4, m // 4, d), BF16),
            pltpu.VMEM((m, d), BF16),
            pltpu.VMEM((2, d, qw), BF16),
            pltpu.VMEM((2, d, 256), BF16),
            pltpu.VMEM((4, m, qw), BF16),
            pltpu.VMEM((4, m, 128), BF16),
            pltpu.VMEM((4, m, 128), BF16),
            pltpu.SemaphoreType.DMA((4,)),
            pltpu.SemaphoreType.DMA((2, 3)),
            pltpu.SemaphoreType.DMA((3, 2, 3)),
            pltpu.SemaphoreType.DMA((3, 2, 3)),
            pltpu.SemaphoreType.DMA((2, 3)),
        ],
        compiler_params=pltpu.CompilerParams(collective_id=1, has_side_effects=True, vmem_limit_bytes=56 * 2**20),
        cost_estimate=pl.CostEstimate(flops=2 * m * d * (4 * qw + 1024), bytes_accessed=80 * 2**20, transcendentals=0),
        name="qkv_exchange",
    )(x, g1.reshape(1, -1), cos, sin, wq, wk, wv)


def _attn_body(q_ref, k_ref, v_ref, own_hbm, oth_hbm, vt, acc, ms, ls, ob, ssem, rsem, lsem):
    rep, tp, s = lax.axis_index("rep"), lax.axis_index("tp"), lax.axis_index("sp")
    step = pl.program_id(0)
    i = (step % 2) * 4 + step // 2
    nh = q_ref.shape[1] // 128
    order = _sp_order(s)

    @pl.when(step == 0)
    def _():
        _barrier([(rep, tp, j) for j in order[:3]] + [(rep, 1 - tp, j) for j in range(4)])

        @pl.loop(0, k_ref.shape[0] // 512)
        def _(j):
            r0 = pl.multiple_of(j * 512, 512)
            vt[:, pl.ds(r0, 512)] = v_ref[pl.ds(r0, 512), :].T

    ms[...] = jnp.full_like(ms, NEG)
    ls[...] = jnp.zeros_like(ls)
    acc[...] = jnp.zeros_like(acc)

    def blk(k0, n, masked):
        k0 = pl.multiple_of(k0, BQ)
        kb = k_ref[pl.ds(k0, n), :]
        vb = vt[:, pl.ds(k0, n)]

        def scores(h):
            return lax.dot_general(kb, q_ref[:, h * 128:(h + 1) * 128], (((1,), (1,)), ((), ())), preferred_element_type=F32)

        sc = scores(0)
        for h in range(nh):
            nxt = scores(h + 1) if h < nh - 1 else None
            if masked:
                kk = lax.broadcasted_iota(jnp.int32, (n, BQ), 0)
                qq = lax.broadcasted_iota(jnp.int32, (n, BQ), 1) + (i * BQ - k0)
                sc = jnp.where(qq >= kk, sc, NEG)
            m0 = ms[h:h + 1, :]
            m1 = jnp.maximum(m0, jnp.max(sc, axis=0, keepdims=True))
            p = jnp.exp2(sc * SCALE_LOG2E - m1 * SCALE_LOG2E)
            a = jnp.exp2((m0 - m1) * SCALE_LOG2E)
            ms[h:h + 1, :] = m1
            ls[h:h + 1, :] = ls[h:h + 1, :] * a + jnp.sum(p, axis=0, keepdims=True)
            acc[h] = acc[h] * a + jnp.dot(vb, p.astype(BF16), preferred_element_type=F32)
            sc = nxt

    start = i * BQ

    @pl.loop(0, start // BK)
    def _(j):
        blk(j * BK, BK, False)

    @pl.when(start % BK != 0)
    def _():
        blk(start - BQ, BQ, False)

    blk(start, BQ, True)
    for h in range(nh):
        o = acc[h] * (1.0 / ls[h:h + 1, :])
        ob[step, :, h * 128:(h + 1) * 128] = o.T.astype(BF16)

    w = q_ref.shape[1]

    def dst(ref, slot, src_s):
        return ref.at[slot, :, pl.ds(pl.multiple_of(src_s * w, 128), w)]

    def to_own(step):
        b = (step % 2) * 4 + step // 2
        d, half = b // 2, b % 2
        slot = (half + tp + 1) % 2
        return d, slot, pltpu.make_async_remote_copy(
            src_ref=ob.at[step], dst_ref=dst(own_hbm, slot, s), send_sem=ssem.at[0, step], recv_sem=rsem.at[0, s, slot],
            device_id=(rep, tp, d), device_id_type=MESH)

    def to_local(step):
        b = (step % 2) * 4 + step // 2
        half = b % 2
        slot = (half + tp + 1) % 2
        return pltpu.make_async_copy(ob.at[step], dst(own_hbm, slot, s), lsem.at[half])

    def to_oth(step):
        b = (step % 2) * 4 + step // 2
        d, half = b // 2, b % 2
        slot = (half + 1 - tp + 1) % 2
        return pltpu.make_async_remote_copy(
            src_ref=ob.at[step], dst_ref=dst(oth_hbm, slot, s), send_sem=ssem.at[1, step], recv_sem=rsem.at[1, s, slot],
            device_id=(rep, 1 - tp, d), device_id_type=MESH)

    to_oth(step).start()
    mine = i // 2 == s

    @pl.when(mine)
    def _():
        to_local(step).start()

    @pl.when(jnp.logical_not(mine))
    def _():
        to_own(step)[2].start()

    @pl.when(step == pl.num_programs(0) - 1)
    def _():
        @pl.loop(0, 8)
        def _(t):
            to_oth(t).wait_send()
            b = (t % 2) * 4 + t // 2

            @pl.when(b // 2 == s)
            def _():
                to_local(t).wait()

            @pl.when(b // 2 != s)
            def _():
                to_own(t)[2].wait_send()

        @pl.loop(0, 4)
        def _(j):
            @pl.loop(0, 2)
            def _(slot):
                pltpu.make_async_remote_copy(
                    src_ref=ob.at[0], dst_ref=dst(oth_hbm, slot, j), send_sem=ssem.at[1, 0], recv_sem=rsem.at[1, j, slot],
                    device_id=(rep, 1 - tp, j), device_id_type=MESH).wait_recv()

                @pl.when(j != s)
                def _():
                    pltpu.make_async_remote_copy(
                        src_ref=ob.at[0], dst_ref=dst(own_hbm, slot, j), send_sem=ssem.at[0, 0], recv_sem=rsem.at[0, j, slot],
                        device_id=(rep, tp, j), device_id_type=MESH).wait_recv()


def _attention(q, k, v):
    n, w = q.shape
    nh = w // 128
    any_ = pl.BlockSpec(memory_space=pl.ANY)
    full = pl.BlockSpec((n, 128), lambda t: (0, 0))
    shape = jax.ShapeDtypeStruct((2, BQ, 4 * w), BF16)
    return pl.pallas_call(
        _attn_body,
        grid=(n // BQ,),
        in_specs=[pl.BlockSpec((BQ, w), lambda t: ((t % 2) * 4 + t // 2, 0)), full, full],
        out_specs=[any_, any_],
        out_shape=[shape, shape],
        scratch_shapes=[
            pltpu.VMEM((128, n), BF16),
            pltpu.VMEM((nh, 128, BQ), F32),
            pltpu.VMEM((8, BQ), F32),
            pltpu.VMEM((8, BQ), F32),
            pltpu.VMEM((n // BQ, BQ, w), BF16),
            pltpu.SemaphoreType.DMA((2, 8)),
            pltpu.SemaphoreType.DMA((2, 4, 2)),
            pltpu.SemaphoreType.DMA((2,)),
        ],
        compiler_params=pltpu.CompilerParams(collective_id=2, has_side_effects=True, vmem_limit_bytes=56 * 2**20),
        cost_estimate=pl.CostEstimate(flops=2 * n * n * w * 2, bytes_accessed=16 * 2**20, transcendentals=0),
        name="attention_exchange",
    )(q, k, v)


NWO, NHID, NW2 = 8, 28, 16
UNITS = NWO + NHID + NW2
NBUF = 3
MB = 256


def _mlp_body(chunks, own_hbm, oth_hbm, x_hbm, wo_hbm, p0, p1, p2, p3, g_ref, w1_hbm, w3_hbm, w2_hbm, y_hbm,
              wb, abuf, xbuf, hid, pbuf, rbuf, ybuf, wsem, asem, ssem, rsem, ysem, yrsem, ylsem):
    rep, tp, s = lax.axis_index("rep"), lax.axis_index("tp"), lax.axis_index("sp")
    hr = wo_hbm.shape[0]
    qr = hr // 4
    hm = x_hbm.shape[0] // 2
    kh = w2_hbm.shape[0] // 2
    total = UNITS * len(chunks)
    s1 = s + 1 - 2 * (s % 2)
    quarters = [(p0, s), (p1, (s + 2) % 4), (p2, s1), (p3, (s1 + 2) % 4)]
    partner = (rep, 1 - tp, s)

    def col(j, w):
        return pl.ds(pl.multiple_of(j * w, w), w)

    def wo_copies(j, sl):
        cs = [pltpu.make_async_copy(wo_hbm.at[:, col(j, 512)], wb.at[sl, pl.ds(0, hr), :], wsem.at[sl, 0])]
        for n, (p, r) in enumerate(quarters):
            cs.append(pltpu.make_async_copy(p.at[:, col(j, 512)], wb.at[sl, pl.ds(pl.multiple_of(hr + r * qr, qr), qr), :], wsem.at[sl, n + 1]))
        return cs

    def hid_copies(j, sl):
        return [pltpu.make_async_copy(w1_hbm.at[:, col(j, 256)], wb.at[sl, :, pl.ds(0, 256)], wsem.at[sl, 0]),
                pltpu.make_async_copy(w3_hbm.at[:, col(j, 256)], wb.at[sl, :, pl.ds(256, 256)], wsem.at[sl, 1])]

    def w2_copies(t, sl):
        return [pltpu.make_async_copy(w2_hbm.at[pl.ds(pl.multiple_of(t % 2 * kh, 128), kh), col(t // 2, 512)], wb.at[sl, pl.ds(0, kh), :], wsem.at[sl, 0])]

    def issue(g):
        sl, u = g % NBUF, g % UNITS

        @pl.when(g < total)
        def _():
            @pl.when(u < NWO)
            def _():
                for c in wo_copies(u, sl):
                    c.start()

            @pl.when((u >= NWO) & (u < NWO + NHID))
            def _():
                for c in hid_copies(u - NWO, sl):
                    c.start()

            @pl.when(u >= NWO + NHID)
            def _():
                for c in w2_copies(u - NWO - NHID, sl):
                    c.start()

    def acts(c):
        slot, r0, nr = chunks[c]
        base = hm * ((tp + slot + 1) % 2) + r0
        rs = pl.ds(0, nr)
        return (pltpu.make_async_copy(x_hbm.at[pl.ds(pl.multiple_of(base, 128), nr), :], xbuf.at[rs, :], asem.at[0]),
                [pltpu.make_async_copy(own_hbm.at[slot, pl.ds(r0, nr), :], abuf.at[rs, pl.ds(0, hr)], asem.at[1]),
                 pltpu.make_async_copy(oth_hbm.at[slot, pl.ds(r0, nr), :], abuf.at[rs, pl.ds(hr, hr)], asem.at[2])])

    for g in range(NBUF - 1):
        issue(g)
    xc, ac = acts(0)
    xc.start()
    for c in ac:
        c.start()
    _barrier([partner])

    def send(ci, j):
        slot, r0, nr = chunks[ci]
        return pltpu.make_async_remote_copy(src_ref=pbuf.at[j, pl.ds(r0, nr), :], dst_ref=rbuf.at[j, pl.ds(r0, nr), :],
                                            send_sem=ssem.at[ci, j], recv_sem=rsem.at[ci, j], device_id=partner, device_id_type=MESH)

    yr0 = pl.multiple_of(tp * hm, 128)

    def ysend(j):
        return pltpu.make_async_remote_copy(src_ref=ybuf.at[j], dst_ref=y_hbm.at[pl.ds(yr0, hm), col(j, 512)],
                                            send_sem=ysem.at[j], recv_sem=yrsem.at[j], device_id=partner, device_id_type=MESH)

    def yrecv(j):
        return pltpu.make_async_remote_copy(src_ref=ybuf.at[j], dst_ref=y_hbm.at[pl.ds(pl.multiple_of((1 - tp) * hm, 128), hm), col(j, 512)],
                                            send_sem=ysem.at[j], recv_sem=yrsem.at[j], device_id=partner, device_id_type=MESH)

    def yown(j):
        return pltpu.make_async_copy(ybuf.at[j], y_hbm.at[pl.ds(yr0, hm), col(j, 512)], ylsem.at[j])

    nsend = len(chunks) - 1
    for ci, (slot, r0, nr) in enumerate(chunks):
        g0 = ci * UNITS
        xc, ac = acts(ci)
        xc.wait()
        for c in ac:
            c.wait()

        @pl.loop(0, NWO)
        def _(j, g0=g0, nr=nr):
            g = g0 + j
            sl = g % NBUF
            issue(g + NBUF - 1)
            for c in wo_copies(j, sl):
                c.wait()
            for b in range(nr // MB):
                rs = pl.ds(b * MB, MB)
                o = jnp.dot(abuf[rs, :], wb[sl], preferred_element_type=F32)
                xbuf[rs, col(j, 512)] = (xbuf[rs, col(j, 512)].astype(F32) + o).astype(BF16)

        @pl.loop(0, nr // 64)
        def _(i):
            rs = pl.ds(pl.multiple_of(i * 64, 64), 64)
            xs = xbuf[rs, :].astype(F32)
            r = lax.rsqrt(jnp.mean(xs * xs, axis=-1, keepdims=True) + EPS)
            abuf[rs, :] = (xs * r * g_ref[...]).astype(BF16)

        if ci + 1 < len(chunks):
            acts(ci + 1)[0].start()

        @pl.loop(0, NHID)
        def _(j, g0=g0, nr=nr):
            g = g0 + NWO + j
            sl = g % NBUF
            issue(g + NBUF - 1)
            for c in hid_copies(j, sl):
                c.wait()
            for b in range(nr // MB):
                rs = pl.ds(b * MB, MB)
                ab = jnp.dot(abuf[rs, :], wb[sl], preferred_element_type=F32)
                a = ab[:, :256]
                hid[rs, col(j, 256)] = (a / (1.0 + jnp.exp(-a)) * ab[:, 256:]).astype(BF16)

        if ci + 1 < len(chunks):
            for c in acts(ci + 1)[1]:
                c.start()

        @pl.loop(0, NW2 // 2)
        def _(j, g0=g0, ci=ci, slot=slot, r0=r0, nr=nr):
            g = g0 + NWO + NHID + 2 * j
            for h in range(2):
                sl = (g + h) % NBUF
                issue(g + h + NBUF - 1)
                for c in w2_copies(2 * j + h, sl):
                    c.wait()
                for b in range(nr // MB):
                    rs = pl.ds(b * MB, MB)
                    ps = pl.ds(r0 + b * MB, MB)
                    o = jnp.dot(hid[rs, h * kh:(h + 1) * kh], wb[sl, pl.ds(0, kh), :], preferred_element_type=F32)
                    if h == 0:
                        pbuf[j if slot == 0 else NW2 // 2, ps, :] = o
                    elif slot == 0:
                        pbuf[j, ps, :] = pbuf[j, ps, :] + o
                    else:
                        if b == 0:
                            for k in range(nsend):
                                send(k, j).wait_recv()
                        o = o + pbuf[NW2 // 2, ps, :] + rbuf[j, ps, :]
                        ybuf[j, ps, :] = (xbuf[rs, col(j, 512)].astype(F32) + o).astype(BF16)
            if slot == 0:
                send(ci, j).start()
            else:
                ysend(j).start()
                yown(j).start()

    @pl.loop(0, NW2 // 2)
    def _(j):
        for k in range(nsend):
            send(k, j).wait_send()
        ysend(j).wait_send()
        yown(j).wait()
        yrecv(j).wait_recv()


def _mlp(own, oth, x, wo, pieces, g2, w1, w3, w2):
    m, d = x.shape
    hm = m // 2
    chunks = ((0, 0, 256), (0, 256, 256), (1, 0, 512))
    any_ = pl.BlockSpec(memory_space=pl.ANY)
    vm = pl.BlockSpec(memory_space=pltpu.VMEM)
    nt = NW2 // 2
    return pl.pallas_call(
        functools.partial(_mlp_body, chunks),
        in_specs=[any_] * 8 + [vm] + [any_] * 3,
        out_specs=any_,
        out_shape=jax.ShapeDtypeStruct((m, d), BF16),
        scratch_shapes=[
            pltpu.VMEM((NBUF, d, 512), BF16),
            pltpu.VMEM((hm, d), BF16),
            pltpu.VMEM((hm, d), BF16),
            pltpu.VMEM((hm, w2.shape[0]), BF16),
            pltpu.VMEM((nt + 1, hm, 512), F32),
            pltpu.VMEM((nt, hm, 512), F32),
            pltpu.VMEM((nt, hm, 512), BF16),
            pltpu.SemaphoreType.DMA((NBUF, 5)),
            pltpu.SemaphoreType.DMA((3,)),
            pltpu.SemaphoreType.DMA((2, nt)),
            pltpu.SemaphoreType.DMA((2, nt)),
            pltpu.SemaphoreType.DMA((nt,)),
            pltpu.SemaphoreType.DMA((nt,)),
            pltpu.SemaphoreType.DMA((nt,)),
        ],
        compiler_params=pltpu.CompilerParams(collective_id=3, has_side_effects=True, vmem_limit_bytes=67043328),
        cost_estimate=pl.CostEstimate(flops=2 * m * d * (d + 3 * w1.shape[1]), bytes_accessed=640 * 2**20, transcendentals=0),
        name="mlp_sum",
    )(own, oth, x, wo, *pieces, g2.reshape(1, -1), w1, w3, w2)


def solution(mesh):
    tok = P(("rep", "sp"), None)
    col = P(None, "tp")
    row = P("tp", None)
    cache = P("rep", ("tp", "sp"), None)
    swap = [(0, 1), (1, 0)]

    def local(x, pos, g1, g2, wq, wk, wv, wo, w1, w3, w2):
        m, d = x.shape
        n = m * mesh.shape["sp"]
        s = lax.axis_index("sp")
        qr = wo.shape[0] // 4
        piece = lax.ppermute(lax.dynamic_slice(wo, (s * qr, 0), (qr, d)), "tp", swap)
        cos, sin = _tables(pos)
        q, k, v = _qkv(x, g1, cos, sin, wq, wk, wv, n)
        piece, q = lax.optimization_barrier((piece, q))
        far = lax.ppermute(piece, "sp", [(0, 2), (2, 0), (1, 3), (3, 1)])
        own, oth = _attention(q, k, v)
        far, own, oth = lax.optimization_barrier((far, own, oth))
        cross = [(0, 1), (1, 0), (2, 3), (3, 2)]
        near = lax.ppermute(piece, "sp", cross)
        near2 = lax.ppermute(far, "sp", cross)
        y = _mlp(own, oth, x, wo, (piece, far, near, near2), g2, w1, w3, w2)
        return y, k.reshape(n, 1, 128), v.reshape(n, 1, 128)

    return jax.shard_map(
        local,
        mesh=mesh,
        in_specs=(tok, P(("rep", "sp")), P(), P(), col, col, col, row, col, col, row),
        out_specs=(tok, cache, cache),
        check_vma=False,
    )
```

```python
import functools

import jax
import jax.numpy as jnp
from jax import lax
from jax.experimental import pallas as pl
from jax.experimental.pallas import tpu as pltpu
from jax.sharding import PartitionSpec as P

HEAD_DIM = 128
EPS = 1e-5
ROPE_BASE = 5e5
SCALE_LOG2E = HEAD_DIM ** -0.5 * 1.4426950408889634
NEG = -1e30
BQ = 512
BK = 1024
WOP = 128
WOY = 3
MESH = pl.DeviceIdType.MESH
F32 = jnp.float32
BF16 = jnp.bfloat16


def _rms(x, g):
    x32 = x.astype(F32)
    r = lax.rsqrt(jnp.mean(x32 * x32, axis=-1, keepdims=True) + EPS)
    return (x32 * r * g).astype(BF16)


def _tables(pos):
    half = HEAD_DIM // 2
    inv = ROPE_BASE ** (-2.0 * jnp.arange(half, dtype=F32) / HEAD_DIM)
    ang = pos.astype(F32)[:, None] * inv
    c, s = jnp.cos(ang), jnp.sin(ang)
    return jnp.concatenate([c, c], axis=1), jnp.concatenate([-s, s], axis=1)


def _barrier(peers):
    sem = pltpu.get_barrier_semaphore()
    for p in peers:
        pl.semaphore_signal(sem, inc=1, device_id=p, device_id_type=MESH)
    pl.semaphore_wait(sem, len(peers))


def _sp_order(s):
    return [(s + 2) % 4, 3 - s, s + 1 - 2 * (s % 2), s]


def _wo_y(tp, s, rep, wo_hbm, wo_dst, ssem, rsem, k, nr):
    r0 = pl.multiple_of(s * (wo_hbm.shape[0] // 4) + k * nr, 128)
    return pltpu.make_async_remote_copy(src_ref=wo_hbm.at[pl.ds(r0, nr), :], dst_ref=wo_dst.at[pl.ds(r0, nr), :],
                                        send_sem=ssem, recv_sem=rsem, device_id=(rep, 1 - tp, s), device_id_type=MESH)


def _qkv_body(x_hbm, g_ref, cos_ref, sin_ref, wq_hbm, wk_hbm, wv_hbm, wo_hbm, q_hbm, k0_hbm, v0_hbm, k1_hbm, v1_hbm, wo_dst,
              xbuf, u, wq, wkv, qo, ko, vo, xsem, wsem, ssem, rsem, lsem, qsem, qrsem, wosem, worsem):
    rep, tp, s = lax.axis_index("rep"), lax.axis_index("tp"), lax.axis_index("sp")
    order = _sp_order(s)
    far, diag, mate = order[:3]
    on_x0 = s // 2 == 0
    m = u.shape[0]
    nb = xbuf.shape[0]
    rows = m // nb
    qw = qo.shape[2]

    def kvcopies(t):
        j, sl = order[t], t % 2
        return [
            pltpu.make_async_copy(wk_hbm.at[:, pl.ds(pl.multiple_of(j * 128, 128), 128)], wkv.at[sl, :, pl.ds(0, 128)], wsem.at[sl, 1]),
            pltpu.make_async_copy(wv_hbm.at[:, pl.ds(pl.multiple_of(j * 128, 128), 128)], wkv.at[sl, :, pl.ds(128, 128)], wsem.at[sl, 2]),
        ]

    groups = [mate, (mate + 2) % 4, s, far]

    def qcopy(t):
        return pltpu.make_async_copy(wq_hbm.at[:, pl.ds(pl.multiple_of(groups[t] * qw, 128), qw)], wq.at[t % 2], wsem.at[t % 2, 0])

    xc = [pltpu.make_async_copy(x_hbm.at[pl.ds(b * rows, rows), :], xbuf.at[b], xsem.at[b]) for b in range(nb)]
    xc[0].start()
    for c in kvcopies(0):
        c.start()
    for c in xc[1:]:
        c.start()
    for c in kvcopies(1):
        c.start()
    qcopy(0).start()
    qcopy(1).start()
    _barrier([(rep, tp, far), (rep, tp, diag), (rep, tp, mate), (rep, 1 - tp, s)])
    wo_sends = [_wo_y(tp, s, rep, wo_hbm, wo_dst, wosem.at[k], worsem.at[k], k, WOP) for k in range(WOY)]
    for c in wo_sends:
        c.start()
    for b in range(nb):
        xc[b].wait()

        @pl.loop(0, rows // 64)
        def _(i, b=b):
            xs = xbuf[b, pl.ds(pl.multiple_of(i * 64, 64), 64), :].astype(F32)
            r = lax.rsqrt(jnp.mean(xs * xs, axis=-1, keepdims=True) + EPS)
            u[pl.ds(pl.multiple_of(b * rows + i * 64, 64), 64), :] = (xs * r * g_ref[...]).astype(BF16)

    def rope(t, r0):
        c = cos_ref[pl.ds(r0, t.shape[0]), :]
        sn = sin_ref[pl.ds(r0, t.shape[0]), :]
        return t * c + pltpu.roll(t, 64, 1) * sn

    dst = pl.ds(pl.multiple_of(s * m, 128), m)

    def remote(t, sl, j):
        pair = ((ko, k0_hbm), (vo, v0_hbm)) if sl == 0 else ((ko, k1_hbm), (vo, v1_hbm))
        return [pltpu.make_async_remote_copy(src_ref=a.at[t], dst_ref=b.at[dst, :], send_sem=ssem.at[sl, t, i], recv_sem=rsem.at[sl, t, i],
                                             device_id=(rep, tp, j), device_id_type=MESH) for i, (a, b) in enumerate(pair)]

    def local(t, sl):
        pair = ((ko, k0_hbm), (vo, v0_hbm)) if sl == 0 else ((ko, k1_hbm), (vo, v1_hbm))
        return [pltpu.make_async_copy(a.at[t], b.at[dst, :], lsem.at[sl, i]) for i, (a, b) in enumerate(pair)]

    sends = [[(0, far, False)], [(0, diag, False), (1, mate, False)], [(0, mate, False), (1, diag, True)], [(1, far, True)]]
    for t in range(4):
        sl = t % 2
        for c in kvcopies(t):
            c.wait()

        @pl.loop(0, m // 256)
        def _(i, t=t, sl=sl):
            r0 = pl.multiple_of(i * 256, 256)
            kv = jnp.dot(u[pl.ds(r0, 256), :], wkv[sl], preferred_element_type=F32)
            ko[t, pl.ds(r0, 256), :] = rope(kv[:, :128], r0).astype(BF16)
            vo[t, pl.ds(r0, 256), :] = kv[:, 128:].astype(BF16)
        for slot, j, x0_only in sends[t]:
            def go(t=t, slot=slot, j=j):
                for c in remote(t, slot, j):
                    c.start()
            if x0_only:
                pl.when(on_x0)(go)
            else:
                go()
        if t == 0 or t == 3:
            for c in local(t, 1 if t == 0 else 0):
                c.start()
        if t < 2:
            for c in kvcopies(t + 2):
                c.start()

    qrow = pl.ds(pl.multiple_of(s % 2 * m, 128), m)

    def qremote(t):
        return pltpu.make_async_remote_copy(src_ref=qo.at[t], dst_ref=q_hbm.at[t % 2, qrow, :], send_sem=qsem.at[t], recv_sem=qrsem.at[t],
                                            device_id=(rep, tp, mate), device_id_type=MESH)

    def qlocal(t):
        return pltpu.make_async_copy(qo.at[t], q_hbm.at[t % 2, qrow, :], qsem.at[t])

    for t in range(4):
        qcopy(t).wait()

        @pl.loop(0, m // 256)
        def _(i, t=t):
            r0 = pl.multiple_of(i * 256, 256)
            qq = jnp.dot(u[pl.ds(r0, 256), :], wq[t % 2], preferred_element_type=F32)
            for n in range(qw // 128):
                qo[t, pl.ds(r0, 256), n * 128:(n + 1) * 128] = rope(qq[:, n * 128:(n + 1) * 128], r0).astype(BF16)
        (qremote(t) if t < 2 else qlocal(t)).start()
        if t < 2:
            qcopy(t + 2).start()

    for t in range(2):
        qremote(t).wait()
        qlocal(t + 2).wait()
    for c in local(0, 1) + local(3, 0):
        c.wait()
    for t in range(4):
        for slot, j, x0_only in sends[t]:
            cs = remote(t, slot, j)
            if x0_only:
                @pl.when(on_x0)
                def _(cs=cs):
                    for c in cs:
                        c.wait_send()

                @pl.when(jnp.logical_not(on_x0))
                def _(cs=cs):
                    for c in cs:
                        c.wait_recv()
            else:
                for c in cs:
                    c.wait()
    for c in wo_sends:
        c.wait()


def _qkv(x, g1, cos, sin, wq, wk, wv, wo, n):
    m, d = x.shape
    qw = wq.shape[1] // 4
    any_ = pl.BlockSpec(memory_space=pl.ANY)
    vm = pl.BlockSpec(memory_space=pltpu.VMEM)
    kv = jax.ShapeDtypeStruct((n, 128), BF16)
    return pl.pallas_call(
        _qkv_body,
        in_specs=[any_, vm, vm, vm, any_, any_, any_, any_],
        out_specs=[any_] * 6,
        out_shape=[jax.ShapeDtypeStruct((2, 2 * m, qw), BF16), kv, kv, kv, kv, jax.ShapeDtypeStruct(wo.shape, BF16)],
        scratch_shapes=[
            pltpu.VMEM((4, m // 4, d), BF16),
            pltpu.VMEM((m, d), BF16),
            pltpu.VMEM((2, d, qw), BF16),
            pltpu.VMEM((2, d, 256), BF16),
            pltpu.VMEM((4, m, qw), BF16),
            pltpu.VMEM((4, m, 128), BF16),
            pltpu.VMEM((4, m, 128), BF16),
            pltpu.SemaphoreType.DMA((4,)),
            pltpu.SemaphoreType.DMA((2, 3)),
            pltpu.SemaphoreType.DMA((2, 4, 2)),
            pltpu.SemaphoreType.DMA((2, 4, 2)),
            pltpu.SemaphoreType.DMA((2, 2)),
            pltpu.SemaphoreType.DMA((4,)),
            pltpu.SemaphoreType.DMA((2,)),
            pltpu.SemaphoreType.DMA((4,)),
            pltpu.SemaphoreType.DMA((4,)),
        ],
        compiler_params=pltpu.CompilerParams(collective_id=1, has_side_effects=True, vmem_limit_bytes=56 * 2**20),
        cost_estimate=pl.CostEstimate(flops=2 * m * d * (4 * qw + 1024), bytes_accessed=80 * 2**20, transcendentals=0),
        name="qkv_exchange",
    )(x, g1.reshape(1, -1), cos, sin, wq, wk, wv, wo)


def _attn_body(q_ref, k0_hbm, v0_hbm, k1_hbm, v1_hbm, wo_hbm, woi_hbm, own_hbm, oth_hbm, wo_dst,
               kb, vb, vt, acc, ms, ls, ob, kvsem, ssem, rsem0, rsem1, lsem, wsem, wrsem):
    rep, tp, s = lax.axis_index("rep"), lax.axis_index("tp"), lax.axis_index("sp")
    step = pl.program_id(0)
    order = _sp_order(s)
    far, diag, mate = order[:3]
    nh = q_ref.shape[2] // 128
    m = q_ref.shape[1] * 2
    xrow = s // 2 * (2 * m)
    qr = wo_hbm.shape[0] // 4
    grp, r = step % 2, step // 2
    nk = kb.shape[1]

    wo_y = [_wo_y(tp, s, rep, wo_hbm, wo_dst, wsem.at[0, k], wrsem.at[0, k], k, WOP) for k in range(WOY, 4)]

    def wo_piece(kind, k):
        quarter = far if kind == 3 else s
        r0 = pl.multiple_of(quarter * qr + k * WOP, 128)
        return pltpu.make_async_remote_copy(src_ref=wo_dst.at[pl.ds(r0, WOP), :], dst_ref=wo_dst.at[pl.ds(r0, WOP), :],
                                            send_sem=wsem.at[kind, k], recv_sem=wrsem.at[kind, k],
                                            device_id=(rep, tp, far if kind == 1 else mate), device_id_type=MESH)

    def kv_copies(g):
        return [pltpu.make_async_copy((k0_hbm, k1_hbm)[g], kb.at[g], kvsem.at[g, 0]),
                pltpu.make_async_copy((v0_hbm, v1_hbm)[g], vb.at[g], kvsem.at[g, 1])]

    @pl.when(step == 0)
    def _():
        for g in range(2):
            for c in kv_copies(g):
                c.start()
        _barrier([(rep, tp, far), (rep, tp, mate), (rep, 1 - tp, s), (rep, 1 - tp, mate)])
        for c in wo_y:
            c.start()
        for k in range(WOY):
            wo_piece(1, k).start()
            wo_piece(2, k).start()
        for g in range(2):
            for c in kv_copies(g):
                c.wait()

            @pl.loop(0, nk // 512)
            def _(j, g=g):
                r0 = pl.multiple_of(j * 512, 512)
                vt[g, :, pl.ds(r0, 512)] = vb[g, pl.ds(r0, 512), :].T

    ms[...] = jnp.full_like(ms, NEG)
    ls[...] = jnp.zeros_like(ls)
    acc[...] = jnp.zeros_like(acc)
    start = xrow + r * BQ

    def blk(k0, n, masked):
        k0 = pl.multiple_of(k0, BQ)
        kk_ = kb[grp, pl.ds(k0, n), :]
        vv_ = vt[grp, :, pl.ds(k0, n)]

        def scores(h):
            return lax.dot_general(kk_, q_ref[0, :, h * 128:(h + 1) * 128], (((1,), (1,)), ((), ())), preferred_element_type=F32)

        sc = scores(0)
        for h in range(nh):
            nxt = scores(h + 1) if h < nh - 1 else None
            if masked:
                kk = lax.broadcasted_iota(jnp.int32, (n, BQ), 0)
                qq = lax.broadcasted_iota(jnp.int32, (n, BQ), 1)
                sc = jnp.where(qq >= kk, sc, NEG)
            m0 = ms[h:h + 1, :]
            m1 = jnp.maximum(m0, jnp.max(sc, axis=0, keepdims=True))
            p = jnp.exp2(sc * SCALE_LOG2E - m1 * SCALE_LOG2E)
            a = jnp.exp2((m0 - m1) * SCALE_LOG2E)
            ms[h:h + 1, :] = m1
            ls[h:h + 1, :] = ls[h:h + 1, :] * a + jnp.sum(p, axis=0, keepdims=True)
            acc[h] = acc[h] * a + jnp.dot(vv_, p.astype(BF16), preferred_element_type=F32)
            sc = nxt

    @pl.loop(0, start // BK)
    def _(j):
        blk(j * BK, BK, False)

    @pl.when(start % BK != 0)
    def _():
        blk(start - BQ, BQ, False)

    blk(start, BQ, True)
    for h in range(nh):
        o = acc[h] * (1.0 / ls[h:h + 1, :])
        ob[step, :, h * 128:(h + 1) * 128] = o.T.astype(BF16)

    w = q_ref.shape[2]

    def dst(ref, slot, src_s, g):
        return ref.at[slot, :, pl.ds(pl.multiple_of((src_s + 2 * g) % 4 * w, 128), w)]

    def place(t):
        rr = t // 2
        return t % 2, s // 2 * 2 + rr // 2, rr % 2

    def to_own(t):
        g, d, half = place(t)
        slot = (half + tp + 1) % 2
        return pltpu.make_async_remote_copy(
            src_ref=ob.at[t], dst_ref=dst(own_hbm, slot, s, g), send_sem=ssem.at[0, t], recv_sem=rsem0.at[g, slot],
            device_id=(rep, tp, mate), device_id_type=MESH)

    def to_local(t):
        g, d, half = place(t)
        slot = (half + tp + 1) % 2
        return pltpu.make_async_copy(ob.at[t], dst(own_hbm, slot, s, g), lsem.at[g, half])

    def to_oth(t):
        g, d, half = place(t)
        slot = (half + tp) % 2
        return pltpu.make_async_remote_copy(
            src_ref=ob.at[t], dst_ref=dst(oth_hbm, slot, s, g), send_sem=ssem.at[1, t], recv_sem=rsem1.at[s % 2, g, slot],
            device_id=(rep, 1 - tp, d), device_id_type=MESH)

    to_oth(step).start()
    mine = place(step)[1] == s

    @pl.when(mine)
    def _():
        to_local(step).start()

    @pl.when(jnp.logical_not(mine))
    def _():
        to_own(step).start()

    @pl.when(step == 2)
    def _():
        for i, c in enumerate(wo_y):
            c.wait_recv()
            wo_piece(1, WOY + i).start()
            wo_piece(2, WOY + i).start()

    for k in range(3):
        @pl.when(step == 3 + k)
        def _(k=k):
            wo_piece(1, k).wait_recv()
            wo_piece(3, k).start()

    @pl.when(step == pl.num_programs(0) - 1)
    def _():
        wo_piece(1, 3).wait_recv()
        wo_piece(3, 3).start()

        @pl.loop(0, 8)
        def _(t):
            to_oth(t).wait_send()

            @pl.when(place(t)[1] == s)
            def _():
                to_local(t).wait()

            @pl.when(place(t)[1] != s)
            def _():
                to_own(t).wait_send()

        for g in range(2):
            for slot in range(2):
                pltpu.make_async_remote_copy(
                    src_ref=ob.at[0], dst_ref=dst(own_hbm, slot, mate, g), send_sem=ssem.at[0, 0], recv_sem=rsem0.at[g, slot],
                    device_id=(rep, tp, mate), device_id_type=MESH).wait_recv()
                for core in range(2):
                    src_s = s // 2 * 2 + core
                    pltpu.make_async_remote_copy(
                        src_ref=ob.at[0], dst_ref=dst(oth_hbm, slot, src_s, g), send_sem=ssem.at[1, 0], recv_sem=rsem1.at[core, g, slot],
                        device_id=(rep, 1 - tp, src_s), device_id_type=MESH).wait_recv()
        for c in wo_y:
            c.wait_send()
        for k in range(4):
            wo_piece(1, k).wait_send()
            wo_piece(2, k).wait()
            wo_piece(3, k).wait()


def _attention(q, k0, v0, k1, v1, wo, wo_oth):
    n = k0.shape[0]
    _, m2, w = q.shape
    nh = w // 128
    steps = 2 * m2 // BQ
    any_ = pl.BlockSpec(memory_space=pl.ANY)
    shape = jax.ShapeDtypeStruct((2, BQ, 4 * w), BF16)
    return pl.pallas_call(
        _attn_body,
        grid=(steps,),
        in_specs=[pl.BlockSpec((1, BQ, w), lambda t: (t % 2, t // 2, 0))] + [any_] * 6,
        out_specs=[any_] * 3,
        out_shape=[shape, shape, jax.ShapeDtypeStruct(wo.shape, BF16)],
        input_output_aliases={6: 2},
        scratch_shapes=[
            pltpu.VMEM((2, n, 128), BF16),
            pltpu.VMEM((2, n, 128), BF16),
            pltpu.VMEM((2, 128, n), BF16),
            pltpu.VMEM((nh, 128, BQ), F32),
            pltpu.VMEM((8, BQ), F32),
            pltpu.VMEM((8, BQ), F32),
            pltpu.VMEM((steps, BQ, w), BF16),
            pltpu.SemaphoreType.DMA((2, 2)),
            pltpu.SemaphoreType.DMA((2, 8)),
            pltpu.SemaphoreType.DMA((2, 2)),
            pltpu.SemaphoreType.DMA((2, 2, 2)),
            pltpu.SemaphoreType.DMA((2, 2)),
            pltpu.SemaphoreType.DMA((4, 4)),
            pltpu.SemaphoreType.DMA((4, 4)),
        ],
        compiler_params=pltpu.CompilerParams(collective_id=2, has_side_effects=True, vmem_limit_bytes=56 * 2**20),
        cost_estimate=pl.CostEstimate(flops=2 * n * n * w * 2, bytes_accessed=16 * 2**20, transcendentals=0),
        name="attention_exchange",
    )(q, k0, v0, k1, v1, wo, wo_oth)


NWO, NHID, NW2 = 8, 28, 16
UNITS = NWO + NHID + NW2
NBUF = 3
MB = 256


def _mlp_body(chunks, own_hbm, oth_hbm, x_hbm, wo_hbm, wo_oth_hbm, g_ref, w1_hbm, w3_hbm, w2_hbm, y_hbm,
              wb, abuf, xbuf, hid, pbuf, rbuf, ybuf, wsem, asem, ssem, rsem, ysem, yrsem, ylsem):
    rep, tp, s = lax.axis_index("rep"), lax.axis_index("tp"), lax.axis_index("sp")
    hr = wo_hbm.shape[0]
    hm = x_hbm.shape[0] // 2
    kh = w2_hbm.shape[0] // 2
    total = UNITS * len(chunks)
    partner = (rep, 1 - tp, s)

    def col(j, w):
        return pl.ds(pl.multiple_of(j * w, w), w)

    def wo_copies(j, sl):
        return [pltpu.make_async_copy(wo_hbm.at[:, col(j, 512)], wb.at[sl, pl.ds(0, hr), :], wsem.at[sl, 0]),
                pltpu.make_async_copy(wo_oth_hbm.at[:, col(j, 512)], wb.at[sl, pl.ds(hr, hr), :], wsem.at[sl, 1])]

    def hid_copies(j, sl):
        return [pltpu.make_async_copy(w1_hbm.at[:, col(j, 256)], wb.at[sl, :, pl.ds(0, 256)], wsem.at[sl, 0]),
                pltpu.make_async_copy(w3_hbm.at[:, col(j, 256)], wb.at[sl, :, pl.ds(256, 256)], wsem.at[sl, 1])]

    def w2_copies(t, sl):
        return [pltpu.make_async_copy(w2_hbm.at[pl.ds(pl.multiple_of(t % 2 * kh, 128), kh), col(t // 2, 512)], wb.at[sl, pl.ds(0, kh), :], wsem.at[sl, 0])]

    def issue(g):
        sl, u = g % NBUF, g % UNITS

        @pl.when(g < total)
        def _():
            @pl.when(u < NWO)
            def _():
                for c in wo_copies(u, sl):
                    c.start()

            @pl.when((u >= NWO) & (u < NWO + NHID))
            def _():
                for c in hid_copies(u - NWO, sl):
                    c.start()

            @pl.when(u >= NWO + NHID)
            def _():
                for c in w2_copies(u - NWO - NHID, sl):
                    c.start()

    def acts(c):
        slot, r0, nr = chunks[c]
        base = hm * ((tp + slot + 1) % 2) + r0
        rs = pl.ds(0, nr)
        return (pltpu.make_async_copy(x_hbm.at[pl.ds(pl.multiple_of(base, 128), nr), :], xbuf.at[rs, :], asem.at[0]),
                [pltpu.make_async_copy(own_hbm.at[slot, pl.ds(r0, nr), :], abuf.at[rs, pl.ds(0, hr)], asem.at[1]),
                 pltpu.make_async_copy(oth_hbm.at[slot, pl.ds(r0, nr), :], abuf.at[rs, pl.ds(hr, hr)], asem.at[2])])

    for g in range(NBUF - 1):
        issue(g)
    xc, ac = acts(0)
    xc.start()
    for c in ac:
        c.start()
    _barrier([partner])

    def send(ci, j):
        slot, r0, nr = chunks[ci]
        return pltpu.make_async_remote_copy(src_ref=pbuf.at[j, pl.ds(r0, nr), :], dst_ref=rbuf.at[j, pl.ds(r0, nr), :],
                                            send_sem=ssem.at[ci, j], recv_sem=rsem.at[ci, j], device_id=partner, device_id_type=MESH)

    yr0 = pl.multiple_of(tp * hm, 128)

    def ysend(j):
        return pltpu.make_async_remote_copy(src_ref=ybuf.at[j], dst_ref=y_hbm.at[pl.ds(yr0, hm), col(j, 512)],
                                            send_sem=ysem.at[j], recv_sem=yrsem.at[j], device_id=partner, device_id_type=MESH)

    def yrecv(j):
        return pltpu.make_async_remote_copy(src_ref=ybuf.at[j], dst_ref=y_hbm.at[pl.ds(pl.multiple_of((1 - tp) * hm, 128), hm), col(j, 512)],
                                            send_sem=ysem.at[j], recv_sem=yrsem.at[j], device_id=partner, device_id_type=MESH)

    def yown(j):
        return pltpu.make_async_copy(ybuf.at[j], y_hbm.at[pl.ds(yr0, hm), col(j, 512)], ylsem.at[j])

    nsend = len(chunks) - 1
    for ci, (slot, r0, nr) in enumerate(chunks):
        g0 = ci * UNITS
        xc, ac = acts(ci)
        xc.wait()
        for c in ac:
            c.wait()

        @pl.loop(0, NWO)
        def _(j, g0=g0, nr=nr):
            g = g0 + j
            sl = g % NBUF
            issue(g + NBUF - 1)
            for c in wo_copies(j, sl):
                c.wait()
            for b in range(nr // MB):
                rs = pl.ds(b * MB, MB)
                o = jnp.dot(abuf[rs, :], wb[sl], preferred_element_type=F32)
                xbuf[rs, col(j, 512)] = (xbuf[rs, col(j, 512)].astype(F32) + o).astype(BF16)

        @pl.loop(0, nr // 64)
        def _(i):
            rs = pl.ds(pl.multiple_of(i * 64, 64), 64)
            xs = xbuf[rs, :].astype(F32)
            r = lax.rsqrt(jnp.mean(xs * xs, axis=-1, keepdims=True) + EPS)
            abuf[rs, :] = (xs * r * g_ref[...]).astype(BF16)

        if ci + 1 < len(chunks):
            acts(ci + 1)[0].start()

        @pl.loop(0, NHID)
        def _(j, g0=g0, nr=nr):
            g = g0 + NWO + j
            sl = g % NBUF
            issue(g + NBUF - 1)
            for c in hid_copies(j, sl):
                c.wait()
            for b in range(nr // MB):
                rs = pl.ds(b * MB, MB)
                ab = jnp.dot(abuf[rs, :], wb[sl], preferred_element_type=F32)
                a = ab[:, :256]
                hid[rs, col(j, 256)] = (a / (1.0 + jnp.exp(-a)) * ab[:, 256:]).astype(BF16)

        if ci + 1 < len(chunks):
            for c in acts(ci + 1)[1]:
                c.start()

        @pl.loop(0, NW2 // 2)
        def _(j, g0=g0, ci=ci, slot=slot, r0=r0, nr=nr):
            g = g0 + NWO + NHID + 2 * j
            for h in range(2):
                sl = (g + h) % NBUF
                issue(g + h + NBUF - 1)
                for c in w2_copies(2 * j + h, sl):
                    c.wait()
                for b in range(nr // MB):
                    rs = pl.ds(b * MB, MB)
                    ps = pl.ds(r0 + b * MB, MB)
                    o = jnp.dot(hid[rs, h * kh:(h + 1) * kh], wb[sl, pl.ds(0, kh), :], preferred_element_type=F32)
                    if h == 0:
                        pbuf[j if slot == 0 else NW2 // 2, ps, :] = o
                    elif slot == 0:
                        pbuf[j, ps, :] = pbuf[j, ps, :] + o
                    else:
                        if b == 0:
                            for k in range(nsend):
                                send(k, j).wait_recv()
                        o = o + pbuf[NW2 // 2, ps, :] + rbuf[j, ps, :]
                        ybuf[j, ps, :] = (xbuf[rs, col(j, 512)].astype(F32) + o).astype(BF16)
            if slot == 0:
                send(ci, j).start()
            else:
                ysend(j).start()
                yown(j).start()

    @pl.loop(0, NW2 // 2)
    def _(j):
        for k in range(nsend):
            send(k, j).wait_send()
        ysend(j).wait_send()
        yown(j).wait()
        yrecv(j).wait_recv()


def _mlp(own, oth, x, wo, wo_oth, g2, w1, w3, w2):
    m, d = x.shape
    hm = m // 2
    chunks = ((0, 0, 256), (0, 256, 256), (1, 0, 512))
    any_ = pl.BlockSpec(memory_space=pl.ANY)
    vm = pl.BlockSpec(memory_space=pltpu.VMEM)
    nt = NW2 // 2
    return pl.pallas_call(
        functools.partial(_mlp_body, chunks),
        in_specs=[any_] * 5 + [vm] + [any_] * 3,
        out_specs=any_,
        out_shape=jax.ShapeDtypeStruct((m, d), BF16),
        scratch_shapes=[
            pltpu.VMEM((NBUF, d, 512), BF16),
            pltpu.VMEM((hm, d), BF16),
            pltpu.VMEM((hm, d), BF16),
            pltpu.VMEM((hm, w2.shape[0]), BF16),
            pltpu.VMEM((nt + 1, hm, 512), F32),
            pltpu.VMEM((nt, hm, 512), F32),
            pltpu.VMEM((nt, hm, 512), BF16),
            pltpu.SemaphoreType.DMA((NBUF, 2)),
            pltpu.SemaphoreType.DMA((3,)),
            pltpu.SemaphoreType.DMA((2, nt)),
            pltpu.SemaphoreType.DMA((2, nt)),
            pltpu.SemaphoreType.DMA((nt,)),
            pltpu.SemaphoreType.DMA((nt,)),
            pltpu.SemaphoreType.DMA((nt,)),
        ],
        compiler_params=pltpu.CompilerParams(collective_id=3, has_side_effects=True, vmem_limit_bytes=67043328),
        cost_estimate=pl.CostEstimate(flops=2 * m * d * (d + 3 * w1.shape[1]), bytes_accessed=640 * 2**20, transcendentals=0),
        name="mlp_sum",
    )(own, oth, x, wo, wo_oth, g2.reshape(1, -1), w1, w3, w2)


def solution(mesh):
    tok = P(("rep", "sp"), None)
    col = P(None, "tp")
    row = P("tp", None)
    cache = P("rep", ("tp", "sp"), None)

    def local(x, pos, g1, g2, wq, wk, wv, wo, w1, w3, w2):
        m, d = x.shape
        n = m * mesh.shape["sp"]
        cos, sin = _tables(pos)
        q, k, v, k1, v1, wo_oth = _qkv(x, g1, cos, sin, wq, wk, wv, wo, n)
        own, oth, wo_oth = _attention(q, k, v, k1, v1, wo, wo_oth)
        y = _mlp(own, oth, x, wo, wo_oth, g2, w1, w3, w2)
        return y, k.reshape(n, 1, 128), v.reshape(n, 1, 128)

    return jax.shard_map(
        local,
        mesh=mesh,
        in_specs=(tok, P(("rep", "sp")), P(), P(), col, col, col, row, col, col, row),
        out_specs=(tok, cache, cache),
        check_vma=False,
    )
```

```python
import functools

import jax
import jax.numpy as jnp
from jax import lax
from jax.experimental import pallas as pl
from jax.experimental.pallas import tpu as pltpu
from jax.sharding import PartitionSpec as P

HEAD_DIM = 128
EPS = 1e-5
ROPE_BASE = 5e5
SCALE_LOG2E = HEAD_DIM ** -0.5 * 1.4426950408889634
NEG = -1e30
BQ = 512
BK = 1024
WOP = 128
WOY = 2
MESH = pl.DeviceIdType.MESH
F32 = jnp.float32
BF16 = jnp.bfloat16


def _rms(x, g):
    x32 = x.astype(F32)
    r = lax.rsqrt(jnp.mean(x32 * x32, axis=-1, keepdims=True) + EPS)
    return (x32 * r * g).astype(BF16)


def _tables(pos):
    half = HEAD_DIM // 2
    inv = ROPE_BASE ** (-2.0 * jnp.arange(half, dtype=F32) / HEAD_DIM)
    ang = pos.astype(F32)[:, None] * inv
    c, s = jnp.cos(ang), jnp.sin(ang)
    return jnp.concatenate([c, c], axis=1), jnp.concatenate([-s, s], axis=1)


def _barrier(peers):
    sem = pltpu.get_barrier_semaphore()
    for p in peers:
        pl.semaphore_signal(sem, inc=1, device_id=p, device_id_type=MESH)
    pl.semaphore_wait(sem, len(peers))


def _sp_order(s):
    return [(s + 2) % 4, 3 - s, s + 1 - 2 * (s % 2), s]


def _wo_y(tp, s, rep, wo_hbm, wo_dst, ssem, rsem, k, nr):
    r0 = pl.multiple_of(s * (wo_hbm.shape[0] // 4) + k * nr, 128)
    return pltpu.make_async_remote_copy(src_ref=wo_hbm.at[pl.ds(r0, nr), :], dst_ref=wo_dst.at[pl.ds(r0, nr), :],
                                        send_sem=ssem, recv_sem=rsem, device_id=(rep, 1 - tp, s), device_id_type=MESH)


def _qkv_body(x_hbm, g_ref, cos_ref, sin_ref, wq_hbm, wk_hbm, wv_hbm, wo_hbm, q_hbm, k0_hbm, v0_hbm, k1_hbm, v1_hbm, wo_dst,
              xbuf, u, wq, wkv, qo, ko, vo, xsem, wsem, ssem, rsem, lsem, qsem, qrsem, wosem, worsem):
    rep, tp, s = lax.axis_index("rep"), lax.axis_index("tp"), lax.axis_index("sp")
    order = _sp_order(s)
    far, diag, mate = order[:3]
    on_x0 = s // 2 == 0
    m = u.shape[0]
    nb = xbuf.shape[0]
    rows = m // nb
    qw = qo.shape[2]

    def kvcopies(t):
        j, sl = order[t], t % 2
        return [
            pltpu.make_async_copy(wk_hbm.at[:, pl.ds(pl.multiple_of(j * 128, 128), 128)], wkv.at[sl, :, pl.ds(0, 128)], wsem.at[sl, 1]),
            pltpu.make_async_copy(wv_hbm.at[:, pl.ds(pl.multiple_of(j * 128, 128), 128)], wkv.at[sl, :, pl.ds(128, 128)], wsem.at[sl, 2]),
        ]

    groups = [mate, (mate + 2) % 4, s, far]

    def qcopy(t):
        return pltpu.make_async_copy(wq_hbm.at[:, pl.ds(pl.multiple_of(groups[t] * qw, 128), qw)], wq.at[t % 2], wsem.at[t % 2, 0])

    xc = [pltpu.make_async_copy(x_hbm.at[pl.ds(b * rows, rows), :], xbuf.at[b], xsem.at[b]) for b in range(nb)]
    xc[0].start()
    for c in kvcopies(0):
        c.start()
    for c in xc[1:]:
        c.start()
    for c in kvcopies(1):
        c.start()
    qcopy(0).start()
    qcopy(1).start()
    _barrier([(rep, tp, far), (rep, tp, diag), (rep, tp, mate), (rep, 1 - tp, s)])
    wo_sends = [_wo_y(tp, s, rep, wo_hbm, wo_dst, wosem.at[k], worsem.at[k], k, WOP) for k in range(WOY)]
    for c in wo_sends:
        c.start()
    for b in range(nb):
        xc[b].wait()

        @pl.loop(0, rows // 64)
        def _(i, b=b):
            xs = xbuf[b, pl.ds(pl.multiple_of(i * 64, 64), 64), :].astype(F32)
            r = lax.rsqrt(jnp.mean(xs * xs, axis=-1, keepdims=True) + EPS)
            u[pl.ds(pl.multiple_of(b * rows + i * 64, 64), 64), :] = (xs * r * g_ref[...]).astype(BF16)

    def rope(t, r0):
        c = cos_ref[pl.ds(r0, t.shape[0]), :]
        sn = sin_ref[pl.ds(r0, t.shape[0]), :]
        return t * c + pltpu.roll(t, 64, 1) * sn

    dst = pl.ds(pl.multiple_of(s * m, 128), m)

    def remote(t, sl, j):
        pair = ((ko, k0_hbm), (vo, v0_hbm)) if sl == 0 else ((ko, k1_hbm), (vo, v1_hbm))
        return [pltpu.make_async_remote_copy(src_ref=a.at[t], dst_ref=b.at[dst, :], send_sem=ssem.at[sl, t, i], recv_sem=rsem.at[sl, t, i],
                                             device_id=(rep, tp, j), device_id_type=MESH) for i, (a, b) in enumerate(pair)]

    def local(t, sl):
        pair = ((ko, k0_hbm), (vo, v0_hbm)) if sl == 0 else ((ko, k1_hbm), (vo, v1_hbm))
        return [pltpu.make_async_copy(a.at[t], b.at[dst, :], lsem.at[sl, i]) for i, (a, b) in enumerate(pair)]

    sends = [[(0, far, False)], [(0, diag, False), (1, mate, False)], [(0, mate, False), (1, diag, True)], [(1, far, True)]]
    for t in range(4):
        sl = t % 2
        for c in kvcopies(t):
            c.wait()

        @pl.loop(0, m // 256)
        def _(i, t=t, sl=sl):
            r0 = pl.multiple_of(i * 256, 256)
            kv = jnp.dot(u[pl.ds(r0, 256), :], wkv[sl], preferred_element_type=F32)
            ko[t, pl.ds(r0, 256), :] = rope(kv[:, :128], r0).astype(BF16)
            vo[t, pl.ds(r0, 256), :] = kv[:, 128:].astype(BF16)
        for slot, j, x0_only in sends[t]:
            def go(t=t, slot=slot, j=j):
                for c in remote(t, slot, j):
                    c.start()
            if x0_only:
                pl.when(on_x0)(go)
            else:
                go()
        if t == 0 or t == 3:
            for c in local(t, 1 if t == 0 else 0):
                c.start()
        if t < 2:
            for c in kvcopies(t + 2):
                c.start()

    hm = m // 2

    def qmove(t, h):
        src = qo.at[t, pl.ds(h * hm, hm), :]
        to = q_hbm.at[t % 2, pl.ds(pl.multiple_of(((h + tp) % 2 * 2 + s % 2) * hm, 128), hm), :]
        if t < 2:
            return pltpu.make_async_remote_copy(src_ref=src, dst_ref=to, send_sem=qsem.at[t, h], recv_sem=qrsem.at[t, h],
                                                device_id=(rep, tp, mate), device_id_type=MESH)
        return pltpu.make_async_copy(src, to, qsem.at[t, h])

    for t in range(4):
        qcopy(t).wait()

        @pl.loop(0, m // 256)
        def _(i, t=t):
            r0 = pl.multiple_of(i * 256, 256)
            qq = jnp.dot(u[pl.ds(r0, 256), :], wq[t % 2], preferred_element_type=F32)
            for n in range(qw // 128):
                qo[t, pl.ds(r0, 256), n * 128:(n + 1) * 128] = rope(qq[:, n * 128:(n + 1) * 128], r0).astype(BF16)
        for h in range(2):
            qmove(t, h).start()
        if t < 2:
            qcopy(t + 2).start()

    for t in range(4):
        for h in range(2):
            qmove(t, h).wait()
    for c in local(0, 1) + local(3, 0):
        c.wait()
    for t in range(4):
        for slot, j, x0_only in sends[t]:
            cs = remote(t, slot, j)
            if x0_only:
                @pl.when(on_x0)
                def _(cs=cs):
                    for c in cs:
                        c.wait_send()

                @pl.when(jnp.logical_not(on_x0))
                def _(cs=cs):
                    for c in cs:
                        c.wait_recv()
            else:
                for c in cs:
                    c.wait()
    for c in wo_sends:
        c.wait()


def _qkv(x, g1, cos, sin, wq, wk, wv, wo, n):
    m, d = x.shape
    qw = wq.shape[1] // 4
    any_ = pl.BlockSpec(memory_space=pl.ANY)
    vm = pl.BlockSpec(memory_space=pltpu.VMEM)
    kv = jax.ShapeDtypeStruct((n, 128), BF16)
    return pl.pallas_call(
        _qkv_body,
        in_specs=[any_, vm, vm, vm, any_, any_, any_, any_],
        out_specs=[any_] * 6,
        out_shape=[jax.ShapeDtypeStruct((2, 2 * m, qw), BF16), kv, kv, kv, kv, jax.ShapeDtypeStruct(wo.shape, BF16)],
        scratch_shapes=[
            pltpu.VMEM((4, m // 4, d), BF16),
            pltpu.VMEM((m, d), BF16),
            pltpu.VMEM((2, d, qw), BF16),
            pltpu.VMEM((2, d, 256), BF16),
            pltpu.VMEM((4, m, qw), BF16),
            pltpu.VMEM((4, m, 128), BF16),
            pltpu.VMEM((4, m, 128), BF16),
            pltpu.SemaphoreType.DMA((4,)),
            pltpu.SemaphoreType.DMA((2, 3)),
            pltpu.SemaphoreType.DMA((2, 4, 2)),
            pltpu.SemaphoreType.DMA((2, 4, 2)),
            pltpu.SemaphoreType.DMA((2, 2)),
            pltpu.SemaphoreType.DMA((4, 2)),
            pltpu.SemaphoreType.DMA((2, 2)),
            pltpu.SemaphoreType.DMA((4,)),
            pltpu.SemaphoreType.DMA((4,)),
        ],
        compiler_params=pltpu.CompilerParams(collective_id=1, has_side_effects=True, vmem_limit_bytes=56 * 2**20),
        cost_estimate=pl.CostEstimate(flops=2 * m * d * (4 * qw + 1024), bytes_accessed=80 * 2**20, transcendentals=0),
        name="qkv_exchange",
    )(x, g1.reshape(1, -1), cos, sin, wq, wk, wv, wo)


def _place(t, tp):
    i = t // 2
    return t % 2, i % 2, (tp + i // 2) % 2


def _attn_body(q_ref, k0_hbm, v0_hbm, k1_hbm, v1_hbm, wo_hbm, woi_hbm, own_hbm, oth_hbm, wo_dst, late_hbm,
               kb, vb, vt, acc, ms, ls, ob, kvsem, ssem, rsem0, rsem1, lsem, lasem, wsem, wrsem):
    rep, tp, s = lax.axis_index("rep"), lax.axis_index("tp"), lax.axis_index("sp")
    step = pl.program_id(0)
    order = _sp_order(s)
    far, diag, mate = order[:3]
    nh = q_ref.shape[2] // 128
    m = q_ref.shape[1] * 2
    xrow = s // 2 * (2 * m)
    qr = wo_hbm.shape[0] // 4
    grp, cc, half = _place(step, tp)
    r = 2 * cc + half
    nk = kb.shape[1]

    wo_y = [_wo_y(tp, s, rep, wo_hbm, wo_dst, wsem.at[0, k], wrsem.at[0, k], k, WOP) for k in range(WOY, 4)]

    def wo_piece(kind, k):
        quarter = far if kind == 3 else s
        r0 = pl.multiple_of(quarter * qr + k * WOP, 128)
        return pltpu.make_async_remote_copy(src_ref=wo_dst.at[pl.ds(r0, WOP), :], dst_ref=wo_dst.at[pl.ds(r0, WOP), :],
                                            send_sem=wsem.at[kind, k], recv_sem=wrsem.at[kind, k],
                                            device_id=(rep, tp, far if kind == 1 else mate), device_id_type=MESH)

    def kv_copies(g):
        return [pltpu.make_async_copy((k0_hbm, k1_hbm)[g], kb.at[g], kvsem.at[g, 0]),
                pltpu.make_async_copy((v0_hbm, v1_hbm)[g], vb.at[g], kvsem.at[g, 1])]

    @pl.when(step == 0)
    def _():
        for g in range(2):
            for c in kv_copies(g):
                c.start()
        _barrier([(rep, tp, far), (rep, tp, mate), (rep, 1 - tp, s), (rep, 1 - tp, mate)])
        for c in wo_y:
            c.start()
        for k in range(WOY):
            wo_piece(1, k).start()
            wo_piece(2, k).start()
        for g in range(2):
            for c in kv_copies(g):
                c.wait()

            @pl.loop(0, nk // 512)
            def _(j, g=g):
                r0 = pl.multiple_of(j * 512, 512)
                vt[g, :, pl.ds(r0, 512)] = vb[g, pl.ds(r0, 512), :].T

    ms[...] = jnp.full_like(ms, NEG)
    ls[...] = jnp.zeros_like(ls)
    acc[...] = jnp.zeros_like(acc)
    start = xrow + r * BQ

    def blk(k0, n, masked):
        k0 = pl.multiple_of(k0, BQ)
        kk_ = kb[grp, pl.ds(k0, n), :]
        vv_ = vt[grp, :, pl.ds(k0, n)]

        def scores(h):
            return lax.dot_general(kk_, q_ref[0, :, h * 128:(h + 1) * 128], (((1,), (1,)), ((), ())), preferred_element_type=F32)

        sc = scores(0)
        for h in range(nh):
            nxt = scores(h + 1) if h < nh - 1 else None
            if masked:
                kk = lax.broadcasted_iota(jnp.int32, (n, BQ), 0)
                qq = lax.broadcasted_iota(jnp.int32, (n, BQ), 1)
                sc = jnp.where(qq >= kk, sc, NEG)
            m0 = ms[h:h + 1, :]
            m1 = jnp.maximum(m0, jnp.max(sc, axis=0, keepdims=True))
            p = jnp.exp2(sc * SCALE_LOG2E - m1 * SCALE_LOG2E)
            a = jnp.exp2((m0 - m1) * SCALE_LOG2E)
            ms[h:h + 1, :] = m1
            ls[h:h + 1, :] = ls[h:h + 1, :] * a + jnp.sum(p, axis=0, keepdims=True)
            acc[h] = acc[h] * a + jnp.dot(vv_, p.astype(BF16), preferred_element_type=F32)
            sc = nxt

    @pl.loop(0, start // BK)
    def _(j):
        blk(j * BK, BK, False)

    @pl.when(start % BK != 0)
    def _():
        blk(start - BQ, BQ, False)

    blk(start, BQ, True)
    for h in range(nh):
        o = acc[h] * (1.0 / ls[h:h + 1, :])
        ob[step, :, h * 128:(h + 1) * 128] = o.T.astype(BF16)

    w = q_ref.shape[2]

    def cols(src_s, g):
        return pl.ds(pl.multiple_of((src_s + 2 * g) % 4 * w, 128), w)

    def dst(ref, slot, src_s, g):
        return ref.at[slot, :, cols(src_s, g)]

    def to_own(t):
        g, _, half = _place(t, tp)
        slot = (half + tp + 1) % 2
        return pltpu.make_async_remote_copy(
            src_ref=ob.at[t], dst_ref=dst(own_hbm, slot, s, g), send_sem=ssem.at[0, t], recv_sem=rsem0.at[g, slot],
            device_id=(rep, tp, mate), device_id_type=MESH)

    def to_local(t):
        g, _, half = _place(t, tp)
        slot = (half + tp + 1) % 2
        return pltpu.make_async_copy(ob.at[t], dst(own_hbm, slot, s, g), lsem.at[g, half])

    def to_oth(t):
        g, cc, _ = _place(t, tp)
        return pltpu.make_async_remote_copy(
            src_ref=ob.at[t], dst_ref=oth_hbm.at[:, cols(s, g)], send_sem=ssem.at[1, t], recv_sem=rsem1.at[s % 2, g],
            device_id=(rep, 1 - tp, s // 2 * 2 + cc), device_id_type=MESH)

    def to_late(t):
        g, cc, _ = _place(t, tp)
        return pltpu.make_async_copy(ob.at[t], late_hbm.at[g, cc], lasem.at[g, cc])

    @pl.when(step < 4)
    def _():
        to_oth(step).start()

    @pl.when(step >= 4)
    def _():
        to_late(step).start()

    def mine(t):
        return _place(t, tp)[1] == s % 2

    @pl.when(mine(step))
    def _():
        to_local(step).start()

    @pl.when(jnp.logical_not(mine(step)))
    def _():
        to_own(step).start()

    for k in range(WOY, 4):
        @pl.when(step == 2 * (k - WOY) + 2)
        def _(k=k):
            wo_y[k - WOY].wait_recv()
            wo_piece(1, k).start()
            wo_piece(2, k).start()

    for k in range(3):
        @pl.when(step == 2 * k + 2)
        def _(k=k):
            wo_piece(1, k).wait_recv()
            wo_piece(3, k).start()

    @pl.when(step == pl.num_programs(0) - 1)
    def _():
        wo_piece(1, 3).wait_recv()
        wo_piece(3, 3).start()

        @pl.loop(0, 4)
        def _(t):
            to_oth(t).wait_send()
            to_late(t + 4).wait()

        @pl.loop(0, 8)
        def _(t):
            @pl.when(mine(t))
            def _():
                to_local(t).wait()

            @pl.when(jnp.logical_not(mine(t)))
            def _():
                to_own(t).wait_send()

        for g in range(2):
            for slot in range(2):
                pltpu.make_async_remote_copy(
                    src_ref=ob.at[0], dst_ref=dst(own_hbm, slot, mate, g), send_sem=ssem.at[0, 0], recv_sem=rsem0.at[g, slot],
                    device_id=(rep, tp, mate), device_id_type=MESH).wait_recv()
            for core in range(2):
                src_s = s // 2 * 2 + core
                pltpu.make_async_remote_copy(
                    src_ref=ob.at[0], dst_ref=oth_hbm.at[:, cols(src_s, g)], send_sem=ssem.at[1, 0], recv_sem=rsem1.at[core, g],
                    device_id=(rep, 1 - tp, src_s), device_id_type=MESH).wait_recv()
        for c in wo_y:
            c.wait_send()
        for k in range(4):
            wo_piece(1, k).wait_send()
            wo_piece(2, k).wait()
            wo_piece(3, k).wait()


def _attention(q, k0, v0, k1, v1, wo, wo_oth):
    n = k0.shape[0]
    _, m2, w = q.shape
    nh = w // 128
    steps = 2 * m2 // BQ
    any_ = pl.BlockSpec(memory_space=pl.ANY)
    shape = jax.ShapeDtypeStruct((2, BQ, 4 * w), BF16)
    return pl.pallas_call(
        _attn_body,
        grid=(steps,),
        in_specs=[pl.BlockSpec((1, BQ, w), lambda t: (t % 2, t // 2, 0))] + [any_] * 6,
        out_specs=[any_] * 4,
        out_shape=[shape, jax.ShapeDtypeStruct((BQ, 4 * w), BF16), jax.ShapeDtypeStruct(wo.shape, BF16),
                   jax.ShapeDtypeStruct((2, 2, BQ, w), BF16)],
        input_output_aliases={6: 2},
        scratch_shapes=[
            pltpu.VMEM((2, n, 128), BF16),
            pltpu.VMEM((2, n, 128), BF16),
            pltpu.VMEM((2, 128, n), BF16),
            pltpu.VMEM((nh, 128, BQ), F32),
            pltpu.VMEM((8, BQ), F32),
            pltpu.VMEM((8, BQ), F32),
            pltpu.VMEM((steps, BQ, w), BF16),
            pltpu.SemaphoreType.DMA((2, 2)),
            pltpu.SemaphoreType.DMA((2, 8)),
            pltpu.SemaphoreType.DMA((2, 2)),
            pltpu.SemaphoreType.DMA((2, 2)),
            pltpu.SemaphoreType.DMA((2, 2)),
            pltpu.SemaphoreType.DMA((2, 2)),
            pltpu.SemaphoreType.DMA((4, 4)),
            pltpu.SemaphoreType.DMA((4, 4)),
        ],
        compiler_params=pltpu.CompilerParams(collective_id=2, has_side_effects=True, vmem_limit_bytes=56 * 2**20),
        cost_estimate=pl.CostEstimate(flops=2 * n * n * w * 2, bytes_accessed=16 * 2**20, transcendentals=0),
        name="attention_exchange",
    )(q, k0, v0, k1, v1, wo, wo_oth)


NWO, NHID, NW2 = 8, 28, 16
UNITS = NWO + NHID + NW2
NBUF = 3
MB = 256


def _mlp_body(chunks, own_hbm, oth_hbm, x_hbm, wo_hbm, wo_oth_hbm, g_ref, w1_hbm, w3_hbm, w2_hbm, late_hbm, y_hbm, olate_hbm,
              wb, abuf, xbuf, hid, pbuf, rbuf, ybuf, wsem, asem, ssem, rsem, ysem, yrsem, ylsem, lasem, larsem):
    rep, tp, s = lax.axis_index("rep"), lax.axis_index("tp"), lax.axis_index("sp")
    hr = wo_hbm.shape[0]
    hm = x_hbm.shape[0] // 2
    kh = w2_hbm.shape[0] // 2
    total = UNITS * len(chunks)
    partner = (rep, 1 - tp, s)

    def col(j, w):
        return pl.ds(pl.multiple_of(j * w, w), w)

    def wo_copies(j, sl):
        return [pltpu.make_async_copy(wo_hbm.at[:, col(j, 512)], wb.at[sl, pl.ds(0, hr), :], wsem.at[sl, 0]),
                pltpu.make_async_copy(wo_oth_hbm.at[:, col(j, 512)], wb.at[sl, pl.ds(hr, hr), :], wsem.at[sl, 1])]

    def hid_copies(j, sl):
        return [pltpu.make_async_copy(w1_hbm.at[:, col(j, 256)], wb.at[sl, :, pl.ds(0, 256)], wsem.at[sl, 0]),
                pltpu.make_async_copy(w3_hbm.at[:, col(j, 256)], wb.at[sl, :, pl.ds(256, 256)], wsem.at[sl, 1])]

    def w2_copies(t, sl):
        return [pltpu.make_async_copy(w2_hbm.at[pl.ds(pl.multiple_of(t % 2 * kh, 128), kh), col(t // 2, 512)], wb.at[sl, pl.ds(0, kh), :], wsem.at[sl, 0])]

    def issue(g):
        sl, u = g % NBUF, g % UNITS

        @pl.when(g < total)
        def _():
            @pl.when(u < NWO)
            def _():
                for c in wo_copies(u, sl):
                    c.start()

            @pl.when((u >= NWO) & (u < NWO + NHID))
            def _():
                for c in hid_copies(u - NWO, sl):
                    c.start()

            @pl.when(u >= NWO + NHID)
            def _():
                for c in w2_copies(u - NWO - NHID, sl):
                    c.start()

    def acts(c):
        slot, r0, nr = chunks[c]
        base = hm * ((tp + slot + 1) % 2) + r0
        rs = pl.ds(0, nr)
        return (pltpu.make_async_copy(x_hbm.at[pl.ds(pl.multiple_of(base, 128), nr), :], xbuf.at[rs, :], asem.at[0]),
                [pltpu.make_async_copy(own_hbm.at[slot, pl.ds(r0, nr), :], abuf.at[rs, pl.ds(0, hr)], asem.at[1]),
                 pltpu.make_async_copy((oth_hbm if slot == 0 else olate_hbm).at[pl.ds(r0, nr), :], abuf.at[rs, pl.ds(hr, hr)], asem.at[2])])

    for g in range(NBUF - 1):
        issue(g)
    xc, ac = acts(0)
    xc.start()
    for c in ac:
        c.start()
    mate = s + 1 - 2 * (s % 2)
    _barrier([partner, (rep, 1 - tp, mate)])
    w = late_hbm.shape[3]

    def late(g, cc, src_s):
        return pltpu.make_async_remote_copy(
            src_ref=late_hbm.at[g, cc], dst_ref=olate_hbm.at[:, pl.ds(pl.multiple_of((src_s + 2 * g) % 4 * w, 128), w)],
            send_sem=lasem.at[g, cc], recv_sem=larsem.at[g, src_s % 2],
            device_id=(rep, 1 - tp, s // 2 * 2 + cc), device_id_type=MESH)

    for g in range(2):
        for cc in range(2):
            late(g, cc, s).start()

    def send(ci, j):
        slot, r0, nr = chunks[ci]
        return pltpu.make_async_remote_copy(src_ref=pbuf.at[j, pl.ds(r0, nr), :], dst_ref=rbuf.at[j, pl.ds(r0, nr), :],
                                            send_sem=ssem.at[ci, j], recv_sem=rsem.at[ci, j], device_id=partner, device_id_type=MESH)

    yr0 = pl.multiple_of(tp * hm, 128)

    def ysend(j):
        return pltpu.make_async_remote_copy(src_ref=ybuf.at[j], dst_ref=y_hbm.at[pl.ds(yr0, hm), col(j, 512)],
                                            send_sem=ysem.at[j], recv_sem=yrsem.at[j], device_id=partner, device_id_type=MESH)

    def yrecv(j):
        return pltpu.make_async_remote_copy(src_ref=ybuf.at[j], dst_ref=y_hbm.at[pl.ds(pl.multiple_of((1 - tp) * hm, 128), hm), col(j, 512)],
                                            send_sem=ysem.at[j], recv_sem=yrsem.at[j], device_id=partner, device_id_type=MESH)

    def yown(j):
        return pltpu.make_async_copy(ybuf.at[j], y_hbm.at[pl.ds(yr0, hm), col(j, 512)], ylsem.at[j])

    nsend = len(chunks) - 1
    for ci, (slot, r0, nr) in enumerate(chunks):
        g0 = ci * UNITS
        xc, ac = acts(ci)
        xc.wait()
        for c in ac:
            c.wait()

        @pl.loop(0, NWO)
        def _(j, g0=g0, nr=nr):
            g = g0 + j
            sl = g % NBUF
            issue(g + NBUF - 1)
            for c in wo_copies(j, sl):
                c.wait()
            for b in range(nr // MB):
                rs = pl.ds(b * MB, MB)
                o = jnp.dot(abuf[rs, :], wb[sl], preferred_element_type=F32)
                xbuf[rs, col(j, 512)] = (xbuf[rs, col(j, 512)].astype(F32) + o).astype(BF16)

        @pl.loop(0, nr // 64)
        def _(i):
            rs = pl.ds(pl.multiple_of(i * 64, 64), 64)
            xs = xbuf[rs, :].astype(F32)
            r = lax.rsqrt(jnp.mean(xs * xs, axis=-1, keepdims=True) + EPS)
            abuf[rs, :] = (xs * r * g_ref[...]).astype(BF16)

        if ci + 1 < len(chunks):
            acts(ci + 1)[0].start()

        @pl.loop(0, NHID)
        def _(j, g0=g0, nr=nr):
            g = g0 + NWO + j
            sl = g % NBUF
            issue(g + NBUF - 1)
            for c in hid_copies(j, sl):
                c.wait()
            for b in range(nr // MB):
                rs = pl.ds(b * MB, MB)
                ab = jnp.dot(abuf[rs, :], wb[sl], preferred_element_type=F32)
                a = ab[:, :256]
                hid[rs, col(j, 256)] = (a / (1.0 + jnp.exp(-a)) * ab[:, 256:]).astype(BF16)

        if ci + 2 == len(chunks):
            for g in range(2):
                for core in range(2):
                    late(g, core, s // 2 * 2 + core).wait_recv()
        if ci + 1 < len(chunks):
            for c in acts(ci + 1)[1]:
                c.start()

        @pl.loop(0, NW2 // 2)
        def _(j, g0=g0, ci=ci, slot=slot, r0=r0, nr=nr):
            g = g0 + NWO + NHID + 2 * j
            for h in range(2):
                sl = (g + h) % NBUF
                issue(g + h + NBUF - 1)
                for c in w2_copies(2 * j + h, sl):
                    c.wait()
                for b in range(nr // MB):
                    rs = pl.ds(b * MB, MB)
                    ps = pl.ds(r0 + b * MB, MB)
                    o = jnp.dot(hid[rs, h * kh:(h + 1) * kh], wb[sl, pl.ds(0, kh), :], preferred_element_type=F32)
                    if h == 0:
                        pbuf[j if slot == 0 else NW2 // 2, ps, :] = o
                    elif slot == 0:
                        pbuf[j, ps, :] = pbuf[j, ps, :] + o
                    else:
                        if b == 0:
                            for k in range(nsend):
                                send(k, j).wait_recv()
                        o = o + pbuf[NW2 // 2, ps, :] + rbuf[j, ps, :]
                        ybuf[j, ps, :] = (xbuf[rs, col(j, 512)].astype(F32) + o).astype(BF16)
            if slot == 0:
                send(ci, j).start()
            else:
                ysend(j).start()
                yown(j).start()

    for g in range(2):
        for cc in range(2):
            late(g, cc, s).wait_send()

    @pl.loop(0, NW2 // 2)
    def _(j):
        for k in range(nsend):
            send(k, j).wait_send()
        ysend(j).wait_send()
        yown(j).wait()
        yrecv(j).wait_recv()


def _mlp(own, oth, late, x, wo, wo_oth, g2, w1, w3, w2):
    m, d = x.shape
    hm = m // 2
    chunks = ((0, 0, 256), (0, 256, 256), (1, 0, 512))
    any_ = pl.BlockSpec(memory_space=pl.ANY)
    vm = pl.BlockSpec(memory_space=pltpu.VMEM)
    nt = NW2 // 2
    return pl.pallas_call(
        functools.partial(_mlp_body, chunks),
        in_specs=[any_] * 5 + [vm] + [any_] * 4,
        out_specs=[any_, any_],
        out_shape=[jax.ShapeDtypeStruct((m, d), BF16), jax.ShapeDtypeStruct((hm, wo.shape[0]), BF16)],
        scratch_shapes=[
            pltpu.VMEM((NBUF, d, 512), BF16),
            pltpu.VMEM((hm, d), BF16),
            pltpu.VMEM((hm, d), BF16),
            pltpu.VMEM((hm, w2.shape[0]), BF16),
            pltpu.VMEM((nt + 1, hm, 512), F32),
            pltpu.VMEM((nt, hm, 512), F32),
            pltpu.VMEM((nt, hm, 512), BF16),
            pltpu.SemaphoreType.DMA((NBUF, 2)),
            pltpu.SemaphoreType.DMA((3,)),
            pltpu.SemaphoreType.DMA((2, nt)),
            pltpu.SemaphoreType.DMA((2, nt)),
            pltpu.SemaphoreType.DMA((nt,)),
            pltpu.SemaphoreType.DMA((nt,)),
            pltpu.SemaphoreType.DMA((nt,)),
            pltpu.SemaphoreType.DMA((2, 2)),
            pltpu.SemaphoreType.DMA((2, 2)),
        ],
        compiler_params=pltpu.CompilerParams(collective_id=3, has_side_effects=True, vmem_limit_bytes=67043328),
        cost_estimate=pl.CostEstimate(flops=2 * m * d * (d + 3 * w1.shape[1]), bytes_accessed=640 * 2**20, transcendentals=0),
        name="mlp_sum",
    )(own, oth, x, wo, wo_oth, g2.reshape(1, -1), w1, w3, w2, late)[0]


def solution(mesh):
    tok = P(("rep", "sp"), None)
    col = P(None, "tp")
    row = P("tp", None)
    cache = P("rep", ("tp", "sp"), None)

    def local(x, pos, g1, g2, wq, wk, wv, wo, w1, w3, w2):
        m, d = x.shape
        n = m * mesh.shape["sp"]
        cos, sin = _tables(pos)
        q, k, v, k1, v1, wo_oth = _qkv(x, g1, cos, sin, wq, wk, wv, wo, n)
        own, oth, wo_oth, late = _attention(q, k, v, k1, v1, wo, wo_oth)
        y = _mlp(own, oth, late, x, wo, wo_oth, g2, w1, w3, w2)
        return y, k.reshape(n, 1, 128), v.reshape(n, 1, 128)

    return jax.shard_map(
        local,
        mesh=mesh,
        in_specs=(tok, P(("rep", "sp")), P(), P(), col, col, col, row, col, col, row),
        out_specs=(tok, cache, cache),
        check_vma=False,
    )
```

```python
import functools

import jax
import jax.numpy as jnp
from jax import lax
from jax.experimental import pallas as pl
from jax.experimental.pallas import tpu as pltpu
from jax.sharding import PartitionSpec as P

HEAD_DIM = 128
EPS = 1e-5
ROPE_BASE = 5e5
SCALE_LOG2E = HEAD_DIM ** -0.5 * 1.4426950408889634
NEG = -1e30
BQ = 512
BK = 2048
Y1 = (0, 272)
Y2 = ((272, 128), (400, 112))
YX = (480, 32)
XP = ((0, 144), (144, 128), (272, 128), (400, 80))
LATE_ROWS = 128
MESH = pl.DeviceIdType.MESH
F32 = jnp.float32
BF16 = jnp.bfloat16


def _rms(x, g):
    x32 = x.astype(F32)
    r = lax.rsqrt(jnp.mean(x32 * x32, axis=-1, keepdims=True) + EPS)
    return (x32 * r * g).astype(BF16)


def _tables(pos):
    half = HEAD_DIM // 2
    lane = jnp.arange(HEAD_DIM)
    inv = ROPE_BASE ** (-2.0 * (lane % half).astype(F32) / HEAD_DIM)
    ang = pos.astype(F32)[:, None] * inv
    return jnp.cos(ang), jnp.where(lane < half, -1.0, 1.0) * jnp.sin(ang)


def _barrier(peers):
    sem = pltpu.get_barrier_semaphore()
    for p in peers:
        pl.semaphore_signal(sem, inc=1, device_id=p, device_id_type=MESH)
    pl.semaphore_wait(sem, len(peers))


def _sp_order(s):
    return [(s + 2) % 4, 3 - s, s + 1 - 2 * (s % 2), s]


def _wo_y(rep, tp, s, wo_hbm, wo_dst, quarter, piece, ssem, rsem):
    r0 = pl.multiple_of(quarter * (wo_hbm.shape[0] // 4) + piece[0], 16)
    return pltpu.make_async_remote_copy(src_ref=wo_hbm.at[pl.ds(r0, piece[1]), :], dst_ref=wo_dst.at[pl.ds(r0, piece[1]), :],
                                        send_sem=ssem, recv_sem=rsem, device_id=(rep, 1 - tp, s), device_id_type=MESH)


def _qkv_body(x_hbm, g_ref, cos_ref, sin_ref, wq_hbm, wk_hbm, wv_hbm, wo_hbm, q_hbm, k0_hbm, v0_hbm, k1_hbm, v1_hbm, wo_dst,
              xbuf, u, wq, wkv, qo, ko, vo, xsem, wsem, ssem, rsem, lsem, qsem, qrsem, wosem, worsem):
    rep, tp, s = lax.axis_index("rep"), lax.axis_index("tp"), lax.axis_index("sp")
    order = _sp_order(s)
    far, diag, mate = order[:3]
    on_x0 = s // 2 == 0
    m = u.shape[0]
    nb = xbuf.shape[0]
    rows = m // nb
    qw = qo.shape[2]

    def kvcopies(t):
        j, sl = order[t], t % 2
        return [
            pltpu.make_async_copy(wk_hbm.at[:, pl.ds(pl.multiple_of(j * 128, 128), 128)], wkv.at[sl, :, pl.ds(0, 128)], wsem.at[sl, 1]),
            pltpu.make_async_copy(wv_hbm.at[:, pl.ds(pl.multiple_of(j * 128, 128), 128)], wkv.at[sl, :, pl.ds(128, 128)], wsem.at[sl, 2]),
        ]

    groups = [mate, (mate + 2) % 4, s, far]

    def qcopy(t):
        return pltpu.make_async_copy(wq_hbm.at[:, pl.ds(pl.multiple_of(groups[t] * qw, 128), qw)], wq.at[t % 2], wsem.at[t % 2, 0])

    xc = [pltpu.make_async_copy(x_hbm.at[pl.ds(b * rows, rows), :], xbuf.at[b], xsem.at[b]) for b in range(nb)]
    xc[0].start()
    for c in kvcopies(0):
        c.start()
    for c in xc[1:]:
        c.start()
    for c in kvcopies(1):
        c.start()
    qcopy(0).start()
    qcopy(1).start()
    _barrier([(rep, tp, far), (rep, tp, diag), (rep, tp, mate), (rep, 1 - tp, s)])
    wo_send = _wo_y(rep, tp, s, wo_hbm, wo_dst, s, Y1, wosem.at[0], worsem.at[0])
    wo_send.start()
    def rope(t, r0):
        c = cos_ref[pl.ds(r0, t.shape[0]), :]
        sn = sin_ref[pl.ds(r0, t.shape[0]), :]
        return t * c + pltpu.roll(t, 64, 1) * sn

    hm = m // 2

    def kvpair(t, sl, h):
        pair = ((ko, k0_hbm), (vo, v0_hbm)) if sl == 0 else ((ko, k1_hbm), (vo, v1_hbm))
        dst = pl.ds(pl.multiple_of(s * m + h * hm, 128), hm)
        return [(a.at[t, pl.ds(h * hm, hm), :], b.at[dst, :]) for a, b in pair]

    def remote(t, sl, j, h):
        return [pltpu.make_async_remote_copy(src_ref=a, dst_ref=b, send_sem=ssem.at[sl, t, h, i], recv_sem=rsem.at[sl, t, h, i],
                                             device_id=(rep, tp, j), device_id_type=MESH) for i, (a, b) in enumerate(kvpair(t, sl, h))]

    def local(t, sl, h):
        return [pltpu.make_async_copy(a, b, lsem.at[sl, h, i]) for i, (a, b) in enumerate(kvpair(t, sl, h))]

    sends = [[(0, far, False)], [(0, diag, False), (1, mate, False)], [(0, mate, False), (1, diag, True)], [(1, far, True)]]
    def norm(b):
        xc[b].wait()

        @pl.loop(0, rows // 64)
        def _(i):
            xs = xbuf[b, pl.ds(pl.multiple_of(i * 64, 64), 64), :].astype(F32)
            r = lax.rsqrt(jnp.mean(xs * xs, axis=-1, keepdims=True) + EPS)
            u[pl.ds(pl.multiple_of(b * rows + i * 64, 64), 64), :] = (xs * r * g_ref[...]).astype(BF16)

    for t in range(4):
        sl = t % 2
        if t > 0:
            for c in kvcopies(t):
                c.wait()
        for h in range(2):
            if t == 0:
                norm(2 * h)
                norm(2 * h + 1)
                if h == 0:
                    for c in kvcopies(0):
                        c.wait()

            @pl.loop(h * 2, h * 2 + 2)
            def _(i, t=t, sl=sl):
                r0 = pl.multiple_of(i * 256, 256)
                kv = jnp.dot(u[pl.ds(r0, 256), :], wkv[sl], preferred_element_type=F32)
                ko[t, pl.ds(r0, 256), :] = rope(kv[:, :128], r0).astype(BF16)
                vo[t, pl.ds(r0, 256), :] = kv[:, 128:].astype(BF16)
            for slot, j, x0_only in sends[t]:
                def go(t=t, slot=slot, j=j, h=h):
                    for c in remote(t, slot, j, h):
                        c.start()
                if x0_only:
                    pl.when(on_x0)(go)
                else:
                    go()
            if t == 0 or t == 3:
                for c in local(t, 1 if t == 0 else 0, h):
                    c.start()
        if t < 2:
            for c in kvcopies(t + 2):
                c.start()

    def qmove(t, h):
        src = qo.at[t, pl.ds(h * hm, hm), :]
        to = q_hbm.at[t % 2, pl.ds(pl.multiple_of(((h + tp) % 2 * 2 + s % 2) * hm, 128), hm), :]
        if t < 2:
            return pltpu.make_async_remote_copy(src_ref=src, dst_ref=to, send_sem=qsem.at[t, h], recv_sem=qrsem.at[t, h],
                                                device_id=(rep, tp, mate), device_id_type=MESH)
        return pltpu.make_async_copy(src, to, qsem.at[t, h])

    for t in range(4):
        qcopy(t).wait()

        @pl.loop(0, m // 256)
        def _(i, t=t):
            r0 = pl.multiple_of(i * 256, 256)
            qq = jnp.dot(u[pl.ds(r0, 256), :], wq[t % 2], preferred_element_type=F32)
            for n in range(qw // 128):
                qo[t, pl.ds(r0, 256), n * 128:(n + 1) * 128] = rope(qq[:, n * 128:(n + 1) * 128], r0).astype(BF16)
        for h in range(2):
            qmove(t, h).start()
        if t < 2:
            qcopy(t + 2).start()

    for t in range(4):
        for h in range(2):
            qmove(t, h).wait()
    for h in range(2):
        for c in local(0, 1, h) + local(3, 0, h):
            c.wait()
        for t in range(4):
            for slot, j, x0_only in sends[t]:
                cs = remote(t, slot, j, h)
                if x0_only:
                    @pl.when(on_x0)
                    def _(cs=cs):
                        for c in cs:
                            c.wait_send()

                    @pl.when(jnp.logical_not(on_x0))
                    def _(cs=cs):
                        for c in cs:
                            c.wait_recv()
                else:
                    for c in cs:
                        c.wait()
    wo_send.wait()


def _qkv(x, g1, cos, sin, wq, wk, wv, wo, n):
    m, d = x.shape
    qw = wq.shape[1] // 4
    any_ = pl.BlockSpec(memory_space=pl.ANY)
    vm = pl.BlockSpec(memory_space=pltpu.VMEM)
    kv = jax.ShapeDtypeStruct((n, 128), BF16)
    return pl.pallas_call(
        _qkv_body,
        in_specs=[any_, vm, vm, vm, any_, any_, any_, any_],
        out_specs=[any_] * 6,
        out_shape=[jax.ShapeDtypeStruct((2, 2 * m, qw), BF16), kv, kv, kv, kv, jax.ShapeDtypeStruct(wo.shape, BF16)],
        scratch_shapes=[
            pltpu.VMEM((4, m // 4, d), BF16),
            pltpu.VMEM((m, d), BF16),
            pltpu.VMEM((2, d, qw), BF16),
            pltpu.VMEM((2, d, 256), BF16),
            pltpu.VMEM((4, m, qw), BF16),
            pltpu.VMEM((4, m, 128), BF16),
            pltpu.VMEM((4, m, 128), BF16),
            pltpu.SemaphoreType.DMA((4,)),
            pltpu.SemaphoreType.DMA((2, 3)),
            pltpu.SemaphoreType.DMA((2, 4, 2, 2)),
            pltpu.SemaphoreType.DMA((2, 4, 2, 2)),
            pltpu.SemaphoreType.DMA((2, 2, 2)),
            pltpu.SemaphoreType.DMA((4, 2)),
            pltpu.SemaphoreType.DMA((2, 2)),
            pltpu.SemaphoreType.DMA((1,)),
            pltpu.SemaphoreType.DMA((1,)),
        ],
        compiler_params=pltpu.CompilerParams(collective_id=1, has_side_effects=True, vmem_limit_bytes=56 * 2**20),
        cost_estimate=pl.CostEstimate(flops=2 * m * d * (4 * qw + 1024), bytes_accessed=80 * 2**20, transcendentals=0),
        name="qkv_exchange",
    )(x, g1.reshape(1, -1), cos, sin, wq, wk, wv, wo)


def _place(t, tp):
    i = t // 2
    return t % 2, i % 2, (tp + i // 2) % 2


def _attn_body(q_ref, k0_hbm, v0_hbm, k1_hbm, v1_hbm, wo_hbm, woi_hbm, own_hbm, oth_hbm, wo_dst, late_hbm, late2_hbm,
               kb, vb, vt, eye, acc, ms, ls, ob, kvsem, ssem, rsem0, rsem1, lsem, lasem, l2sem, wsem, wrsem):
    rep, tp, s = lax.axis_index("rep"), lax.axis_index("tp"), lax.axis_index("sp")
    step = pl.program_id(0)
    order = _sp_order(s)
    far, diag, mate = order[:3]
    nh = q_ref.shape[2] // 128
    m = q_ref.shape[1] * 2
    xrow = s // 2 * (2 * m)
    qr = wo_hbm.shape[0] // 4
    grp, cc, half = _place(step, tp)
    r = 2 * cc + half
    nk = kb.shape[1]

    wo_y = [_wo_y(rep, tp, s, wo_hbm, wo_dst, s, p, wsem.at[0, k], wrsem.at[0, k]) for k, p in enumerate(Y2)]
    wo_y.append(_wo_y(rep, tp, s, wo_hbm, wo_dst, far, YX, wsem.at[0, 2], wrsem.at[0, 2]))

    def wo_move(quarter, piece, peer, kind, k):
        r0 = pl.multiple_of(quarter * qr + piece[0], 16)
        return pltpu.make_async_remote_copy(src_ref=wo_dst.at[pl.ds(r0, piece[1]), :], dst_ref=wo_dst.at[pl.ds(r0, piece[1]), :],
                                            send_sem=wsem.at[kind, k], recv_sem=wrsem.at[kind, k],
                                            device_id=(rep, tp, peer), device_id_type=MESH)

    def wo_x(k):
        return wo_move(s, XP[k], far, 1, k)

    def wo_near(k):
        return wo_move(s, (Y1, *Y2)[k], mate, 2, k)

    def wo_near_far(k):
        return wo_move(far, (*XP, YX)[k], mate, 3, k)

    def kv_copies(g):
        return [pltpu.make_async_copy((k0_hbm, k1_hbm)[g], kb.at[g], kvsem.at[g, 0]),
                pltpu.make_async_copy((v0_hbm, v1_hbm)[g], vb.at[g], kvsem.at[g, 1])]

    @pl.when(step == 0)
    def _():
        for g in range(2):
            for c in kv_copies(g):
                c.start()
        _barrier([(rep, tp, far), (rep, tp, mate), (rep, 1 - tp, s), (rep, 1 - tp, mate)])
        for c in wo_y:
            c.start()
        wo_x(0).start()
        wo_x(1).start()
        wo_near(0).start()
        eye[...] = (lax.broadcasted_iota(jnp.int32, eye.shape, 0) == lax.broadcasted_iota(jnp.int32, eye.shape, 1)).astype(F32).astype(BF16)
        for g in range(2):
            for c in kv_copies(g):
                c.wait()

            @pl.loop(0, nk // 512)
            def _(j, g=g):
                r0 = pl.multiple_of(j * 512, 512)
                vt[g, :, pl.ds(r0, 512)] = lax.dot_general(
                    eye[:128, :128], vb[g, pl.ds(r0, 512), :], (((1,), (1,)), ((), ())), preferred_element_type=F32).astype(BF16)

    ms[...] = jnp.full_like(ms, NEG)
    ls[...] = jnp.zeros_like(ls)
    acc[...] = jnp.zeros_like(acc)
    start = xrow + r * BQ

    def blk(k0, n, masked):
        k0 = pl.multiple_of(k0, BQ)
        kk_ = kb[grp, pl.ds(k0, n), :]
        vv_ = vt[grp, :, pl.ds(k0, n)]

        def scores(h):
            return lax.dot_general(kk_, q_ref[0, :, h * 128:(h + 1) * 128], (((1,), (1,)), ((), ())), preferred_element_type=F32)

        sc = scores(0)
        for h in range(nh):
            nxt = scores(h + 1) if h < nh - 1 else None
            if masked:
                kk = lax.broadcasted_iota(jnp.int32, (n, BQ), 0)
                qq = lax.broadcasted_iota(jnp.int32, (n, BQ), 1)
                sc = jnp.where(qq >= kk, sc, NEG)
            m0 = ms[h:h + 1, :]
            m1 = jnp.maximum(m0, jnp.max(sc, axis=0, keepdims=True))
            p = jnp.exp2((sc - m1) * SCALE_LOG2E)
            a = jnp.exp2((m0 - m1) * SCALE_LOG2E)
            ms[h:h + 1, :] = m1
            ls[h:h + 1, :] = ls[h:h + 1, :] * a + jnp.sum(p, axis=0, keepdims=True)
            acc[h] = acc[h] * a + jnp.dot(vv_, p.astype(BF16), preferred_element_type=F32)
            sc = nxt

    @pl.loop(0, start // BK)
    def _(j):
        blk(j * BK, BK, False)

    @pl.when(start // 1024 % 2 == 1)
    def _():
        blk(start // BK * BK, 1024, False)

    @pl.when(start // BQ % 2 == 1)
    def _():
        blk(start - BQ, BQ, False)

    blk(start, BQ, True)
    for h in range(nh):
        o = acc[h] * (1.0 / ls[h:h + 1, :])
        ob[step, :, h * 128:(h + 1) * 128] = lax.dot_general(
            eye[...], o.astype(BF16), (((1,), (1,)), ((), ())), preferred_element_type=F32).astype(BF16)

    w = q_ref.shape[2]

    def cols(src_s, g):
        return pl.ds(pl.multiple_of((src_s + 2 * g) % 4 * w, 128), w)

    def dst(ref, slot, src_s, g):
        return ref.at[slot, :, cols(src_s, g)]

    def to_own(t):
        g, _, half = _place(t, tp)
        slot = (half + tp + 1) % 2
        return pltpu.make_async_remote_copy(
            src_ref=ob.at[t], dst_ref=dst(own_hbm, slot, s, g), send_sem=ssem.at[0, t], recv_sem=rsem0.at[g, slot],
            device_id=(rep, tp, mate), device_id_type=MESH)

    def to_local(t):
        g, _, half = _place(t, tp)
        slot = (half + tp + 1) % 2
        return pltpu.make_async_copy(ob.at[t], dst(own_hbm, slot, s, g), lsem.at[g, half])

    def first_rows(g):
        return BQ if g == 0 else BQ - LATE_ROWS

    def to_oth(t, g):
        cc, nr = _place(t, tp)[1], first_rows(g)
        return pltpu.make_async_remote_copy(
            src_ref=ob.at[t, pl.ds(0, nr), :], dst_ref=oth_hbm.at[pl.ds(0, nr), cols(s, g)],
            send_sem=ssem.at[1, t], recv_sem=rsem1.at[s % 2, g],
            device_id=(rep, 1 - tp, s // 2 * 2 + cc), device_id_type=MESH)

    def to_late2(t):
        cc = _place(t, tp)[1]
        return pltpu.make_async_copy(ob.at[t, pl.ds(BQ - LATE_ROWS, LATE_ROWS), :], late2_hbm.at[cc], l2sem.at[cc])

    def to_late(t):
        g, cc, _ = _place(t, tp)
        return pltpu.make_async_copy(ob.at[t], late_hbm.at[g, cc], lasem.at[g, cc])

    @pl.when((step < 4) & (grp == 0))
    def _():
        to_oth(step, 0).start()

    @pl.when((step < 4) & (grp == 1))
    def _():
        to_oth(step, 1).start()
        to_late2(step).start()

    @pl.when(step >= 4)
    def _():
        to_late(step).start()

    def mine(t):
        return _place(t, tp)[1] == s % 2

    @pl.when(mine(step))
    def _():
        to_local(step).start()

    @pl.when(jnp.logical_not(mine(step)))
    def _():
        to_own(step).start()

    @pl.when(step == 2)
    def _():
        wo_y[0].wait_recv()
        wo_x(2).start()
        wo_near(1).start()
        wo_x(0).wait_recv()
        wo_near_far(0).start()

    @pl.when(step == 4)
    def _():
        wo_y[1].wait_recv()
        wo_x(3).start()
        wo_near(2).start()
        wo_y[2].wait_recv()
        wo_near_far(4).start()

    for k in (1, 2):
        @pl.when(step == 4 + k)
        def _(k=k):
            wo_x(k).wait_recv()
            wo_near_far(k).start()

    @pl.when(step == pl.num_programs(0) - 1)
    def _():
        wo_x(3).wait_recv()
        wo_near_far(3).start()

        for t in range(4):
            to_oth(t, t % 2).wait_send()
            to_late(t + 4).wait()
        to_late2(1).wait()
        to_late2(3).wait()

        @pl.loop(0, 8)
        def _(t):
            @pl.when(mine(t))
            def _():
                to_local(t).wait()

            @pl.when(jnp.logical_not(mine(t)))
            def _():
                to_own(t).wait_send()

        for g in range(2):
            for slot in range(2):
                pltpu.make_async_remote_copy(
                    src_ref=ob.at[0], dst_ref=dst(own_hbm, slot, mate, g), send_sem=ssem.at[0, 0], recv_sem=rsem0.at[g, slot],
                    device_id=(rep, tp, mate), device_id_type=MESH).wait_recv()
            for core in range(2):
                src_s = s // 2 * 2 + core
                pltpu.make_async_remote_copy(
                    src_ref=ob.at[0, pl.ds(0, first_rows(g)), :], dst_ref=oth_hbm.at[pl.ds(0, first_rows(g)), cols(src_s, g)],
                    send_sem=ssem.at[1, 0], recv_sem=rsem1.at[core, g],
                    device_id=(rep, 1 - tp, src_s), device_id_type=MESH).wait_recv()
        for c in wo_y:
            c.wait_send()
        for k in range(4):
            wo_x(k).wait_send()
        for k in range(3):
            wo_near(k).wait()
        for k in range(5):
            wo_near_far(k).wait()


def _attention(q, k0, v0, k1, v1, wo, wo_oth):
    n = k0.shape[0]
    _, m2, w = q.shape
    nh = w // 128
    steps = 2 * m2 // BQ
    any_ = pl.BlockSpec(memory_space=pl.ANY)
    shape = jax.ShapeDtypeStruct((2, BQ, 4 * w), BF16)
    return pl.pallas_call(
        _attn_body,
        grid=(steps,),
        in_specs=[pl.BlockSpec((1, BQ, w), lambda t: (t % 2, t // 2, 0))] + [any_] * 6,
        out_specs=[any_] * 5,
        out_shape=[shape, jax.ShapeDtypeStruct((BQ, 4 * w), BF16), jax.ShapeDtypeStruct(wo.shape, BF16),
                   jax.ShapeDtypeStruct((2, 2, BQ, w), BF16), jax.ShapeDtypeStruct((2, LATE_ROWS, w), BF16)],
        input_output_aliases={6: 2},
        scratch_shapes=[
            pltpu.VMEM((2, n, 128), BF16),
            pltpu.VMEM((2, n, 128), BF16),
            pltpu.VMEM((2, 128, n), BF16),
            pltpu.VMEM((BQ, BQ), BF16),
            pltpu.VMEM((nh, 128, BQ), F32),
            pltpu.VMEM((8, BQ), F32),
            pltpu.VMEM((8, BQ), F32),
            pltpu.VMEM((steps, BQ, w), BF16),
            pltpu.SemaphoreType.DMA((2, 2)),
            pltpu.SemaphoreType.DMA((2, 8)),
            pltpu.SemaphoreType.DMA((2, 2)),
            pltpu.SemaphoreType.DMA((2, 2)),
            pltpu.SemaphoreType.DMA((2, 2)),
            pltpu.SemaphoreType.DMA((2, 2)),
            pltpu.SemaphoreType.DMA((2,)),
            pltpu.SemaphoreType.DMA((4, 5)),
            pltpu.SemaphoreType.DMA((4, 5)),
        ],
        compiler_params=pltpu.CompilerParams(collective_id=2, has_side_effects=True, vmem_limit_bytes=56 * 2**20),
        cost_estimate=pl.CostEstimate(flops=2 * n * n * w * 2, bytes_accessed=16 * 2**20, transcendentals=0),
        name="attention_exchange",
    )(q, k0, v0, k1, v1, wo, wo_oth)


NWO, NHID, NW2 = 8, 28, 16
UNITS = NWO + NHID + NW2
NBUF = 3
MB = 256


def _mlp_body(chunks, own_hbm, oth_hbm, x_hbm, wo_hbm, wo_oth_hbm, g_ref, w1_hbm, w3_hbm, w2_hbm, late_hbm, late2_hbm, y_hbm, olate_hbm, olate2_hbm,
              wb, abuf, xbuf, hid, pbuf, rbuf, ybuf, wsem, asem, ssem, rsem, ysem, yrsem, ylsem, lasem, larsem, l2sem, l2rsem):
    rep, tp, s = lax.axis_index("rep"), lax.axis_index("tp"), lax.axis_index("sp")
    hr = wo_hbm.shape[0]
    hm = x_hbm.shape[0] // 2
    kh = w2_hbm.shape[0] // 2
    total = UNITS * len(chunks)
    partner = (rep, 1 - tp, s)

    def col(j, w):
        return pl.ds(pl.multiple_of(j * w, w), w)

    def wo_copies(j, sl):
        return [pltpu.make_async_copy(wo_hbm.at[:, col(j, 512)], wb.at[sl, pl.ds(0, hr), :], wsem.at[sl, 0]),
                pltpu.make_async_copy(wo_oth_hbm.at[:, col(j, 512)], wb.at[sl, pl.ds(hr, hr), :], wsem.at[sl, 1])]

    def hid_copies(j, sl):
        return [pltpu.make_async_copy(w1_hbm.at[:, col(j, 256)], wb.at[sl, :, pl.ds(0, 256)], wsem.at[sl, 0]),
                pltpu.make_async_copy(w3_hbm.at[:, col(j, 256)], wb.at[sl, :, pl.ds(256, 256)], wsem.at[sl, 1])]

    def w2_copies(t, sl):
        return [pltpu.make_async_copy(w2_hbm.at[pl.ds(pl.multiple_of(t % 2 * kh, 128), kh), col(t // 2, 512)], wb.at[sl, pl.ds(0, kh), :], wsem.at[sl, 0])]

    def issue(g):
        sl, u = g % NBUF, g % UNITS

        @pl.when(g < total)
        def _():
            @pl.when(u < NWO)
            def _():
                for c in wo_copies(u, sl):
                    c.start()

            @pl.when((u >= NWO) & (u < NWO + NHID))
            def _():
                for c in hid_copies(u - NWO, sl):
                    c.start()

            @pl.when(u >= NWO + NHID)
            def _():
                for c in w2_copies(u - NWO - NHID, sl):
                    c.start()

    def acts(c):
        slot, r0, nr = chunks[c]
        base = hm * ((tp + slot + 1) % 2) + r0
        rs = pl.ds(0, nr)
        xcopy = pltpu.make_async_copy(x_hbm.at[pl.ds(pl.multiple_of(base, 128), nr), :], xbuf.at[rs, :], asem.at[0])
        cs = [pltpu.make_async_copy(own_hbm.at[slot, pl.ds(r0, nr), :], abuf.at[rs, pl.ds(0, hr)], asem.at[1])]
        late_at = hm - LATE_ROWS
        if slot == 1:
            cs.append(pltpu.make_async_copy(olate_hbm.at[pl.ds(r0, nr), :], abuf.at[rs, pl.ds(hr, hr)], asem.at[2]))
        elif r0 + nr <= late_at:
            cs.append(pltpu.make_async_copy(oth_hbm.at[pl.ds(r0, nr), :], abuf.at[rs, pl.ds(hr, hr)], asem.at[2]))
        else:
            n0 = late_at - r0
            c0 = pl.multiple_of(s // 2 * (hr // 2), 128)
            c1 = pl.multiple_of((1 - s // 2) * (hr // 2), 128)
            ls = pl.ds(n0, LATE_ROWS)
            cs.append(pltpu.make_async_copy(oth_hbm.at[pl.ds(r0, n0), :], abuf.at[pl.ds(0, n0), pl.ds(hr, hr)], asem.at[2]))
            cs.append(pltpu.make_async_copy(oth_hbm.at[pl.ds(late_at, LATE_ROWS), pl.ds(c0, hr // 2)], abuf.at[ls, pl.ds(hr + c0, hr // 2)], asem.at[3]))
            cs.append(pltpu.make_async_copy(olate2_hbm, abuf.at[ls, pl.ds(hr + c1, hr // 2)], asem.at[4]))
        return xcopy, cs

    for g in range(NBUF - 1):
        issue(g)
    xc, ac = acts(0)
    xc.start()
    for c in ac:
        c.start()
    mate = s + 1 - 2 * (s % 2)
    _barrier([partner, (rep, 1 - tp, mate)])
    w = late_hbm.shape[3]

    def late(g, cc, src_s):
        return pltpu.make_async_remote_copy(
            src_ref=late_hbm.at[g, cc], dst_ref=olate_hbm.at[:, pl.ds(pl.multiple_of((src_s + 2 * g) % 4 * w, 128), w)],
            send_sem=lasem.at[g, cc], recv_sem=larsem.at[g, src_s % 2],
            device_id=(rep, 1 - tp, s // 2 * 2 + cc), device_id_type=MESH)

    def late2(cc, src_s):
        return pltpu.make_async_remote_copy(
            src_ref=late2_hbm.at[cc], dst_ref=olate2_hbm.at[:, pl.ds(pl.multiple_of(src_s % 2 * w, 128), w)],
            send_sem=l2sem.at[cc], recv_sem=l2rsem.at[src_s % 2],
            device_id=(rep, 1 - tp, s // 2 * 2 + cc), device_id_type=MESH)

    for cc in range(2):
        late2(cc, s).start()
    for g in range(2):
        for cc in range(2):
            late(g, cc, s).start()

    def send(ci, j):
        slot, r0, nr = chunks[ci]
        return pltpu.make_async_remote_copy(src_ref=pbuf.at[j, pl.ds(r0, nr), :], dst_ref=rbuf.at[j, pl.ds(r0, nr), :],
                                            send_sem=ssem.at[ci, j], recv_sem=rsem.at[ci, j], device_id=partner, device_id_type=MESH)

    yr0 = pl.multiple_of(tp * hm, 128)

    def ysend(j):
        return pltpu.make_async_remote_copy(src_ref=ybuf.at[j], dst_ref=y_hbm.at[pl.ds(yr0, hm), col(j, 512)],
                                            send_sem=ysem.at[j], recv_sem=yrsem.at[j], device_id=partner, device_id_type=MESH)

    def yrecv(j):
        return pltpu.make_async_remote_copy(src_ref=ybuf.at[j], dst_ref=y_hbm.at[pl.ds(pl.multiple_of((1 - tp) * hm, 128), hm), col(j, 512)],
                                            send_sem=ysem.at[j], recv_sem=yrsem.at[j], device_id=partner, device_id_type=MESH)

    def yown(j):
        return pltpu.make_async_copy(ybuf.at[j], y_hbm.at[pl.ds(yr0, hm), col(j, 512)], ylsem.at[j])

    nsend = len(chunks) - 1
    for ci, (slot, r0, nr) in enumerate(chunks):
        g0 = ci * UNITS
        xc, ac = acts(ci)
        xc.wait()
        for c in ac:
            c.wait()

        @pl.loop(0, NWO)
        def _(j, g0=g0, nr=nr):
            g = g0 + j
            sl = g % NBUF
            issue(g + NBUF - 1)
            for c in wo_copies(j, sl):
                c.wait()
            for b in range(nr // MB):
                rs = pl.ds(b * MB, MB)
                o = jnp.dot(abuf[rs, :], wb[sl], preferred_element_type=F32)
                xbuf[rs, col(j, 512)] = (xbuf[rs, col(j, 512)].astype(F32) + o).astype(BF16)

        @pl.loop(0, nr // 64)
        def _(i):
            rs = pl.ds(pl.multiple_of(i * 64, 64), 64)
            xs = xbuf[rs, :].astype(F32)
            r = lax.rsqrt(jnp.mean(xs * xs, axis=-1, keepdims=True) + EPS)
            abuf[rs, :] = (xs * r * g_ref[...]).astype(BF16)

        if ci + 1 < len(chunks):
            acts(ci + 1)[0].start()

        @pl.loop(0, NHID)
        def _(j, g0=g0, nr=nr):
            g = g0 + NWO + j
            sl = g % NBUF
            issue(g + NBUF - 1)
            for c in hid_copies(j, sl):
                c.wait()
            for b in range(nr // MB):
                rs = pl.ds(b * MB, MB)
                ab = jnp.dot(abuf[rs, :], wb[sl], preferred_element_type=F32)
                a = ab[:, :256]
                hid[rs, col(j, 256)] = (a / (1.0 + jnp.exp(-a)) * ab[:, 256:]).astype(BF16)

        if ci + 3 == len(chunks):
            for core in range(2):
                late2(core, s // 2 * 2 + core).wait_recv()
        if ci + 2 == len(chunks):
            for g in range(2):
                for core in range(2):
                    late(g, core, s // 2 * 2 + core).wait_recv()
        if ci + 1 < len(chunks):
            for c in acts(ci + 1)[1]:
                c.start()

        @pl.loop(0, NW2 // 2)
        def _(j, g0=g0, ci=ci, slot=slot, r0=r0, nr=nr):
            g = g0 + NWO + NHID + 2 * j
            for h in range(2):
                sl = (g + h) % NBUF
                issue(g + h + NBUF - 1)
                for c in w2_copies(2 * j + h, sl):
                    c.wait()
                for b in range(nr // MB):
                    rs = pl.ds(b * MB, MB)
                    ps = pl.ds(r0 + b * MB, MB)
                    o = jnp.dot(hid[rs, h * kh:(h + 1) * kh], wb[sl, pl.ds(0, kh), :], preferred_element_type=F32)
                    if h == 0:
                        pbuf[j if slot == 0 else NW2 // 2, ps, :] = o
                    elif slot == 0:
                        pbuf[j, ps, :] = pbuf[j, ps, :] + o
                    else:
                        if b == 0:
                            for k in range(nsend):
                                send(k, j).wait_recv()
                        o = o + pbuf[NW2 // 2, ps, :] + rbuf[j, ps, :]
                        ybuf[j, ps, :] = (xbuf[rs, col(j, 512)].astype(F32) + o).astype(BF16)
            if slot == 0:
                send(ci, j).start()
            else:
                ysend(j).start()
                yown(j).start()

    for cc in range(2):
        late2(cc, s).wait_send()
        for g in range(2):
            late(g, cc, s).wait_send()

    @pl.loop(0, NW2 // 2)
    def _(j):
        for k in range(nsend):
            send(k, j).wait_send()
        ysend(j).wait_send()
        yown(j).wait()
        yrecv(j).wait_recv()


def _mlp(own, oth, late, late2, x, wo, wo_oth, g2, w1, w3, w2):
    m, d = x.shape
    hm = m // 2
    chunks = ((0, 0, 256), (0, 256, 256), (1, 0, 512))
    any_ = pl.BlockSpec(memory_space=pl.ANY)
    vm = pl.BlockSpec(memory_space=pltpu.VMEM)
    nt = NW2 // 2
    return pl.pallas_call(
        functools.partial(_mlp_body, chunks),
        in_specs=[any_] * 5 + [vm] + [any_] * 5,
        out_specs=[any_] * 3,
        out_shape=[jax.ShapeDtypeStruct((m, d), BF16), jax.ShapeDtypeStruct((hm, wo.shape[0]), BF16),
                   jax.ShapeDtypeStruct((LATE_ROWS, wo.shape[0] // 2), BF16)],
        scratch_shapes=[
            pltpu.VMEM((NBUF, d, 512), BF16),
            pltpu.VMEM((hm, d), BF16),
            pltpu.VMEM((hm, d), BF16),
            pltpu.VMEM((hm, w2.shape[0]), BF16),
            pltpu.VMEM((nt + 1, hm, 512), F32),
            pltpu.VMEM((nt, hm, 512), F32),
            pltpu.VMEM((nt, hm, 512), BF16),
            pltpu.SemaphoreType.DMA((NBUF, 2)),
            pltpu.SemaphoreType.DMA((5,)),
            pltpu.SemaphoreType.DMA((2, nt)),
            pltpu.SemaphoreType.DMA((2, nt)),
            pltpu.SemaphoreType.DMA((nt,)),
            pltpu.SemaphoreType.DMA((nt,)),
            pltpu.SemaphoreType.DMA((nt,)),
            pltpu.SemaphoreType.DMA((2, 2)),
            pltpu.SemaphoreType.DMA((2, 2)),
            pltpu.SemaphoreType.DMA((2,)),
            pltpu.SemaphoreType.DMA((2,)),
        ],
        compiler_params=pltpu.CompilerParams(collective_id=3, has_side_effects=True, vmem_limit_bytes=67043328),
        cost_estimate=pl.CostEstimate(flops=2 * m * d * (d + 3 * w1.shape[1]), bytes_accessed=640 * 2**20, transcendentals=0),
        name="mlp_sum",
    )(own, oth, x, wo, wo_oth, g2.reshape(1, -1), w1, w3, w2, late, late2)[0]


def _copy_body(y_ref, k_ref, v_ref, yo_ref, ko_ref, vo_ref, buf, kbuf, sem):
    n, nr = buf.shape[:2]
    moves = [(y_ref.at[pl.ds(i * nr, nr), :], yo_ref.at[pl.ds(i * nr, nr), :], buf.at[i]) for i in range(n)]
    moves += [(k_ref, ko_ref, kbuf.at[0]), (v_ref, vo_ref, kbuf.at[1])]
    get = [pltpu.make_async_copy(a, b, sem.at[0, i]) for i, (a, _, b) in enumerate(moves)]
    put = [pltpu.make_async_copy(b, c, sem.at[1, i]) for i, (_, c, b) in enumerate(moves)]
    for c in get:
        c.start()
    for g, p in zip(get, put):
        g.wait()
        p.start()
    for p in put:
        p.wait()


def _copy(*arrays):
    y, k, _ = arrays
    m, d = y.shape
    any_ = pl.BlockSpec(memory_space=pl.ANY)
    return pl.pallas_call(
        _copy_body,
        in_specs=[any_] * 3,
        out_specs=[any_] * 3,
        out_shape=[jax.ShapeDtypeStruct(a.shape, a.dtype) for a in arrays],
        scratch_shapes=[pltpu.VMEM((8, m // 8, d), BF16), pltpu.VMEM((2, *k.shape), BF16), pltpu.SemaphoreType.DMA((2, 10))],
        compiler_params=pltpu.CompilerParams(vmem_limit_bytes=67043328),
        name="result_copy",
    )(*arrays)


def solution(mesh):
    tok = P(("rep", "sp"), None)
    col = P(None, "tp")
    row = P("tp", None)
    cache = P("rep", ("tp", "sp"), None)

    def local(x, pos, g1, g2, wq, wk, wv, wo, w1, w3, w2):
        m, d = x.shape
        n = m * mesh.shape["sp"]
        cos, sin = _tables(pos)
        q, k, v, k1, v1, wo_oth = _qkv(x, g1, cos, sin, wq, wk, wv, wo, n)
        own, oth, wo_oth, late, late2 = _attention(q, k, v, k1, v1, wo, wo_oth)
        y = _mlp(own, oth, late, late2, x, wo, wo_oth, g2, w1, w3, w2)
        y, k, v = _copy(y, k, v)
        return y, k.reshape(n, 1, 128), v.reshape(n, 1, 128)

    return jax.shard_map(
        local,
        mesh=mesh,
        in_specs=(tok, P(("rep", "sp")), P(), P(), col, col, col, row, col, col, row),
        out_specs=(tok, cache, cache),
        check_vma=False,
    )
```

```python
import functools

import jax
import jax.numpy as jnp
from jax import lax
from jax.experimental import pallas as pl
from jax.experimental.pallas import tpu as pltpu
from jax.sharding import PartitionSpec as P

HEAD_DIM = 128
EPS = 1e-5
ROPE_BASE = 5e5
SCALE_LOG2E = HEAD_DIM ** -0.5 * 1.4426950408889634
NEG = -1e30
BQ = 512
BK = 2048
Y1 = (0, 272)
Y2 = ((272, 128), (400, 112))
YX = (480, 32)
XP = ((0, 144), (144, 128), (272, 128), (400, 80))
LATE_ROWS = 128
MESH = pl.DeviceIdType.MESH
F32 = jnp.float32
BF16 = jnp.bfloat16
LANES = 128
RB = 256
TILE = 512
HALF = 64
SP = 4
CORES = 2
MIB = 2**20
KERNEL_VMEM = 56 * MIB
MAX_VMEM = 67043328


def _rms(x, g):
    x32 = x.astype(F32)
    r = lax.rsqrt(jnp.mean(x32 * x32, axis=-1, keepdims=True) + EPS)
    return (x32 * r * g).astype(BF16)


def _tables(pos):
    half = HEAD_DIM // 2
    lane = jnp.arange(HEAD_DIM)
    inv = ROPE_BASE ** (-2.0 * (lane % half).astype(F32) / HEAD_DIM)
    ang = pos.astype(F32)[:, None] * inv
    return jnp.cos(ang), jnp.where(lane < half, -1.0, 1.0) * jnp.sin(ang)


def _barrier(peers):
    sem = pltpu.get_barrier_semaphore()
    for p in peers:
        pl.semaphore_signal(sem, inc=1, device_id=p, device_id_type=MESH)
    pl.semaphore_wait(sem, len(peers))


def _sp_order(s):
    return [(s + 2) % SP, 3 - s, s + 1 - 2 * (s % CORES), s]


def _wo_y(rep, tp, s, wo_hbm, wo_dst, quarter, piece, ssem, rsem):
    r0 = pl.multiple_of(quarter * (wo_hbm.shape[0] // SP) + piece[0], 16)
    return pltpu.make_async_remote_copy(src_ref=wo_hbm.at[pl.ds(r0, piece[1]), :], dst_ref=wo_dst.at[pl.ds(r0, piece[1]), :],
                                        send_sem=ssem, recv_sem=rsem, device_id=(rep, 1 - tp, s), device_id_type=MESH)


def _qkv_body(x_hbm, g_ref, cos_ref, sin_ref, wq_hbm, wk_hbm, wv_hbm, wo_hbm, q_hbm, k0_hbm, v0_hbm, k1_hbm, v1_hbm, wo_dst,
              xbuf, u, wq, wkv, qo, ko, vo, xsem, wsem, ssem, rsem, lsem, qsem, qrsem, wosem, worsem):
    rep, tp, s = lax.axis_index("rep"), lax.axis_index("tp"), lax.axis_index("sp")
    order = _sp_order(s)
    far, diag, mate = order[:3]
    on_x0 = s // CORES == 0
    m = u.shape[0]
    nb = xbuf.shape[0]
    rows = m // nb
    qw = qo.shape[2]

    def kvcopies(t):
        j, sl = order[t], t % 2
        return [
            pltpu.make_async_copy(wk_hbm.at[:, pl.ds(pl.multiple_of(j * LANES, LANES), LANES)], wkv.at[sl, :, pl.ds(0, LANES)], wsem.at[sl, 1]),
            pltpu.make_async_copy(wv_hbm.at[:, pl.ds(pl.multiple_of(j * LANES, LANES), LANES)], wkv.at[sl, :, pl.ds(LANES, LANES)], wsem.at[sl, 2]),
        ]

    groups = [mate, (mate + 2) % SP, s, far]

    def qcopy(t):
        return pltpu.make_async_copy(wq_hbm.at[:, pl.ds(pl.multiple_of(groups[t] * qw, LANES), qw)], wq.at[t % 2], wsem.at[t % 2, 0])

    xc = [pltpu.make_async_copy(x_hbm.at[pl.ds(b * rows, rows), :], xbuf.at[b], xsem.at[b]) for b in range(nb)]
    xc[0].start()
    for c in kvcopies(0):
        c.start()
    for c in xc[1:]:
        c.start()
    for c in kvcopies(1):
        c.start()
    qcopy(0).start()
    qcopy(1).start()
    _barrier([(rep, tp, far), (rep, tp, diag), (rep, tp, mate), (rep, 1 - tp, s)])
    wo_send = _wo_y(rep, tp, s, wo_hbm, wo_dst, s, Y1, wosem.at[0], worsem.at[0])
    wo_send.start()
    def rope(t, r0):
        c = cos_ref[pl.ds(r0, t.shape[0]), :]
        sn = sin_ref[pl.ds(r0, t.shape[0]), :]
        return t * c + pltpu.roll(t, HALF, 1) * sn

    hm = m // 2

    def kvpair(t, sl, h):
        pair = ((ko, k0_hbm), (vo, v0_hbm)) if sl == 0 else ((ko, k1_hbm), (vo, v1_hbm))
        dst = pl.ds(pl.multiple_of(s * m + h * hm, LANES), hm)
        return [(a.at[t, pl.ds(h * hm, hm), :], b.at[dst, :]) for a, b in pair]

    def remote(t, sl, j, h):
        return [pltpu.make_async_remote_copy(src_ref=a, dst_ref=b, send_sem=ssem.at[sl, t, h, i], recv_sem=rsem.at[sl, t, h, i],
                                             device_id=(rep, tp, j), device_id_type=MESH) for i, (a, b) in enumerate(kvpair(t, sl, h))]

    def local(t, sl, h):
        return [pltpu.make_async_copy(a, b, lsem.at[sl, h, i]) for i, (a, b) in enumerate(kvpair(t, sl, h))]

    sends = [[(0, far, False)], [(0, diag, False), (1, mate, False)], [(0, mate, False), (1, diag, True)], [(1, far, True)]]
    def norm(b):
        xc[b].wait()

        @pl.loop(0, rows // HALF)
        def _(i):
            xs = xbuf[b, pl.ds(pl.multiple_of(i * HALF, HALF), HALF), :].astype(F32)
            r = lax.rsqrt(jnp.mean(xs * xs, axis=-1, keepdims=True) + EPS)
            u[pl.ds(pl.multiple_of(b * rows + i * HALF, HALF), HALF), :] = (xs * r * g_ref[...]).astype(BF16)

    for t in range(SP):
        sl = t % 2
        if t > 0:
            for c in kvcopies(t):
                c.wait()
        for h in range(CORES):
            if t == 0:
                norm(2 * h)
                norm(2 * h + 1)
                if h == 0:
                    for c in kvcopies(0):
                        c.wait()

            @pl.loop(h * 2, h * 2 + 2)
            def _(i, t=t, sl=sl):
                r0 = pl.multiple_of(i * RB, RB)
                kv = jnp.dot(u[pl.ds(r0, RB), :], wkv[sl], preferred_element_type=F32)
                ko[t, pl.ds(r0, RB), :] = rope(kv[:, :LANES], r0).astype(BF16)
                vo[t, pl.ds(r0, RB), :] = kv[:, LANES:].astype(BF16)
            for slot, j, x0_only in sends[t]:
                def go(t=t, slot=slot, j=j, h=h):
                    for c in remote(t, slot, j, h):
                        c.start()
                if x0_only:
                    pl.when(on_x0)(go)
                else:
                    go()
            if t == 0 or t == 3:
                for c in local(t, 1 if t == 0 else 0, h):
                    c.start()
        if t < 2:
            for c in kvcopies(t + 2):
                c.start()

    def qmove(t, h):
        src = qo.at[t, pl.ds(h * hm, hm), :]
        to = q_hbm.at[t % 2, pl.ds(pl.multiple_of(((h + tp) % 2 * 2 + s % CORES) * hm, LANES), hm), :]
        if t < 2:
            return pltpu.make_async_remote_copy(src_ref=src, dst_ref=to, send_sem=qsem.at[t, h], recv_sem=qrsem.at[t, h],
                                                device_id=(rep, tp, mate), device_id_type=MESH)
        return pltpu.make_async_copy(src, to, qsem.at[t, h])

    for t in range(SP):
        qcopy(t).wait()

        @pl.loop(0, m // RB)
        def _(i, t=t):
            r0 = pl.multiple_of(i * RB, RB)
            qq = jnp.dot(u[pl.ds(r0, RB), :], wq[t % 2], preferred_element_type=F32)
            for n in range(qw // LANES):
                qo[t, pl.ds(r0, RB), n * LANES:(n + 1) * LANES] = rope(qq[:, n * LANES:(n + 1) * LANES], r0).astype(BF16)
        for h in range(CORES):
            qmove(t, h).start()
        if t < 2:
            qcopy(t + 2).start()

    for t in range(SP):
        for h in range(CORES):
            qmove(t, h).wait()
    for h in range(CORES):
        for c in local(0, 1, h) + local(3, 0, h):
            c.wait()
        for t in range(SP):
            for slot, j, x0_only in sends[t]:
                cs = remote(t, slot, j, h)
                if x0_only:
                    @pl.when(on_x0)
                    def _(cs=cs):
                        for c in cs:
                            c.wait_send()

                    @pl.when(jnp.logical_not(on_x0))
                    def _(cs=cs):
                        for c in cs:
                            c.wait_recv()
                else:
                    for c in cs:
                        c.wait()
    wo_send.wait()


def _qkv(x, g1, cos, sin, wq, wk, wv, wo, n):
    m, d = x.shape
    qw = wq.shape[1] // SP
    any_ = pl.BlockSpec(memory_space=pl.ANY)
    vm = pl.BlockSpec(memory_space=pltpu.VMEM)
    kv = jax.ShapeDtypeStruct((n, LANES), BF16)
    return pl.pallas_call(
        _qkv_body,
        in_specs=[any_, vm, vm, vm, any_, any_, any_, any_],
        out_specs=[any_] * 6,
        out_shape=[jax.ShapeDtypeStruct((2, 2 * m, qw), BF16), kv, kv, kv, kv, jax.ShapeDtypeStruct(wo.shape, BF16)],
        scratch_shapes=[
            pltpu.VMEM((SP, m // SP, d), BF16),
            pltpu.VMEM((m, d), BF16),
            pltpu.VMEM((2, d, qw), BF16),
            pltpu.VMEM((2, d, RB), BF16),
            pltpu.VMEM((SP, m, qw), BF16),
            pltpu.VMEM((SP, m, LANES), BF16),
            pltpu.VMEM((SP, m, LANES), BF16),
            pltpu.SemaphoreType.DMA((SP,)),
            pltpu.SemaphoreType.DMA((2, 3)),
            pltpu.SemaphoreType.DMA((2, SP, 2, 2)),
            pltpu.SemaphoreType.DMA((2, SP, 2, 2)),
            pltpu.SemaphoreType.DMA((2, 2, 2)),
            pltpu.SemaphoreType.DMA((SP, 2)),
            pltpu.SemaphoreType.DMA((2, 2)),
            pltpu.SemaphoreType.DMA((1,)),
            pltpu.SemaphoreType.DMA((1,)),
        ],
        compiler_params=pltpu.CompilerParams(collective_id=1, has_side_effects=True, vmem_limit_bytes=KERNEL_VMEM),
        cost_estimate=pl.CostEstimate(flops=2 * m * d * (SP * qw + 1024), bytes_accessed=80 * MIB, transcendentals=0),
        name="qkv_exchange",
    )(x, g1.reshape(1, -1), cos, sin, wq, wk, wv, wo)


def _place(t, tp):
    i = t // 2
    return t % 2, i % 2, (tp + i // 2) % 2


def _attn_body(q_ref, k0_hbm, v0_hbm, k1_hbm, v1_hbm, wo_hbm, woi_hbm, own_hbm, oth_hbm, wo_dst, late_hbm, late2_hbm,
               kb, vb, vt, eye, acc, ms, ls, ob, kvsem, ssem, rsem0, rsem1, lsem, lasem, l2sem, wsem, wrsem):
    rep, tp, s = lax.axis_index("rep"), lax.axis_index("tp"), lax.axis_index("sp")
    step = pl.program_id(0)
    order = _sp_order(s)
    far, diag, mate = order[:3]
    nh = q_ref.shape[2] // LANES
    m = q_ref.shape[1] * 2
    xrow = s // CORES * (2 * m)
    qr = wo_hbm.shape[0] // SP
    grp, cc, half = _place(step, tp)
    r = 2 * cc + half
    nk = kb.shape[1]

    wo_y = [_wo_y(rep, tp, s, wo_hbm, wo_dst, s, p, wsem.at[0, k], wrsem.at[0, k]) for k, p in enumerate(Y2)]
    wo_y.append(_wo_y(rep, tp, s, wo_hbm, wo_dst, far, YX, wsem.at[0, 2], wrsem.at[0, 2]))

    def wo_move(quarter, piece, peer, kind, k):
        r0 = pl.multiple_of(quarter * qr + piece[0], 16)
        return pltpu.make_async_remote_copy(src_ref=wo_dst.at[pl.ds(r0, piece[1]), :], dst_ref=wo_dst.at[pl.ds(r0, piece[1]), :],
                                            send_sem=wsem.at[kind, k], recv_sem=wrsem.at[kind, k],
                                            device_id=(rep, tp, peer), device_id_type=MESH)

    def wo_x(k):
        return wo_move(s, XP[k], far, 1, k)

    def wo_near(k):
        return wo_move(s, (Y1, *Y2)[k], mate, 2, k)

    def wo_near_far(k):
        return wo_move(far, (*XP, YX)[k], mate, 3, k)

    def kv_copies(g):
        return [pltpu.make_async_copy((k0_hbm, k1_hbm)[g], kb.at[g], kvsem.at[g, 0]),
                pltpu.make_async_copy((v0_hbm, v1_hbm)[g], vb.at[g], kvsem.at[g, 1])]

    @pl.when(step == 0)
    def _():
        for g in range(CORES):
            for c in kv_copies(g):
                c.start()
        _barrier([(rep, tp, far), (rep, tp, mate), (rep, 1 - tp, s), (rep, 1 - tp, mate)])
        for c in wo_y:
            c.start()
        wo_x(0).start()
        wo_x(1).start()
        wo_near(0).start()
        eye[...] = (lax.broadcasted_iota(jnp.int32, eye.shape, 0) == lax.broadcasted_iota(jnp.int32, eye.shape, 1)).astype(F32).astype(BF16)
        for g in range(CORES):
            for c in kv_copies(g):
                c.wait()

            @pl.loop(0, nk // TILE)
            def _(j, g=g):
                r0 = pl.multiple_of(j * TILE, TILE)
                vt[g, :, pl.ds(r0, TILE)] = lax.dot_general(
                    eye[:LANES, :LANES], vb[g, pl.ds(r0, TILE), :], (((1,), (1,)), ((), ())), preferred_element_type=F32).astype(BF16)

    ms[...] = jnp.full_like(ms, NEG)
    ls[...] = jnp.zeros_like(ls)
    acc[...] = jnp.zeros_like(acc)
    start = xrow + r * BQ

    def blk(k0, n, masked):
        k0 = pl.multiple_of(k0, BQ)
        kk_ = kb[grp, pl.ds(k0, n), :]
        vv_ = vt[grp, :, pl.ds(k0, n)]

        def scores(h):
            return lax.dot_general(kk_, q_ref[0, :, h * LANES:(h + 1) * LANES], (((1,), (1,)), ((), ())), preferred_element_type=F32)

        sc = scores(0)
        for h in range(nh):
            nxt = scores(h + 1) if h < nh - 1 else None
            if masked:
                kk = lax.broadcasted_iota(jnp.int32, (n, BQ), 0)
                qq = lax.broadcasted_iota(jnp.int32, (n, BQ), 1)
                sc = jnp.where(qq >= kk, sc, NEG)
            m0 = ms[h:h + 1, :]
            m1 = jnp.maximum(m0, jnp.max(sc, axis=0, keepdims=True))
            p = jnp.exp2((sc - m1) * SCALE_LOG2E)
            a = jnp.exp2((m0 - m1) * SCALE_LOG2E)
            ms[h:h + 1, :] = m1
            ls[h:h + 1, :] = ls[h:h + 1, :] * a + jnp.sum(p, axis=0, keepdims=True)
            acc[h] = acc[h] * a + jnp.dot(vv_, p.astype(BF16), preferred_element_type=F32)
            sc = nxt

    @pl.loop(0, start // BK)
    def _(j):
        blk(j * BK, BK, False)

    @pl.when(start // 1024 % 2 == 1)
    def _():
        blk(start // BK * BK, 1024, False)

    @pl.when(start // BQ % 2 == 1)
    def _():
        blk(start - BQ, BQ, False)

    blk(start, BQ, True)
    for h in range(nh):
        o = acc[h] * (1.0 / ls[h:h + 1, :])
        ob[step, :, h * LANES:(h + 1) * LANES] = lax.dot_general(
            eye[...], o.astype(BF16), (((1,), (1,)), ((), ())), preferred_element_type=F32).astype(BF16)

    w = q_ref.shape[2]

    def cols(src_s, g):
        return pl.ds(pl.multiple_of((src_s + 2 * g) % SP * w, LANES), w)

    def dst(ref, slot, src_s, g):
        return ref.at[slot, :, cols(src_s, g)]

    def to_own(t):
        g, _, half = _place(t, tp)
        slot = (half + tp + 1) % 2
        return pltpu.make_async_remote_copy(
            src_ref=ob.at[t], dst_ref=dst(own_hbm, slot, s, g), send_sem=ssem.at[0, t], recv_sem=rsem0.at[g, slot],
            device_id=(rep, tp, mate), device_id_type=MESH)

    def to_local(t):
        g, _, half = _place(t, tp)
        slot = (half + tp + 1) % 2
        return pltpu.make_async_copy(ob.at[t], dst(own_hbm, slot, s, g), lsem.at[g, half])

    def first_rows(g):
        return BQ if g == 0 else BQ - LATE_ROWS

    def to_oth(t, g):
        cc, nr = _place(t, tp)[1], first_rows(g)
        return pltpu.make_async_remote_copy(
            src_ref=ob.at[t, pl.ds(0, nr), :], dst_ref=oth_hbm.at[pl.ds(0, nr), cols(s, g)],
            send_sem=ssem.at[1, t], recv_sem=rsem1.at[s % CORES, g],
            device_id=(rep, 1 - tp, s // CORES * 2 + cc), device_id_type=MESH)

    def to_late2(t):
        cc = _place(t, tp)[1]
        return pltpu.make_async_copy(ob.at[t, pl.ds(BQ - LATE_ROWS, LATE_ROWS), :], late2_hbm.at[cc], l2sem.at[cc])

    def to_late(t):
        g, cc, _ = _place(t, tp)
        return pltpu.make_async_copy(ob.at[t], late_hbm.at[g, cc], lasem.at[g, cc])

    @pl.when((step < 4) & (grp == 0))
    def _():
        to_oth(step, 0).start()

    @pl.when((step < 4) & (grp == 1))
    def _():
        to_oth(step, 1).start()
        to_late2(step).start()

    @pl.when(step >= 4)
    def _():
        to_late(step).start()

    def mine(t):
        return _place(t, tp)[1] == s % CORES

    @pl.when(mine(step))
    def _():
        to_local(step).start()

    @pl.when(jnp.logical_not(mine(step)))
    def _():
        to_own(step).start()

    @pl.when(step == 2)
    def _():
        wo_y[0].wait_recv()
        wo_x(2).start()
        wo_near(1).start()
        wo_x(0).wait_recv()
        wo_near_far(0).start()

    @pl.when(step == 4)
    def _():
        wo_y[1].wait_recv()
        wo_x(3).start()
        wo_near(2).start()
        wo_y[2].wait_recv()
        wo_near_far(4).start()

    for k in (1, 2):
        @pl.when(step == 4 + k)
        def _(k=k):
            wo_x(k).wait_recv()
            wo_near_far(k).start()

    @pl.when(step == pl.num_programs(0) - 1)
    def _():
        wo_x(3).wait_recv()
        wo_near_far(3).start()

        for t in range(SP):
            to_oth(t, t % 2).wait_send()
            to_late(t + 4).wait()
        to_late2(1).wait()
        to_late2(3).wait()

        @pl.loop(0, 8)
        def _(t):
            @pl.when(mine(t))
            def _():
                to_local(t).wait()

            @pl.when(jnp.logical_not(mine(t)))
            def _():
                to_own(t).wait_send()

        for g in range(CORES):
            for slot in range(CORES):
                pltpu.make_async_remote_copy(
                    src_ref=ob.at[0], dst_ref=dst(own_hbm, slot, mate, g), send_sem=ssem.at[0, 0], recv_sem=rsem0.at[g, slot],
                    device_id=(rep, tp, mate), device_id_type=MESH).wait_recv()
            for core in range(CORES):
                src_s = s // CORES * 2 + core
                pltpu.make_async_remote_copy(
                    src_ref=ob.at[0, pl.ds(0, first_rows(g)), :], dst_ref=oth_hbm.at[pl.ds(0, first_rows(g)), cols(src_s, g)],
                    send_sem=ssem.at[1, 0], recv_sem=rsem1.at[core, g],
                    device_id=(rep, 1 - tp, src_s), device_id_type=MESH).wait_recv()
        for c in wo_y:
            c.wait_send()
        for k in range(SP):
            wo_x(k).wait_send()
        for k in range(3):
            wo_near(k).wait()
        for k in range(5):
            wo_near_far(k).wait()


def _attention(q, k0, v0, k1, v1, wo, wo_oth):
    n = k0.shape[0]
    _, m2, w = q.shape
    nh = w // LANES
    steps = 2 * m2 // BQ
    any_ = pl.BlockSpec(memory_space=pl.ANY)
    shape = jax.ShapeDtypeStruct((2, BQ, SP * w), BF16)
    return pl.pallas_call(
        _attn_body,
        grid=(steps,),
        in_specs=[pl.BlockSpec((1, BQ, w), lambda t: (t % 2, t // 2, 0))] + [any_] * 6,
        out_specs=[any_] * 5,
        out_shape=[shape, jax.ShapeDtypeStruct((BQ, SP * w), BF16), jax.ShapeDtypeStruct(wo.shape, BF16),
                   jax.ShapeDtypeStruct((2, 2, BQ, w), BF16), jax.ShapeDtypeStruct((2, LATE_ROWS, w), BF16)],
        input_output_aliases={6: 2},
        scratch_shapes=[
            pltpu.VMEM((2, n, LANES), BF16),
            pltpu.VMEM((2, n, LANES), BF16),
            pltpu.VMEM((2, LANES, n), BF16),
            pltpu.VMEM((BQ, BQ), BF16),
            pltpu.VMEM((nh, LANES, BQ), F32),
            pltpu.VMEM((8, BQ), F32),
            pltpu.VMEM((8, BQ), F32),
            pltpu.VMEM((steps, BQ, w), BF16),
            pltpu.SemaphoreType.DMA((2, 2)),
            pltpu.SemaphoreType.DMA((2, 8)),
            pltpu.SemaphoreType.DMA((2, 2)),
            pltpu.SemaphoreType.DMA((2, 2)),
            pltpu.SemaphoreType.DMA((2, 2)),
            pltpu.SemaphoreType.DMA((2, 2)),
            pltpu.SemaphoreType.DMA((2,)),
            pltpu.SemaphoreType.DMA((4, 5)),
            pltpu.SemaphoreType.DMA((4, 5)),
        ],
        compiler_params=pltpu.CompilerParams(collective_id=2, has_side_effects=True, vmem_limit_bytes=KERNEL_VMEM),
        cost_estimate=pl.CostEstimate(flops=2 * n * n * w * 2, bytes_accessed=16 * MIB, transcendentals=0),
        name="attention_exchange",
    )(q, k0, v0, k1, v1, wo, wo_oth)


NWO, NHID, NW2 = 8, 28, 16
UNITS = NWO + NHID + NW2
NBUF = 3
MB = RB


def _mlp_body(chunks, own_hbm, oth_hbm, x_hbm, wo_hbm, wo_oth_hbm, g_ref, w1_hbm, w3_hbm, w2_hbm, late_hbm, late2_hbm, y_hbm, olate_hbm, olate2_hbm,
              wb, abuf, xbuf, hid, pbuf, rbuf, ybuf, wsem, asem, ssem, rsem, ysem, yrsem, ylsem, lasem, larsem, l2sem, l2rsem):
    rep, tp, s = lax.axis_index("rep"), lax.axis_index("tp"), lax.axis_index("sp")
    hr = wo_hbm.shape[0]
    hm = x_hbm.shape[0] // 2
    kh = w2_hbm.shape[0] // 2
    total = UNITS * len(chunks)
    partner = (rep, 1 - tp, s)

    def col(j, w):
        return pl.ds(pl.multiple_of(j * w, w), w)

    def wo_copies(j, sl):
        return [pltpu.make_async_copy(wo_hbm.at[:, col(j, TILE)], wb.at[sl, pl.ds(0, hr), :], wsem.at[sl, 0]),
                pltpu.make_async_copy(wo_oth_hbm.at[:, col(j, TILE)], wb.at[sl, pl.ds(hr, hr), :], wsem.at[sl, 1])]

    def hid_copies(j, sl):
        return [pltpu.make_async_copy(w1_hbm.at[:, col(j, RB)], wb.at[sl, :, pl.ds(0, RB)], wsem.at[sl, 0]),
                pltpu.make_async_copy(w3_hbm.at[:, col(j, RB)], wb.at[sl, :, pl.ds(RB, RB)], wsem.at[sl, 1])]

    def w2_copies(t, sl):
        return [pltpu.make_async_copy(w2_hbm.at[pl.ds(pl.multiple_of(t % 2 * kh, LANES), kh), col(t // 2, TILE)], wb.at[sl, pl.ds(0, kh), :], wsem.at[sl, 0])]

    def issue(g):
        sl, u = g % NBUF, g % UNITS

        @pl.when(g < total)
        def _():
            @pl.when(u < NWO)
            def _():
                for c in wo_copies(u, sl):
                    c.start()

            @pl.when((u >= NWO) & (u < NWO + NHID))
            def _():
                for c in hid_copies(u - NWO, sl):
                    c.start()

            @pl.when(u >= NWO + NHID)
            def _():
                for c in w2_copies(u - NWO - NHID, sl):
                    c.start()

    def acts(c):
        slot, r0, nr = chunks[c]
        base = hm * ((tp + slot + 1) % 2) + r0
        rs = pl.ds(0, nr)
        xcopy = pltpu.make_async_copy(x_hbm.at[pl.ds(pl.multiple_of(base, LANES), nr), :], xbuf.at[rs, :], asem.at[0])
        cs = [pltpu.make_async_copy(own_hbm.at[slot, pl.ds(r0, nr), :], abuf.at[rs, pl.ds(0, hr)], asem.at[1])]
        late_at = hm - LATE_ROWS
        if slot == 1:
            cs.append(pltpu.make_async_copy(olate_hbm.at[pl.ds(r0, nr), :], abuf.at[rs, pl.ds(hr, hr)], asem.at[2]))
        elif r0 + nr <= late_at:
            cs.append(pltpu.make_async_copy(oth_hbm.at[pl.ds(r0, nr), :], abuf.at[rs, pl.ds(hr, hr)], asem.at[2]))
        else:
            n0 = late_at - r0
            c0 = pl.multiple_of(s // CORES * (hr // 2), LANES)
            c1 = pl.multiple_of((1 - s // CORES) * (hr // 2), LANES)
            ls = pl.ds(n0, LATE_ROWS)
            cs.append(pltpu.make_async_copy(oth_hbm.at[pl.ds(r0, n0), :], abuf.at[pl.ds(0, n0), pl.ds(hr, hr)], asem.at[2]))
            cs.append(pltpu.make_async_copy(oth_hbm.at[pl.ds(late_at, LATE_ROWS), pl.ds(c0, hr // 2)], abuf.at[ls, pl.ds(hr + c0, hr // 2)], asem.at[3]))
            cs.append(pltpu.make_async_copy(olate2_hbm, abuf.at[ls, pl.ds(hr + c1, hr // 2)], asem.at[4]))
        return xcopy, cs

    for g in range(NBUF - 1):
        issue(g)
    xc, ac = acts(0)
    xc.start()
    for c in ac:
        c.start()
    mate = s + 1 - 2 * (s % CORES)
    _barrier([partner, (rep, 1 - tp, mate)])
    w = late_hbm.shape[3]

    def late(g, cc, src_s):
        return pltpu.make_async_remote_copy(
            src_ref=late_hbm.at[g, cc], dst_ref=olate_hbm.at[:, pl.ds(pl.multiple_of((src_s + 2 * g) % SP * w, LANES), w)],
            send_sem=lasem.at[g, cc], recv_sem=larsem.at[g, src_s % CORES],
            device_id=(rep, 1 - tp, s // CORES * 2 + cc), device_id_type=MESH)

    def late2(cc, src_s):
        return pltpu.make_async_remote_copy(
            src_ref=late2_hbm.at[cc], dst_ref=olate2_hbm.at[:, pl.ds(pl.multiple_of(src_s % CORES * w, LANES), w)],
            send_sem=l2sem.at[cc], recv_sem=l2rsem.at[src_s % CORES],
            device_id=(rep, 1 - tp, s // CORES * 2 + cc), device_id_type=MESH)

    for cc in range(CORES):
        late2(cc, s).start()
    for g in range(CORES):
        for cc in range(CORES):
            late(g, cc, s).start()

    def send(ci, j):
        slot, r0, nr = chunks[ci]
        return pltpu.make_async_remote_copy(src_ref=pbuf.at[j, pl.ds(r0, nr), :], dst_ref=rbuf.at[j, pl.ds(r0, nr), :],
                                            send_sem=ssem.at[ci, j], recv_sem=rsem.at[ci, j], device_id=partner, device_id_type=MESH)

    yr0 = pl.multiple_of(tp * hm, LANES)

    def ysend(j):
        return pltpu.make_async_remote_copy(src_ref=ybuf.at[j], dst_ref=y_hbm.at[pl.ds(yr0, hm), col(j, TILE)],
                                            send_sem=ysem.at[j], recv_sem=yrsem.at[j], device_id=partner, device_id_type=MESH)

    def yrecv(j):
        return pltpu.make_async_remote_copy(src_ref=ybuf.at[j], dst_ref=y_hbm.at[pl.ds(pl.multiple_of((1 - tp) * hm, LANES), hm), col(j, TILE)],
                                            send_sem=ysem.at[j], recv_sem=yrsem.at[j], device_id=partner, device_id_type=MESH)

    def yown(j):
        return pltpu.make_async_copy(ybuf.at[j], y_hbm.at[pl.ds(yr0, hm), col(j, TILE)], ylsem.at[j])

    nsend = len(chunks) - 1
    for ci, (slot, r0, nr) in enumerate(chunks):
        g0 = ci * UNITS
        xc, ac = acts(ci)
        xc.wait()
        for c in ac:
            c.wait()

        @pl.loop(0, NWO)
        def _(j, g0=g0, nr=nr):
            g = g0 + j
            sl = g % NBUF
            issue(g + NBUF - 1)
            for c in wo_copies(j, sl):
                c.wait()
            for b in range(nr // MB):
                rs = pl.ds(b * MB, MB)
                o = jnp.dot(abuf[rs, :], wb[sl], preferred_element_type=F32)
                xbuf[rs, col(j, TILE)] = (xbuf[rs, col(j, TILE)].astype(F32) + o).astype(BF16)

        @pl.loop(0, nr // HALF)
        def _(i):
            rs = pl.ds(pl.multiple_of(i * HALF, HALF), HALF)
            xs = xbuf[rs, :].astype(F32)
            r = lax.rsqrt(jnp.mean(xs * xs, axis=-1, keepdims=True) + EPS)
            abuf[rs, :] = (xs * r * g_ref[...]).astype(BF16)

        if ci + 1 < len(chunks):
            acts(ci + 1)[0].start()

        @pl.loop(0, NHID)
        def _(j, g0=g0, nr=nr):
            g = g0 + NWO + j
            sl = g % NBUF
            issue(g + NBUF - 1)
            for c in hid_copies(j, sl):
                c.wait()
            for b in range(nr // MB):
                rs = pl.ds(b * MB, MB)
                ab = jnp.dot(abuf[rs, :], wb[sl], preferred_element_type=F32)
                a = ab[:, :RB]
                hid[rs, col(j, RB)] = (a / (1.0 + jnp.exp(-a)) * ab[:, RB:]).astype(BF16)

        if ci + 3 == len(chunks):
            for core in range(CORES):
                late2(core, s // CORES * 2 + core).wait_recv()
        if ci + 2 == len(chunks):
            for g in range(CORES):
                for core in range(CORES):
                    late(g, core, s // CORES * 2 + core).wait_recv()
        if ci + 1 < len(chunks):
            for c in acts(ci + 1)[1]:
                c.start()

        @pl.loop(0, NW2 // 2)
        def _(j, g0=g0, ci=ci, slot=slot, r0=r0, nr=nr):
            g = g0 + NWO + NHID + 2 * j
            for h in range(CORES):
                sl = (g + h) % NBUF
                issue(g + h + NBUF - 1)
                for c in w2_copies(2 * j + h, sl):
                    c.wait()
                for b in range(nr // MB):
                    rs = pl.ds(b * MB, MB)
                    ps = pl.ds(r0 + b * MB, MB)
                    o = jnp.dot(hid[rs, h * kh:(h + 1) * kh], wb[sl, pl.ds(0, kh), :], preferred_element_type=F32)
                    if h == 0:
                        pbuf[j if slot == 0 else NW2 // 2, ps, :] = o
                    elif slot == 0:
                        pbuf[j, ps, :] = pbuf[j, ps, :] + o
                    else:
                        if b == 0:
                            for k in range(nsend):
                                send(k, j).wait_recv()
                        o = o + pbuf[NW2 // 2, ps, :] + rbuf[j, ps, :]
                        ybuf[j, ps, :] = (xbuf[rs, col(j, TILE)].astype(F32) + o).astype(BF16)
            if slot == 0:
                send(ci, j).start()
            else:
                ysend(j).start()
                yown(j).start()

    for cc in range(CORES):
        late2(cc, s).wait_send()
        for g in range(CORES):
            late(g, cc, s).wait_send()

    @pl.loop(0, NW2 // 2)
    def _(j):
        for k in range(nsend):
            send(k, j).wait_send()
        ysend(j).wait_send()
        yown(j).wait()
        yrecv(j).wait_recv()


def _mlp(own, oth, late, late2, x, wo, wo_oth, g2, w1, w3, w2):
    m, d = x.shape
    hm = m // 2
    chunks = ((0, 0, RB), (0, RB, RB), (1, 0, TILE))
    any_ = pl.BlockSpec(memory_space=pl.ANY)
    vm = pl.BlockSpec(memory_space=pltpu.VMEM)
    nt = NW2 // 2
    return pl.pallas_call(
        functools.partial(_mlp_body, chunks),
        in_specs=[any_] * 5 + [vm] + [any_] * 5,
        out_specs=[any_] * 3,
        out_shape=[jax.ShapeDtypeStruct((m, d), BF16), jax.ShapeDtypeStruct((hm, wo.shape[0]), BF16),
                   jax.ShapeDtypeStruct((LATE_ROWS, wo.shape[0] // 2), BF16)],
        scratch_shapes=[
            pltpu.VMEM((NBUF, d, TILE), BF16),
            pltpu.VMEM((hm, d), BF16),
            pltpu.VMEM((hm, d), BF16),
            pltpu.VMEM((hm, w2.shape[0]), BF16),
            pltpu.VMEM((nt + 1, hm, TILE), F32),
            pltpu.VMEM((nt, hm, TILE), F32),
            pltpu.VMEM((nt, hm, TILE), BF16),
            pltpu.SemaphoreType.DMA((NBUF, 2)),
            pltpu.SemaphoreType.DMA((5,)),
            pltpu.SemaphoreType.DMA((2, nt)),
            pltpu.SemaphoreType.DMA((2, nt)),
            pltpu.SemaphoreType.DMA((nt,)),
            pltpu.SemaphoreType.DMA((nt,)),
            pltpu.SemaphoreType.DMA((nt,)),
            pltpu.SemaphoreType.DMA((2, 2)),
            pltpu.SemaphoreType.DMA((2, 2)),
            pltpu.SemaphoreType.DMA((2,)),
            pltpu.SemaphoreType.DMA((2,)),
        ],
        compiler_params=pltpu.CompilerParams(collective_id=3, has_side_effects=True, vmem_limit_bytes=MAX_VMEM),
        cost_estimate=pl.CostEstimate(flops=2 * m * d * (d + 3 * w1.shape[1]), bytes_accessed=640 * MIB, transcendentals=0),
        name="mlp_sum",
    )(own, oth, x, wo, wo_oth, g2.reshape(1, -1), w1, w3, w2, late, late2)[0]


def _copy_body(y_ref, k_ref, v_ref, yo_ref, ko_ref, vo_ref, buf, kbuf, sem):
    n, nr = buf.shape[:2]
    moves = [(y_ref.at[pl.ds(i * nr, nr), :], yo_ref.at[pl.ds(i * nr, nr), :], buf.at[i]) for i in range(n)]
    moves += [(k_ref, ko_ref, kbuf.at[0]), (v_ref, vo_ref, kbuf.at[1])]
    get = [pltpu.make_async_copy(a, b, sem.at[0, i]) for i, (a, _, b) in enumerate(moves)]
    put = [pltpu.make_async_copy(b, c, sem.at[1, i]) for i, (_, c, b) in enumerate(moves)]
    for c in get:
        c.start()
    for g, p in zip(get, put):
        g.wait()
        p.start()
    for p in put:
        p.wait()


def _copy(*arrays):
    y, k, _ = arrays
    m, d = y.shape
    any_ = pl.BlockSpec(memory_space=pl.ANY)
    return pl.pallas_call(
        _copy_body,
        in_specs=[any_] * 3,
        out_specs=[any_] * 3,
        out_shape=[jax.ShapeDtypeStruct(a.shape, a.dtype) for a in arrays],
        scratch_shapes=[pltpu.VMEM((8, m // 8, d), BF16), pltpu.VMEM((2, *k.shape), BF16), pltpu.SemaphoreType.DMA((2, 10))],
        compiler_params=pltpu.CompilerParams(vmem_limit_bytes=MAX_VMEM),
        name="result_copy",
    )(*arrays)


def solution(mesh):
    tok = P(("rep", "sp"), None)
    col = P(None, "tp")
    row = P("tp", None)
    cache = P("rep", ("tp", "sp"), None)

    def local(x, pos, g1, g2, wq, wk, wv, wo, w1, w3, w2):
        m, d = x.shape
        n = m * mesh.shape["sp"]
        cos, sin = _tables(pos)
        q, k, v, k1, v1, wo_oth = _qkv(x, g1, cos, sin, wq, wk, wv, wo, n)
        own, oth, wo_oth, late, late2 = _attention(q, k, v, k1, v1, wo, wo_oth)
        y = _mlp(own, oth, late, late2, x, wo, wo_oth, g2, w1, w3, w2)
        y, k, v = _copy(y, k, v)
        return y, k.reshape(n, 1, LANES), v.reshape(n, 1, LANES)

    return jax.shard_map(
        local,
        mesh=mesh,
        in_specs=(tok, P(("rep", "sp")), P(), P(), col, col, col, row, col, col, row),
        out_specs=(tok, cache, cache),
        check_vma=False,
    )
```

```python
import functools

import jax
import jax.numpy as jnp
from jax import lax
from jax.experimental import pallas as pl
from jax.experimental.pallas import tpu as pltpu
from jax.sharding import PartitionSpec as P

HEAD_DIM = 128
EPS = 1e-5
ROPE_BASE = 5e5
SCALE_LOG2E = HEAD_DIM ** -0.5 * 1.4426950408889634
NEG = -1e30
BQ = 512
BK = 2048
Y1 = (0, 272)
Y2 = ((272, 128), (400, 112))
YX = (480, 32)
XP = ((0, 144), (144, 128), (272, 128), (400, 80))
LATE_ROWS = 128
MESH = pl.DeviceIdType.MESH
F32 = jnp.float32
BF16 = jnp.bfloat16
LANES = 128
RB = 256
TILE = 512
HALF = 64
SP = 4
CORES = 2
MIB = 2**20
KERNEL_VMEM = 56 * MIB
MAX_VMEM = 67043328


def _rms(x, g):
    x32 = x.astype(F32)
    r = lax.rsqrt(jnp.mean(x32 * x32, axis=-1, keepdims=True) + EPS)
    return (x32 * r * g).astype(BF16)


def _tables(pos):
    half = HEAD_DIM // 2
    lane = jnp.arange(HEAD_DIM)
    inv = ROPE_BASE ** (-2.0 * (lane % half).astype(F32) / HEAD_DIM)
    ang = pos.astype(F32)[:, None] * inv
    return jnp.cos(ang), jnp.where(lane < half, -1.0, 1.0) * jnp.sin(ang)


def _barrier(peers):
    sem = pltpu.get_barrier_semaphore()
    for p in peers:
        pl.semaphore_signal(sem, inc=1, device_id=p, device_id_type=MESH)
    pl.semaphore_wait(sem, len(peers))


def _sp_order(s):
    return [(s + 2) % SP, 3 - s, s + 1 - 2 * (s % CORES), s]


def _wo_y(rep, tp, s, wo_hbm, wo_dst, quarter, piece, ssem, rsem):
    r0 = pl.multiple_of(quarter * (wo_hbm.shape[0] // SP) + piece[0], 16)
    return pltpu.make_async_remote_copy(src_ref=wo_hbm.at[pl.ds(r0, piece[1]), :], dst_ref=wo_dst.at[pl.ds(r0, piece[1]), :],
                                        send_sem=ssem, recv_sem=rsem, device_id=(rep, 1 - tp, s), device_id_type=MESH)


def _qkv_body(x_hbm, g_ref, cos_ref, sin_ref, wq_hbm, wk_hbm, wv_hbm, wo_hbm, q_hbm, k0_hbm, v0_hbm, k1_hbm, v1_hbm, wo_dst,
              xbuf, u, wq, wkv, qo, ko, vo, xsem, wsem, ssem, rsem, lsem, qsem, qrsem, wosem, worsem):
    rep, tp, s = lax.axis_index("rep"), lax.axis_index("tp"), lax.axis_index("sp")
    order = _sp_order(s)
    far, diag, mate = order[:3]
    on_x0 = s // CORES == 0
    m = u.shape[0]
    nb = xbuf.shape[0]
    rows = m // nb
    qw = qo.shape[2]

    def kvcopies(t):
        j, sl = order[t], t % 2
        return [
            pltpu.make_async_copy(wk_hbm.at[:, pl.ds(pl.multiple_of(j * LANES, LANES), LANES)], wkv.at[sl, :, pl.ds(0, LANES)], wsem.at[sl, 1]),
            pltpu.make_async_copy(wv_hbm.at[:, pl.ds(pl.multiple_of(j * LANES, LANES), LANES)], wkv.at[sl, :, pl.ds(LANES, LANES)], wsem.at[sl, 2]),
        ]

    groups = [mate, (mate + 2) % SP, s, far]

    def qcopy(t):
        return pltpu.make_async_copy(wq_hbm.at[:, pl.ds(pl.multiple_of(groups[t] * qw, LANES), qw)], wq.at[t % 2], wsem.at[t % 2, 0])

    xc = [pltpu.make_async_copy(x_hbm.at[pl.ds(b * rows, rows), :], xbuf.at[b], xsem.at[b]) for b in range(nb)]
    xc[0].start()
    for c in kvcopies(0):
        c.start()
    for c in xc[1:]:
        c.start()
    for c in kvcopies(1):
        c.start()
    qcopy(0).start()
    qcopy(1).start()
    _barrier([(rep, tp, far), (rep, tp, diag), (rep, tp, mate), (rep, 1 - tp, s)])
    wo_send = _wo_y(rep, tp, s, wo_hbm, wo_dst, s, Y1, wosem.at[0], worsem.at[0])
    wo_send.start()
    def rope(t, r0):
        c = cos_ref[pl.ds(r0, t.shape[0]), :]
        sn = sin_ref[pl.ds(r0, t.shape[0]), :]
        return t * c + pltpu.roll(t, HALF, 1) * sn

    hm = m // 2

    def kvpair(t, sl, h):
        pair = ((ko, k0_hbm), (vo, v0_hbm)) if sl == 0 else ((ko, k1_hbm), (vo, v1_hbm))
        dst = pl.ds(pl.multiple_of(s * m + h * hm, LANES), hm)
        return [(a.at[t, pl.ds(h * hm, hm), :], b.at[dst, :]) for a, b in pair]

    def remote(t, sl, j, h):
        return [pltpu.make_async_remote_copy(src_ref=a, dst_ref=b, send_sem=ssem.at[sl, t, h, i], recv_sem=rsem.at[sl, t, h, i],
                                             device_id=(rep, tp, j), device_id_type=MESH) for i, (a, b) in enumerate(kvpair(t, sl, h))]

    def local(t, sl, h):
        return [pltpu.make_async_copy(a, b, lsem.at[sl, h, i]) for i, (a, b) in enumerate(kvpair(t, sl, h))]

    sends = [[(0, far, False)], [(0, diag, False), (1, mate, False)], [(0, mate, False), (1, diag, True)], [(1, far, True)]]
    def norm(b):
        xc[b].wait()

        @pl.loop(0, rows // HALF)
        def _(i):
            xs = xbuf[b, pl.ds(pl.multiple_of(i * HALF, HALF), HALF), :].astype(F32)
            r = lax.rsqrt(jnp.mean(xs * xs, axis=-1, keepdims=True) + EPS)
            u[pl.ds(pl.multiple_of(b * rows + i * HALF, HALF), HALF), :] = (xs * r * g_ref[...]).astype(BF16)

    for t in range(SP):
        sl = t % 2
        if t > 0:
            for c in kvcopies(t):
                c.wait()
        for h in range(CORES):
            if t == 0:
                norm(2 * h)
                norm(2 * h + 1)
                if h == 0:
                    for c in kvcopies(0):
                        c.wait()

            @pl.loop(h * 2, h * 2 + 2)
            def _(i, t=t, sl=sl):
                r0 = pl.multiple_of(i * RB, RB)
                kv = jnp.dot(u[pl.ds(r0, RB), :], wkv[sl], preferred_element_type=F32)
                ko[t, pl.ds(r0, RB), :] = rope(kv[:, :LANES], r0).astype(BF16)
                vo[t, pl.ds(r0, RB), :] = kv[:, LANES:].astype(BF16)
            for slot, j, x0_only in sends[t]:
                def go(t=t, slot=slot, j=j, h=h):
                    for c in remote(t, slot, j, h):
                        c.start()
                if x0_only:
                    pl.when(on_x0)(go)
                else:
                    go()
            if t == 0 or t == 3:
                for c in local(t, 1 if t == 0 else 0, h):
                    c.start()
        if t < 2:
            for c in kvcopies(t + 2):
                c.start()

    def qmove(t, h):
        src = qo.at[t, pl.ds(h * hm, hm), :]
        to = q_hbm.at[t % 2, pl.ds(pl.multiple_of(((h + tp) % 2 * 2 + s % CORES) * hm, LANES), hm), :]
        if t < 2:
            return pltpu.make_async_remote_copy(src_ref=src, dst_ref=to, send_sem=qsem.at[t, h], recv_sem=qrsem.at[t, h],
                                                device_id=(rep, tp, mate), device_id_type=MESH)
        return pltpu.make_async_copy(src, to, qsem.at[t, h])

    for t in range(SP):
        qcopy(t).wait()

        @pl.loop(0, m // RB)
        def _(i, t=t):
            r0 = pl.multiple_of(i * RB, RB)
            qq = jnp.dot(u[pl.ds(r0, RB), :], wq[t % 2], preferred_element_type=F32)
            for n in range(qw // LANES):
                qo[t, pl.ds(r0, RB), n * LANES:(n + 1) * LANES] = rope(qq[:, n * LANES:(n + 1) * LANES], r0).astype(BF16)
        for h in range(CORES):
            qmove(t, h).start()
        if t < 2:
            qcopy(t + 2).start()

    for t in range(SP):
        for h in range(CORES):
            qmove(t, h).wait()
    for h in range(CORES):
        for c in local(0, 1, h) + local(3, 0, h):
            c.wait()
        for t in range(SP):
            for slot, j, x0_only in sends[t]:
                cs = remote(t, slot, j, h)
                if x0_only:
                    @pl.when(on_x0)
                    def _(cs=cs):
                        for c in cs:
                            c.wait_send()

                    @pl.when(jnp.logical_not(on_x0))
                    def _(cs=cs):
                        for c in cs:
                            c.wait_recv()
                else:
                    for c in cs:
                        c.wait()
    wo_send.wait()


def _qkv(x, g1, cos, sin, wq, wk, wv, wo, n):
    m, d = x.shape
    qw = wq.shape[1] // SP
    any_ = pl.BlockSpec(memory_space=pl.ANY)
    vm = pl.BlockSpec(memory_space=pltpu.VMEM)
    kv = jax.ShapeDtypeStruct((n, LANES), BF16)
    return pl.pallas_call(
        _qkv_body,
        in_specs=[any_, vm, vm, vm, any_, any_, any_, any_],
        out_specs=[any_] * 6,
        out_shape=[jax.ShapeDtypeStruct((2, 2 * m, qw), BF16), kv, kv, kv, kv, jax.ShapeDtypeStruct(wo.shape, BF16)],
        scratch_shapes=[
            pltpu.VMEM((SP, m // SP, d), BF16),
            pltpu.VMEM((m, d), BF16),
            pltpu.VMEM((2, d, qw), BF16),
            pltpu.VMEM((2, d, RB), BF16),
            pltpu.VMEM((SP, m, qw), BF16),
            pltpu.VMEM((SP, m, LANES), BF16),
            pltpu.VMEM((SP, m, LANES), BF16),
            pltpu.SemaphoreType.DMA((SP,)),
            pltpu.SemaphoreType.DMA((2, 3)),
            pltpu.SemaphoreType.DMA((2, SP, 2, 2)),
            pltpu.SemaphoreType.DMA((2, SP, 2, 2)),
            pltpu.SemaphoreType.DMA((2, 2, 2)),
            pltpu.SemaphoreType.DMA((SP, 2)),
            pltpu.SemaphoreType.DMA((2, 2)),
            pltpu.SemaphoreType.DMA((1,)),
            pltpu.SemaphoreType.DMA((1,)),
        ],
        compiler_params=pltpu.CompilerParams(collective_id=1, has_side_effects=True, vmem_limit_bytes=KERNEL_VMEM),
        cost_estimate=pl.CostEstimate(flops=2 * m * d * (SP * qw + 1024), bytes_accessed=80 * MIB, transcendentals=0),
        name="qkv_exchange",
    )(x, g1.reshape(1, -1), cos, sin, wq, wk, wv, wo)


def _place(t, tp):
    i = t // 2
    return t % 2, i % 2, (tp + i // 2) % 2


def _attn_body(q_ref, k0_hbm, v0_hbm, k1_hbm, v1_hbm, wo_hbm, woi_hbm, own_hbm, oth_hbm, wo_dst, late_hbm, late2_hbm,
               kb, vb, vt, eye, acc, ms, ls, ob, kvsem, ssem, rsem0, rsem1, lsem, lasem, l2sem, wsem, wrsem):
    rep, tp, s = lax.axis_index("rep"), lax.axis_index("tp"), lax.axis_index("sp")
    step = pl.program_id(0)
    order = _sp_order(s)
    far, diag, mate = order[:3]
    nh = q_ref.shape[2] // LANES
    m = q_ref.shape[1] * 2
    xrow = s // CORES * (2 * m)
    qr = wo_hbm.shape[0] // SP
    grp, cc, half = _place(step, tp)
    r = 2 * cc + half
    nk = kb.shape[1]

    wo_y = [_wo_y(rep, tp, s, wo_hbm, wo_dst, s, p, wsem.at[0, k], wrsem.at[0, k]) for k, p in enumerate(Y2)]
    wo_y.append(_wo_y(rep, tp, s, wo_hbm, wo_dst, far, YX, wsem.at[0, 2], wrsem.at[0, 2]))

    def wo_move(quarter, piece, peer, kind, k):
        r0 = pl.multiple_of(quarter * qr + piece[0], 16)
        return pltpu.make_async_remote_copy(src_ref=wo_dst.at[pl.ds(r0, piece[1]), :], dst_ref=wo_dst.at[pl.ds(r0, piece[1]), :],
                                            send_sem=wsem.at[kind, k], recv_sem=wrsem.at[kind, k],
                                            device_id=(rep, tp, peer), device_id_type=MESH)

    def wo_x(k):
        return wo_move(s, XP[k], far, 1, k)

    def wo_near(k):
        return wo_move(s, (Y1, *Y2)[k], mate, 2, k)

    def wo_near_far(k):
        return wo_move(far, (*XP, YX)[k], mate, 3, k)

    def kv_copies(g):
        return [pltpu.make_async_copy((k0_hbm, k1_hbm)[g], kb.at[g], kvsem.at[g, 0]),
                pltpu.make_async_copy((v0_hbm, v1_hbm)[g], vb.at[g], kvsem.at[g, 1])]

    @pl.when(step == 0)
    def _():
        for g in range(CORES):
            for c in kv_copies(g):
                c.start()
        _barrier([(rep, tp, far), (rep, tp, mate), (rep, 1 - tp, s), (rep, 1 - tp, mate)])
        for c in wo_y:
            c.start()
        wo_x(0).start()
        wo_x(1).start()
        wo_near(0).start()
        eye[...] = (lax.broadcasted_iota(jnp.int32, eye.shape, 0) == lax.broadcasted_iota(jnp.int32, eye.shape, 1)).astype(F32).astype(BF16)
        for g in range(CORES):
            for c in kv_copies(g):
                c.wait()

            @pl.loop(0, nk // TILE)
            def _(j, g=g):
                r0 = pl.multiple_of(j * TILE, TILE)
                vt[g, :, pl.ds(r0, TILE)] = lax.dot_general(
                    eye[:LANES, :LANES], vb[g, pl.ds(r0, TILE), :], (((1,), (1,)), ((), ())), preferred_element_type=F32).astype(BF16)

    ms[...] = jnp.full_like(ms, NEG)
    ls[...] = jnp.zeros_like(ls)
    acc[...] = jnp.zeros_like(acc)
    start = xrow + r * BQ

    def blk(k0, n, masked):
        k0 = pl.multiple_of(k0, BQ)
        kk_ = kb[grp, pl.ds(k0, n), :]
        vv_ = vt[grp, :, pl.ds(k0, n)]

        def scores(h):
            return lax.dot_general(kk_, q_ref[0, :, h * LANES:(h + 1) * LANES], (((1,), (1,)), ((), ())), preferred_element_type=F32)

        sc = scores(0)
        for h in range(nh):
            nxt = scores(h + 1) if h < nh - 1 else None
            if masked:
                kk = lax.broadcasted_iota(jnp.int32, (n, BQ), 0)
                qq = lax.broadcasted_iota(jnp.int32, (n, BQ), 1)
                sc = jnp.where(qq >= kk, sc, NEG)
            m0 = ms[h:h + 1, :]
            m1 = jnp.maximum(m0, jnp.max(sc, axis=0, keepdims=True))
            p = jnp.exp2((sc - m1) * SCALE_LOG2E)
            a = jnp.exp2((m0 - m1) * SCALE_LOG2E)
            ms[h:h + 1, :] = m1
            ls[h:h + 1, :] = ls[h:h + 1, :] * a + jnp.sum(p, axis=0, keepdims=True)
            acc[h] = acc[h] * a + jnp.dot(vv_, p.astype(BF16), preferred_element_type=F32)
            sc = nxt

    @pl.loop(0, start // BK)
    def _(j):
        blk(j * BK, BK, False)

    @pl.when(start // 1024 % 2 == 1)
    def _():
        blk(start // BK * BK, 1024, False)

    @pl.when(start // BQ % 2 == 1)
    def _():
        blk(start - BQ, BQ, False)

    blk(start, BQ, True)
    for h in range(nh):
        o = acc[h] * (1.0 / ls[h:h + 1, :])
        ob[step, :, h * LANES:(h + 1) * LANES] = lax.dot_general(
            eye[...], o.astype(BF16), (((1,), (1,)), ((), ())), preferred_element_type=F32).astype(BF16)

    w = q_ref.shape[2]

    def cols(src_s, g):
        return pl.ds(pl.multiple_of((src_s + 2 * g) % SP * w, LANES), w)

    def dst(ref, slot, src_s, g):
        return ref.at[slot, :, cols(src_s, g)]

    def to_own(t):
        g, _, half = _place(t, tp)
        slot = (half + tp + 1) % 2
        return pltpu.make_async_remote_copy(
            src_ref=ob.at[t], dst_ref=dst(own_hbm, slot, s, g), send_sem=ssem.at[0, t], recv_sem=rsem0.at[g, slot],
            device_id=(rep, tp, mate), device_id_type=MESH)

    def to_local(t):
        g, _, half = _place(t, tp)
        slot = (half + tp + 1) % 2
        return pltpu.make_async_copy(ob.at[t], dst(own_hbm, slot, s, g), lsem.at[g, half])

    def first_rows(g):
        return BQ if g == 0 else BQ - LATE_ROWS

    def to_oth(t, g):
        cc, nr = _place(t, tp)[1], first_rows(g)
        return pltpu.make_async_remote_copy(
            src_ref=ob.at[t, pl.ds(0, nr), :], dst_ref=oth_hbm.at[pl.ds(0, nr), cols(s, g)],
            send_sem=ssem.at[1, t], recv_sem=rsem1.at[s % CORES, g],
            device_id=(rep, 1 - tp, s // CORES * 2 + cc), device_id_type=MESH)

    def to_late2(t):
        cc = _place(t, tp)[1]
        return pltpu.make_async_copy(ob.at[t, pl.ds(BQ - LATE_ROWS, LATE_ROWS), :], late2_hbm.at[cc], l2sem.at[cc])

    def to_late(t):
        g, cc, _ = _place(t, tp)
        return pltpu.make_async_copy(ob.at[t], late_hbm.at[g, cc], lasem.at[g, cc])

    @pl.when((step < 4) & (grp == 0))
    def _():
        to_oth(step, 0).start()

    @pl.when((step < 4) & (grp == 1))
    def _():
        to_oth(step, 1).start()
        to_late2(step).start()

    @pl.when(step >= 4)
    def _():
        to_late(step).start()

    def mine(t):
        return _place(t, tp)[1] == s % CORES

    @pl.when(mine(step))
    def _():
        to_local(step).start()

    @pl.when(jnp.logical_not(mine(step)))
    def _():
        to_own(step).start()

    @pl.when(step == 2)
    def _():
        wo_y[0].wait_recv()
        wo_x(2).start()
        wo_near(1).start()
        wo_x(0).wait_recv()
        wo_near_far(0).start()

    @pl.when(step == 4)
    def _():
        wo_y[1].wait_recv()
        wo_x(3).start()
        wo_near(2).start()
        wo_y[2].wait_recv()
        wo_near_far(4).start()

    for k in (1, 2):
        @pl.when(step == 4 + k)
        def _(k=k):
            wo_x(k).wait_recv()
            wo_near_far(k).start()

    @pl.when(step == pl.num_programs(0) - 1)
    def _():
        wo_x(3).wait_recv()
        wo_near_far(3).start()

        for t in range(SP):
            to_oth(t, t % 2).wait_send()
            to_late(t + 4).wait()
        to_late2(1).wait()
        to_late2(3).wait()

        @pl.loop(0, 8)
        def _(t):
            @pl.when(mine(t))
            def _():
                to_local(t).wait()

            @pl.when(jnp.logical_not(mine(t)))
            def _():
                to_own(t).wait_send()

        for g in range(CORES):
            for slot in range(CORES):
                pltpu.make_async_remote_copy(
                    src_ref=ob.at[0], dst_ref=dst(own_hbm, slot, mate, g), send_sem=ssem.at[0, 0], recv_sem=rsem0.at[g, slot],
                    device_id=(rep, tp, mate), device_id_type=MESH).wait_recv()
            for core in range(CORES):
                src_s = s // CORES * 2 + core
                pltpu.make_async_remote_copy(
                    src_ref=ob.at[0, pl.ds(0, first_rows(g)), :], dst_ref=oth_hbm.at[pl.ds(0, first_rows(g)), cols(src_s, g)],
                    send_sem=ssem.at[1, 0], recv_sem=rsem1.at[core, g],
                    device_id=(rep, 1 - tp, src_s), device_id_type=MESH).wait_recv()
        for c in wo_y:
            c.wait_send()
        for k in range(SP):
            wo_x(k).wait_send()
        for k in range(3):
            wo_near(k).wait()
        for k in range(5):
            wo_near_far(k).wait()


def _attention(q, k0, v0, k1, v1, wo, wo_oth):
    n = k0.shape[0]
    _, m2, w = q.shape
    nh = w // LANES
    steps = 2 * m2 // BQ
    any_ = pl.BlockSpec(memory_space=pl.ANY)
    shape = jax.ShapeDtypeStruct((2, BQ, SP * w), BF16)
    return pl.pallas_call(
        _attn_body,
        grid=(steps,),
        in_specs=[pl.BlockSpec((1, BQ, w), lambda t: (t % 2, t // 2, 0))] + [any_] * 6,
        out_specs=[any_] * 5,
        out_shape=[shape, jax.ShapeDtypeStruct((BQ, SP * w), BF16), jax.ShapeDtypeStruct(wo.shape, BF16),
                   jax.ShapeDtypeStruct((2, 2, BQ, w), BF16), jax.ShapeDtypeStruct((2, LATE_ROWS, w), BF16)],
        input_output_aliases={6: 2},
        scratch_shapes=[
            pltpu.VMEM((2, n, LANES), BF16),
            pltpu.VMEM((2, n, LANES), BF16),
            pltpu.VMEM((2, LANES, n), BF16),
            pltpu.VMEM((BQ, BQ), BF16),
            pltpu.VMEM((nh, LANES, BQ), F32),
            pltpu.VMEM((8, BQ), F32),
            pltpu.VMEM((8, BQ), F32),
            pltpu.VMEM((steps, BQ, w), BF16),
            pltpu.SemaphoreType.DMA((2, 2)),
            pltpu.SemaphoreType.DMA((2, 8)),
            pltpu.SemaphoreType.DMA((2, 2)),
            pltpu.SemaphoreType.DMA((2, 2)),
            pltpu.SemaphoreType.DMA((2, 2)),
            pltpu.SemaphoreType.DMA((2, 2)),
            pltpu.SemaphoreType.DMA((2,)),
            pltpu.SemaphoreType.DMA((4, 5)),
            pltpu.SemaphoreType.DMA((4, 5)),
        ],
        compiler_params=pltpu.CompilerParams(collective_id=2, has_side_effects=True, vmem_limit_bytes=KERNEL_VMEM),
        cost_estimate=pl.CostEstimate(flops=2 * n * n * w * 2, bytes_accessed=16 * MIB, transcendentals=0),
        name="attention_exchange",
    )(q, k0, v0, k1, v1, wo, wo_oth)


NWO, NHID, NW2 = 8, 28, 16
UNITS = NWO + NHID + NW2
NBUF = 3
MB = RB


def _mlp_body(chunks, own_hbm, oth_hbm, x_hbm, wo_hbm, wo_oth_hbm, g_ref, w1_hbm, w3_hbm, w2_hbm, late_hbm, late2_hbm, y_hbm, olate_hbm, olate2_hbm,
              wb, abuf, xbuf, hid, pbuf, rbuf, ybuf, wsem, asem, ssem, rsem, ysem, yrsem, ylsem, lasem, larsem, l2sem, l2rsem):
    rep, tp, s = lax.axis_index("rep"), lax.axis_index("tp"), lax.axis_index("sp")
    hr = wo_hbm.shape[0]
    hm = x_hbm.shape[0] // 2
    kh = w2_hbm.shape[0] // 2
    total = UNITS * len(chunks)
    partner = (rep, 1 - tp, s)

    def col(j, w):
        return pl.ds(pl.multiple_of(j * w, w), w)

    def wo_copies(j, sl):
        return [pltpu.make_async_copy(wo_hbm.at[:, col(j, TILE)], wb.at[sl, pl.ds(0, hr), :], wsem.at[sl, 0]),
                pltpu.make_async_copy(wo_oth_hbm.at[:, col(j, TILE)], wb.at[sl, pl.ds(hr, hr), :], wsem.at[sl, 1])]

    def hid_copies(j, sl):
        return [pltpu.make_async_copy(w1_hbm.at[:, col(j, RB)], wb.at[sl, :, pl.ds(0, RB)], wsem.at[sl, 0]),
                pltpu.make_async_copy(w3_hbm.at[:, col(j, RB)], wb.at[sl, :, pl.ds(RB, RB)], wsem.at[sl, 1])]

    def w2_copies(t, sl):
        return [pltpu.make_async_copy(w2_hbm.at[pl.ds(pl.multiple_of(t % 2 * kh, LANES), kh), col(t // 2, TILE)], wb.at[sl, pl.ds(0, kh), :], wsem.at[sl, 0])]

    def issue(g):
        sl, u = g % NBUF, g % UNITS

        @pl.when(g < total)
        def _():
            @pl.when(u < NWO)
            def _():
                for c in wo_copies(u, sl):
                    c.start()

            @pl.when((u >= NWO) & (u < NWO + NHID))
            def _():
                for c in hid_copies(u - NWO, sl):
                    c.start()

            @pl.when(u >= NWO + NHID)
            def _():
                for c in w2_copies(u - NWO - NHID, sl):
                    c.start()

    def acts(c):
        slot, r0, nr = chunks[c]
        base = hm * ((tp + slot + 1) % 2) + r0
        rs = pl.ds(0, nr)
        xcopy = pltpu.make_async_copy(x_hbm.at[pl.ds(pl.multiple_of(base, LANES), nr), :], xbuf.at[rs, :], asem.at[0])
        cs = [pltpu.make_async_copy(own_hbm.at[slot, pl.ds(r0, nr), :], abuf.at[rs, pl.ds(0, hr)], asem.at[1])]
        late_at = hm - LATE_ROWS
        if slot == 1:
            cs.append(pltpu.make_async_copy(olate_hbm.at[pl.ds(r0, nr), :], abuf.at[rs, pl.ds(hr, hr)], asem.at[2]))
        elif r0 + nr <= late_at:
            cs.append(pltpu.make_async_copy(oth_hbm.at[pl.ds(r0, nr), :], abuf.at[rs, pl.ds(hr, hr)], asem.at[2]))
        else:
            n0 = late_at - r0
            c0 = pl.multiple_of(s // CORES * (hr // 2), LANES)
            c1 = pl.multiple_of((1 - s // CORES) * (hr // 2), LANES)
            ls = pl.ds(n0, LATE_ROWS)
            cs.append(pltpu.make_async_copy(oth_hbm.at[pl.ds(r0, n0), :], abuf.at[pl.ds(0, n0), pl.ds(hr, hr)], asem.at[2]))
            cs.append(pltpu.make_async_copy(oth_hbm.at[pl.ds(late_at, LATE_ROWS), pl.ds(c0, hr // 2)], abuf.at[ls, pl.ds(hr + c0, hr // 2)], asem.at[3]))
            cs.append(pltpu.make_async_copy(olate2_hbm, abuf.at[ls, pl.ds(hr + c1, hr // 2)], asem.at[4]))
        return xcopy, cs

    for g in range(NBUF - 1):
        issue(g)
    xc, ac = acts(0)
    xc.start()
    for c in ac:
        c.start()
    mate = s + 1 - 2 * (s % CORES)
    _barrier([partner, (rep, 1 - tp, mate)])
    w = late_hbm.shape[3]

    def late(g, cc, src_s):
        return pltpu.make_async_remote_copy(
            src_ref=late_hbm.at[g, cc], dst_ref=olate_hbm.at[:, pl.ds(pl.multiple_of((src_s + 2 * g) % SP * w, LANES), w)],
            send_sem=lasem.at[g, cc], recv_sem=larsem.at[g, src_s % CORES],
            device_id=(rep, 1 - tp, s // CORES * 2 + cc), device_id_type=MESH)

    def late2(cc, src_s):
        return pltpu.make_async_remote_copy(
            src_ref=late2_hbm.at[cc], dst_ref=olate2_hbm.at[:, pl.ds(pl.multiple_of(src_s % CORES * w, LANES), w)],
            send_sem=l2sem.at[cc], recv_sem=l2rsem.at[src_s % CORES],
            device_id=(rep, 1 - tp, s // CORES * 2 + cc), device_id_type=MESH)

    for cc in range(CORES):
        late2(cc, s).start()
    for g in range(CORES):
        for cc in range(CORES):
            late(g, cc, s).start()

    def send(ci, j):
        slot, r0, nr = chunks[ci]
        return pltpu.make_async_remote_copy(src_ref=pbuf.at[j, pl.ds(r0, nr), :], dst_ref=rbuf.at[j, pl.ds(r0, nr), :],
                                            send_sem=ssem.at[ci, j], recv_sem=rsem.at[ci, j], device_id=partner, device_id_type=MESH)

    yr0 = pl.multiple_of(tp * hm, LANES)

    def ysend(j):
        return pltpu.make_async_remote_copy(src_ref=ybuf.at[j], dst_ref=y_hbm.at[pl.ds(yr0, hm), col(j, TILE)],
                                            send_sem=ysem.at[j], recv_sem=yrsem.at[j], device_id=partner, device_id_type=MESH)

    def yrecv(j):
        return pltpu.make_async_remote_copy(src_ref=ybuf.at[j], dst_ref=y_hbm.at[pl.ds(pl.multiple_of((1 - tp) * hm, LANES), hm), col(j, TILE)],
                                            send_sem=ysem.at[j], recv_sem=yrsem.at[j], device_id=partner, device_id_type=MESH)

    def yown(j):
        return pltpu.make_async_copy(ybuf.at[j], y_hbm.at[pl.ds(yr0, hm), col(j, TILE)], ylsem.at[j])

    nsend = len(chunks) - 1
    for ci, (slot, r0, nr) in enumerate(chunks):
        g0 = ci * UNITS
        xc, ac = acts(ci)
        xc.wait()
        for c in ac:
            c.wait()

        @pl.loop(0, NWO)
        def _(j, g0=g0, nr=nr):
            g = g0 + j
            sl = g % NBUF
            issue(g + NBUF - 1)
            for c in wo_copies(j, sl):
                c.wait()
            for b in range(nr // MB):
                rs = pl.ds(b * MB, MB)
                o = jnp.dot(abuf[rs, :], wb[sl], preferred_element_type=F32)
                xbuf[rs, col(j, TILE)] = (xbuf[rs, col(j, TILE)].astype(F32) + o).astype(BF16)

        @pl.loop(0, nr // HALF)
        def _(i):
            rs = pl.ds(pl.multiple_of(i * HALF, HALF), HALF)
            xs = xbuf[rs, :].astype(F32)
            r = lax.rsqrt(jnp.mean(xs * xs, axis=-1, keepdims=True) + EPS)
            abuf[rs, :] = (xs * r * g_ref[...]).astype(BF16)

        if ci + 1 < len(chunks):
            acts(ci + 1)[0].start()

        @pl.loop(0, NHID)
        def _(j, g0=g0, nr=nr):
            g = g0 + NWO + j
            sl = g % NBUF
            issue(g + NBUF - 1)
            for c in hid_copies(j, sl):
                c.wait()
            for b in range(nr // MB):
                rs = pl.ds(b * MB, MB)
                ab = jnp.dot(abuf[rs, :], wb[sl], preferred_element_type=F32)
                a = ab[:, :RB]
                hid[rs, col(j, RB)] = (a / (1.0 + jnp.exp(-a)) * ab[:, RB:]).astype(BF16)

        if ci + 3 == len(chunks):
            for core in range(CORES):
                late2(core, s // CORES * 2 + core).wait_recv()
        if ci + 2 == len(chunks):
            for g in range(CORES):
                for core in range(CORES):
                    late(g, core, s // CORES * 2 + core).wait_recv()
        if ci + 1 < len(chunks):
            for c in acts(ci + 1)[1]:
                c.start()

        @pl.loop(0, NW2 // 2)
        def _(j, g0=g0, ci=ci, slot=slot, r0=r0, nr=nr):
            g = g0 + NWO + NHID + 2 * j
            for h in range(CORES):
                sl = (g + h) % NBUF
                issue(g + h + NBUF - 1)
                for c in w2_copies(2 * j + h, sl):
                    c.wait()
                for b in range(nr // MB):
                    rs = pl.ds(b * MB, MB)
                    ps = pl.ds(r0 + b * MB, MB)
                    o = jnp.dot(hid[rs, h * kh:(h + 1) * kh], wb[sl, pl.ds(0, kh), :], preferred_element_type=F32)
                    if h == 0:
                        pbuf[j if slot == 0 else NW2 // 2, ps, :] = o
                    elif slot == 0:
                        pbuf[j, ps, :] = pbuf[j, ps, :] + o
                    else:
                        if b == 0:
                            for k in range(nsend):
                                send(k, j).wait_recv()
                        o = o + pbuf[NW2 // 2, ps, :] + rbuf[j, ps, :]
                        ybuf[j, ps, :] = (xbuf[rs, col(j, TILE)].astype(F32) + o).astype(BF16)
            if slot == 0:
                send(ci, j).start()
            else:
                ysend(j).start()
                yown(j).start()

    for cc in range(CORES):
        late2(cc, s).wait_send()
        for g in range(CORES):
            late(g, cc, s).wait_send()

    @pl.loop(0, NW2 // 2)
    def _(j):
        for k in range(nsend):
            send(k, j).wait_send()
        ysend(j).wait_send()
        yown(j).wait()
        yrecv(j).wait_recv()


def _mlp(own, oth, late, late2, x, wo, wo_oth, g2, w1, w3, w2):
    m, d = x.shape
    hm = m // 2
    chunks = ((0, 0, RB), (0, RB, RB), (1, 0, TILE))
    any_ = pl.BlockSpec(memory_space=pl.ANY)
    vm = pl.BlockSpec(memory_space=pltpu.VMEM)
    nt = NW2 // 2
    return pl.pallas_call(
        functools.partial(_mlp_body, chunks),
        in_specs=[any_] * 5 + [vm] + [any_] * 5,
        out_specs=[any_] * 3,
        out_shape=[jax.ShapeDtypeStruct((m, d), BF16), jax.ShapeDtypeStruct((hm, wo.shape[0]), BF16),
                   jax.ShapeDtypeStruct((LATE_ROWS, wo.shape[0] // 2), BF16)],
        scratch_shapes=[
            pltpu.VMEM((NBUF, d, TILE), BF16),
            pltpu.VMEM((hm, d), BF16),
            pltpu.VMEM((hm, d), BF16),
            pltpu.VMEM((hm, w2.shape[0]), BF16),
            pltpu.VMEM((nt + 1, hm, TILE), F32),
            pltpu.VMEM((nt, hm, TILE), F32),
            pltpu.VMEM((nt, hm, TILE), BF16),
            pltpu.SemaphoreType.DMA((NBUF, 2)),
            pltpu.SemaphoreType.DMA((5,)),
            pltpu.SemaphoreType.DMA((2, nt)),
            pltpu.SemaphoreType.DMA((2, nt)),
            pltpu.SemaphoreType.DMA((nt,)),
            pltpu.SemaphoreType.DMA((nt,)),
            pltpu.SemaphoreType.DMA((nt,)),
            pltpu.SemaphoreType.DMA((2, 2)),
            pltpu.SemaphoreType.DMA((2, 2)),
            pltpu.SemaphoreType.DMA((2,)),
            pltpu.SemaphoreType.DMA((2,)),
        ],
        compiler_params=pltpu.CompilerParams(collective_id=3, has_side_effects=True, vmem_limit_bytes=MAX_VMEM),
        cost_estimate=pl.CostEstimate(flops=2 * m * d * (d + 3 * w1.shape[1]), bytes_accessed=640 * MIB, transcendentals=0),
        name="mlp_sum",
    )(own, oth, x, wo, wo_oth, g2.reshape(1, -1), w1, w3, w2, late, late2)[0]


def _copy_body(y_ref, k_ref, v_ref, yo_ref, ko_ref, vo_ref, buf, kbuf, sem):
    n, nr = buf.shape[:2]
    moves = [(k_ref, ko_ref, kbuf.at[0]), (v_ref, vo_ref, kbuf.at[1])]
    moves += [(y_ref.at[pl.ds(i * nr, nr), :], yo_ref.at[pl.ds(i * nr, nr), :], buf.at[i]) for i in range(n)]
    get = [pltpu.make_async_copy(a, b, sem.at[0, i]) for i, (a, _, b) in enumerate(moves)]
    put = [pltpu.make_async_copy(b, c, sem.at[1, i]) for i, (_, c, b) in enumerate(moves)]
    for c in get:
        c.start()
    for g, p in zip(get, put):
        g.wait()
        p.start()
    for p in put:
        p.wait()


def _copy(*arrays):
    y, k, _ = arrays
    m, d = y.shape
    any_ = pl.BlockSpec(memory_space=pl.ANY)
    return pl.pallas_call(
        _copy_body,
        in_specs=[any_] * 3,
        out_specs=[any_] * 3,
        out_shape=[jax.ShapeDtypeStruct(a.shape, a.dtype) for a in arrays],
        scratch_shapes=[pltpu.VMEM((16, m // 16, d), BF16), pltpu.VMEM((2, *k.shape), BF16), pltpu.SemaphoreType.DMA((2, 18))],
        compiler_params=pltpu.CompilerParams(vmem_limit_bytes=MAX_VMEM),
        name="result_copy",
    )(*arrays)


def solution(mesh):
    tok = P(("rep", "sp"), None)
    col = P(None, "tp")
    row = P("tp", None)
    cache = P("rep", ("tp", "sp"), None)

    def local(x, pos, g1, g2, wq, wk, wv, wo, w1, w3, w2):
        m, d = x.shape
        n = m * mesh.shape["sp"]
        cos, sin = _tables(pos)
        q, k, v, k1, v1, wo_oth = _qkv(x, g1, cos, sin, wq, wk, wv, wo, n)
        own, oth, wo_oth, late, late2 = _attention(q, k, v, k1, v1, wo, wo_oth)
        y = _mlp(own, oth, late, late2, x, wo, wo_oth, g2, w1, w3, w2)
        y, k, v = _copy(y, k, v)
        return y, k.reshape(n, 1, LANES), v.reshape(n, 1, LANES)

    return jax.shard_map(
        local,
        mesh=mesh,
        in_specs=(tok, P(("rep", "sp")), P(), P(), col, col, col, row, col, col, row),
        out_specs=(tok, cache, cache),
        check_vma=False,
    )
```
